8 devices in a mesh: fsdp: 8 (over z, y, x, core).
Axes of the slice: x: 2, y: 2, z: 1, core: 2. Of those that a mesh axis runs over, the one named last changes fastest.
Arguments:
- tokens: int32 [96, 256], P('fsdp')
- positions: int32 [96, 256], P('fsdp')
- embed_table: bfloat16 [49152, 576], P('fsdp')
- attn_norm: bfloat16 [576], P('fsdp')
- w_query: bfloat16 [576, 576], P('fsdp')
- w_key: bfloat16 [576, 192], P('fsdp')
- w_value: bfloat16 [576, 192], P('fsdp')
- q_norm: bfloat16 [64], replicated
- k_norm: bfloat16 [64], replicated
- w_out: bfloat16 [576, 576], P('fsdp')
- mlp_norm: bfloat16 [576], P('fsdp')
- w_gate: bfloat16 [576, 1536], P('fsdp')
- w_up: bfloat16 [576, 1536], P('fsdp')
- w_down: bfloat16 [1536, 576], P('fsdp')
- dy_out: bfloat16 [96, 256, 576], P('fsdp')
Outputs:
- output 1: bfloat16 [96, 256, 576], P('fsdp')
- output 2: float32 [49152, 576], P('fsdp')
- output 3: float32 [576], P('fsdp')
- output 4: float32 [576, 576], P('fsdp')
- output 5: float32 [576, 192], P('fsdp')
- output 6: float32 [576, 192], P('fsdp')
- output 7: float32 [64], replicated
- output 8: float32 [64], replicated
- output 9: float32 [576, 576], P('fsdp')
- output 10: float32 [576], P('fsdp')
- output 11: float32 [576, 1536], P('fsdp')
- output 12: float32 [576, 1536], P('fsdp')
- output 13: float32 [1536, 576], P('fsdp')
All inputs are finite; a program needn't handle non-finite values.
Results may differ from the reference program's by a relative error of at most 0.02.
Values are sent between devices in bfloat16 or wider.
A program may use at most 1 GiB of HBM per device.

```python
import math
import jax
import jax.numpy as jnp
from jax import lax

D = 576
HEADS = 9
KV_HEADS = 3
HEAD = 64
FF = 1536
VOCAB = 49152
VOCAB_P = 49152
GROUP = 8
BATCH_DEV = 12
SEQ = 256

BATCH = GROUP * BATCH_DEV
Q_PER_KV = HEADS // KV_HEADS
ROWS_SHARD = VOCAB_P // GROUP
DOC_SPAN = max(SEQ // 4, 2)
NORM_EPS = 1e-6
ROPE_THETA = 1.0e6


def draw_tokens(rng_key):
    key_list = jax.random.split(rng_key, 4)
    id_top = jax.random.randint(key_list[0], (BATCH, SEQ), 1, VOCAB + 1)
    id_mid = jax.random.randint(key_list[1], (BATCH, SEQ), 0, id_top)
    token_ids = jax.random.randint(key_list[2], (BATCH, SEQ), 0, id_mid + 1)
    shard_lo = (jnp.arange(BATCH) % GROUP) * ROWS_SHARD
    shard_hi = jnp.minimum(shard_lo + ROWS_SHARD, VOCAB)
    cover_ids = jax.random.randint(key_list[3], (BATCH,), shard_lo, shard_hi)
    token_ids = token_ids.at[:, 0].set(cover_ids)
    return token_ids.at[BATCH - 1, SEQ - 1].set(VOCAB - 1).astype(jnp.int32)


def draw_positions(rng_key):
    seq_idx = jnp.arange(SEQ, dtype=jnp.int32)[None, :]
    starts = (jax.random.randint(rng_key, (BATCH, SEQ), 0, DOC_SPAN) == 0) | (seq_idx == 0)
    last_start = lax.cummax(jnp.where(starts, seq_idx, 0), axis=1)
    return (seq_idx - last_start).astype(jnp.int32)


def setup_inputs(seed: int = 0) -> dict:
    key_list = jax.random.split(jax.random.key(seed), 16)

    def weight(key_idx, arr_shape, fan_in):
        return (jax.random.normal(key_list[key_idx], arr_shape, jnp.float32) * fan_in ** -0.5).astype(jnp.bfloat16)

    def gain_vec(key_idx, vec_len):
        return (1.0 + 0.25 * jax.random.normal(key_list[key_idx], (vec_len,), jnp.float32)).astype(jnp.bfloat16)

    table_f = jax.random.normal(key_list[2], (VOCAB_P, D), jnp.float32)
    table_f = jnp.where(jnp.arange(VOCAB_P)[:, None] < VOCAB, table_f, 0.0)
    return {
        'tokens': draw_tokens(key_list[0]),
        'positions': draw_positions(key_list[1]),
        'embed_table': table_f.astype(jnp.bfloat16),
        'attn_norm': gain_vec(3, D),
        'w_query': weight(4, (D, HEADS * HEAD), D),
        'w_key': weight(5, (D, KV_HEADS * HEAD), D),
        'w_value': weight(6, (D, KV_HEADS * HEAD), D),
        'q_norm': gain_vec(7, HEAD),
        'k_norm': gain_vec(8, HEAD),
        'w_out': weight(9, (HEADS * HEAD, D), HEADS * HEAD),
        'mlp_norm': gain_vec(10, D),
        'w_gate': weight(11, (D, FF), D),
        'w_up': weight(12, (D, FF), D),
        'w_down': weight(13, (FF, D), FF),
        'dy_out': jax.random.normal(key_list[14], (BATCH, SEQ, D), jnp.float32).astype(jnp.bfloat16),
    }


def to_bf16(values):
    return values + lax.stop_gradient(values.astype(jnp.bfloat16).astype(jnp.float32) - values)


def rms_scale(values, norm_gain):
    inv_rms = lax.rsqrt(jnp.mean(values * values, axis=-1, keepdims=True) + NORM_EPS)
    return values * inv_rms * norm_gain


def rope_tables(positions):
    half_dim = HEAD // 2
    inv_freq = jnp.exp(jnp.arange(half_dim, dtype=jnp.float32) * (-2.0 * math.log(ROPE_THETA) / HEAD))
    angles = positions.astype(jnp.float32)[:, :, None] * inv_freq
    return jnp.cos(angles), jnp.sin(angles)


def rotate(values, cos_t, sin_t):
    half_dim = values.shape[-1] // 2
    lead_half = values[..., :half_dim]
    tail_half = values[..., half_dim:]
    return jnp.concatenate([lead_half * cos_t - tail_half * sin_t, tail_half * cos_t + lead_half * sin_t], axis=-1)


def seq_attend(operands):
    q_seq, k_seq, v_seq = operands
    scores = jnp.einsum('qgrh,kgh->grqk', q_seq, k_seq) * (HEAD ** -0.5)
    causal = jnp.arange(SEQ)[:, None] >= jnp.arange(SEQ)[None, :]
    scores = jnp.where(causal, scores, -1e30)
    attn_probs = to_bf16(jax.nn.softmax(scores, axis=-1))
    return to_bf16(jnp.einsum('grqk,kgh->qgrh', attn_probs, v_seq))


def reference(tokens, positions, embed_table, attn_norm, w_query, w_key, w_value, q_norm, k_norm, w_out, mlp_norm, w_gate, w_up, w_down, dy_out):
    cos_t, sin_t = rope_tables(positions)
    cos_q = cos_t[:, :, None, None, :]
    sin_q = sin_t[:, :, None, None, :]
    cos_k = cos_t[:, :, None, :]
    sin_k = sin_t[:, :, None, :]

    def layer_fwd(x_emb, g_attn, wt_query, wt_key, wt_value, g_query, g_key, wt_out, g_mlp, wt_gate, wt_up, wt_down):
        normed = to_bf16(rms_scale(x_emb, g_attn)).reshape(BATCH * SEQ, D)
        q_proj = to_bf16(jnp.dot(normed, wt_query, preferred_element_type=jnp.float32)).reshape(BATCH, SEQ, KV_HEADS, Q_PER_KV, HEAD)
        k_proj = to_bf16(jnp.dot(normed, wt_key, preferred_element_type=jnp.float32)).reshape(BATCH, SEQ, KV_HEADS, HEAD)
        v_proj = to_bf16(jnp.dot(normed, wt_value, preferred_element_type=jnp.float32)).reshape(BATCH, SEQ, KV_HEADS, HEAD)
        q_rot = to_bf16(rotate(rms_scale(q_proj, g_query), cos_q, sin_q))
        k_rot = to_bf16(rotate(rms_scale(k_proj, g_key), cos_k, sin_k))
        attn_heads = lax.map(jax.checkpoint(seq_attend), (q_rot, k_rot, v_proj))
        attn_proj = jnp.dot(attn_heads.reshape(BATCH * SEQ, HEADS * HEAD), wt_out, preferred_element_type=jnp.float32)
        hidden = to_bf16(x_emb + attn_proj.reshape(BATCH, SEQ, D))
        mlp_in = to_bf16(rms_scale(hidden, g_mlp)).reshape(BATCH * SEQ, D)
        gate_pre = jnp.dot(mlp_in, wt_gate, preferred_element_type=jnp.float32)
        up_proj = jnp.dot(mlp_in, wt_up, preferred_element_type=jnp.float32)
        mlp_act = to_bf16(jax.nn.silu(gate_pre) * up_proj)
        mlp_proj = jnp.dot(mlp_act, wt_down, preferred_element_type=jnp.float32)
        return to_bf16(hidden + mlp_proj.reshape(BATCH, SEQ, D))

    x_emb = jnp.take(embed_table, tokens, axis=0).astype(jnp.float32)
    params = [weight_arr.astype(jnp.float32) for weight_arr in (attn_norm, w_query, w_key, w_value, q_norm, k_norm, w_out, mlp_norm, w_gate, w_up, w_down)]
    layer_out, pullback = jax.vjp(layer_fwd, x_emb, *params)
    grad_list = pullback(dy_out.astype(jnp.float32))
    d_table = jax.ops.segment_sum(grad_list[0].reshape(BATCH * SEQ, D), tokens.reshape(BATCH * SEQ), num_segments=VOCAB_P)
    return (layer_out.astype(jnp.bfloat16), d_table, grad_list[1], grad_list[2], grad_list[3], grad_list[4], grad_list[5], grad_list[6], grad_list[7], grad_list[8], grad_list[9], grad_list[10], grad_list[11])
```

```python
import functools
import math
import jax
import jax.numpy as jnp
from jax import lax
from jax.experimental import pallas as pl
from jax.experimental.pallas import tpu as pltpu
from jax.sharding import PartitionSpec as P

NORM_EPS = 1e-6
ROPE_THETA = 1.0e6
AXIS_NAME = 'fsdp'
SEQ = 256
D = 576
FF = 1536
HEAD = 64
HEADS = 9
KV = 3
GRP = 3
C_QKV, C_OUT, C_GATE, C_UP, C_NORM, C_HEAD = 0, 1024, 1664, 3200, 4736, 4864
W_COLS, G_COLS = 4864, 4992
X_K, X_V, X_COLS = HEADS * 128, (HEADS + KV) * 128, (HEADS + 2 * KV) * 128
FF_STEP = 512
CHUNKS = (4, 4, 4)
BF, F32 = jnp.bfloat16, jnp.float32


def mm(lhs, rhs, lhs_dim=1, rhs_dim=0):
    return lax.dot_general(lhs, rhs, (((lhs_dim,), (rhs_dim,)), ((), ())), preferred_element_type=F32)


def fold8(values):
    return jnp.sum(values.reshape(values.shape[0] // 8, 8, values.shape[1]), axis=0)


def norm_bwd(grad_out, normed, inv_rms, norm_gain):
    grad_normed = grad_out * norm_gain
    return inv_rms * (grad_normed - normed * jnp.mean(grad_normed * normed, axis=-1, keepdims=True))


def head_norm_rope(head_ext, gain_ext, cs):
    head_f = head_ext.astype(F32)
    inv = lax.rsqrt(jnp.sum(head_f * head_f, axis=-1, keepdims=True) * (1.0 / 128) + NORM_EPS)
    turned = head_f * inv * gain_ext * cs
    return turned + pltpu.roll(turned, 64, 1), inv


def head_norm_rope_bwd(grad_ext, head_ext, inv, gain_low, cs_bwd, low):
    turned = grad_ext * cs_bwd
    grad_t = turned + pltpu.roll(turned, 64, 1)
    normed = jnp.where(low, head_ext.astype(F32), 0.0) * inv
    grad_normed = grad_t * gain_low
    mean_term = jnp.sum(grad_normed * normed, axis=-1, keepdims=True) * (1.0 / HEAD)
    return inv * (grad_normed - normed * mean_term), fold8(grad_t * normed)


def pack_pairs(heads):
    tiles = []
    for idx in range(0, len(heads), 2):
        tile = heads[idx]
        if idx + 1 < len(heads):
            tile = tile + pltpu.roll(heads[idx + 1], 64, 1)
        tiles.append(tile.astype(BF))
    return tiles


def layer_kernel(first, last, steps, *refs):
    (x_ref, dy_ref, cs_ref, w_ref, wd_ref, gains_ref, head_gains_ref) = refs[:7]
    refs = refs[7:]
    if not first:
        acc_in, accd_in, _ = refs[:3]
        refs = refs[3:]
    (y_ref, dx_ref, acc_out, accd_out) = refs[:4]
    (acc, accd, norm_acc, head_acc, wx, wox, qkv_s, probs_s, tbuf, sems) = refs[4:]
    step = pl.program_id(0)
    low = lax.broadcasted_iota(jnp.int32, (1, 128), 1) < 64

    @pl.when(step == 0)
    def _():
        if first:
            acc[...] = jnp.zeros_like(acc)
            accd[...] = jnp.zeros_like(accd)
        else:
            load_acc = pltpu.make_async_copy(acc_in, acc, sems.at[0])
            load_accd = pltpu.make_async_copy(accd_in, accd, sems.at[1])
            load_acc.start()
            load_accd.start()
        norm_acc[...] = jnp.zeros_like(norm_acc)
        head_acc[...] = jnp.zeros_like(head_acc)
        for h in range(HEADS + 2 * KV):
            tile = w_ref[:, (h // 2) * 128:(h // 2) * 128 + 128].astype(F32)
            moved = pltpu.roll(tile, 64, 1)
            if h >= HEADS + KV:
                both = jnp.where(low, moved if h % 2 else tile, 0.0)
            else:
                twice = jnp.where(low, moved, tile) if h % 2 else jnp.where(low, tile, moved)
                both = jnp.where(low, twice, pltpu.roll(twice, 32, 1))
            wx[:, h * 128:h * 128 + 128] = both.astype(BF)
        for h in range(HEADS):
            wox[h * 128:h * 128 + 64, :] = w_ref[h * 64:h * 64 + 64, C_OUT:C_OUT + D]
            wox[h * 128 + 64:h * 128 + 128, :] = jnp.zeros((64, D), BF)
        if not first:
            load_acc.wait()
            load_accd.wait()

    gain1 = gains_ref[0:1, :]
    gain2 = gains_ref[1:2, :]
    gain_q, gain_k = head_gains_ref[0:1, :], head_gains_ref[1:2, :]
    low_q, low_k = jnp.where(low, gain_q, 0.0), jnp.where(low, gain_k, 0.0)
    cs = cs_ref[...]
    cs_bwd = jnp.where(low, cs, -cs)
    causal = ((lax.broadcasted_iota(jnp.int32, (GRP * SEQ, SEQ), 0) & (SEQ - 1))
              >= lax.broadcasted_iota(jnp.int32, (GRP * SEQ, SEQ), 1))

    x = x_ref[...].astype(F32)
    inv1 = lax.rsqrt(jnp.mean(x * x, axis=-1, keepdims=True) + NORM_EPS)
    m1 = (x * inv1 * gain1).astype(BF)
    qkv_s[...] = mm(m1, wx[...]).astype(BF)
    saved = []
    heads = []
    for g in range(KV):
        ke = qkv_s[:, X_K + g * 128:X_K + g * 128 + 128]
        v0 = qkv_s[:, X_V + g * 128:X_V + g * 128 + 128]
        k_rot, k_inv = head_norm_rope(ke, gain_k, cs)
        k0 = jnp.where(low, k_rot, 0.0).astype(BF)
        k_swap = jnp.where(low, k_rot, pltpu.roll(k_rot, 32, 1)).astype(BF)
        qs, q_swaps, q_invs = [], [], []
        for r in range(GRP):
            h = g * GRP + r
            q_rot, q_inv = head_norm_rope(qkv_s[:, h * 128:h * 128 + 128], gain_q, cs)
            qs.append(q_rot.astype(BF))
            q_swaps.append(jnp.where(low, q_rot, pltpu.roll(q_rot, 32, 1)).astype(BF))
            q_invs.append(q_inv)
        scores = mm(jnp.concatenate(qs, axis=0), k0, 1, 1) * (HEAD ** -0.5)
        scores = jnp.where(causal, scores, -1e30)
        expd = jnp.exp(scores - jnp.max(scores, axis=-1, keepdims=True))
        probs = expd / jnp.sum(expd, axis=-1, keepdims=True)
        probs_s[g] = probs
        o = mm(probs.astype(BF), v0)
        for r in range(GRP):
            heads.append(o[r * SEQ:(r + 1) * SEQ])
        saved.append((k_swap, jnp.concatenate(q_swaps, axis=0), q_invs, k_inv))
    attn = jnp.concatenate(pack_pairs(heads), axis=1)
    hidden_b = (x + mm(attn[:, :D], w_ref[:, C_OUT:C_OUT + D])).astype(BF)
    hidden = hidden_b.astype(F32)
    inv2 = lax.rsqrt(jnp.mean(hidden * hidden, axis=-1, keepdims=True) + NORM_EPS)
    m2 = (hidden * inv2 * gain2).astype(BF)

    dy = dy_ref[...]
    m2_t = m2.T
    dy_t = dy.T
    y = hidden
    dm2 = jnp.zeros((SEQ, D), F32)
    for f in range(0, FF, FF_STEP):
        wg = w_ref[:, C_GATE + f:C_GATE + f + FF_STEP]
        wu = w_ref[:, C_UP + f:C_UP + f + FF_STEP]
        wd = wd_ref[f:f + FF_STEP, :]
        gate = mm(m2, wg)
        up = mm(m2, wu)
        dact = mm(dy, wd, 1, 1)
        sig = 1.0 / (1.0 + jnp.exp(-gate))
        silu = gate * sig
        act = (silu * up).astype(BF)
        y = y + mm(act, wd)
        dgate = (dact * up * sig * (1.0 + gate * (1.0 - sig))).astype(BF)
        dup = (dact * silu).astype(BF)
        dm2 = dm2 + mm(dgate, wg, 1, 1) + mm(dup, wu, 1, 1)
        acc[:, C_GATE + f:C_GATE + f + FF_STEP] += mm(m2_t, dgate)
        acc[:, C_UP + f:C_UP + f + FF_STEP] += mm(m2_t, dup)
        accd[:, f:f + FF_STEP] += mm(dy_t, act)
    y_ref[...] = y.astype(BF)
    n2 = hidden * inv2
    norm_acc[1] += fold8(dm2 * n2)
    dh = dy.astype(F32) + norm_bwd(dm2, n2, inv2, gain2)
    dh_b = dh.astype(BF)
    acc[:, C_OUT:C_OUT + D] += mm(attn.T, dh_b)[:D]

    do = mm(dh_b, wox[...], 1, 1).astype(BF)
    dqs, dks, dvs = [], [], []
    for g in range(KV):
        k_swap, q_swap, q_invs, k_inv = saved[g]
        v0 = qkv_s[:, X_V + g * 128:X_V + g * 128 + 128]
        do_g = jnp.concatenate([do[:, h * 128:h * 128 + 128] for h in range(g * GRP, (g + 1) * GRP)], axis=0)
        probs = probs_s[g]
        dprobs = mm(do_g, v0, 1, 1)
        dvs.append(mm(do_g.T, probs.astype(BF)).T)
        dscores = probs * (dprobs - jnp.sum(dprobs * probs, axis=-1, keepdims=True)) * (HEAD ** -0.5)
        dscores = dscores.astype(BF)
        dq = mm(dscores, k_swap)
        dk = mm(q_swap.T, dscores).T
        dk, dk_gain = head_norm_rope_bwd(dk, qkv_s[:, X_K + g * 128:X_K + g * 128 + 128], k_inv, low_k, cs_bwd, low)
        dks.append(dk)
        head_acc[1] += dk_gain
        for r in range(GRP):
            h = g * GRP + r
            dq_h, dq_gain = head_norm_rope_bwd(dq[r * SEQ:(r + 1) * SEQ], qkv_s[:, h * 128:h * 128 + 128], q_invs[r], low_q, cs_bwd, low)
            dqs.append(dq_h)
            head_acc[0] += dq_gain
    dqkv = jnp.concatenate(pack_pairs(dqs + dks + dvs), axis=1)
    acc[:, 0:1024] += mm(m1.T, dqkv)
    dm1 = mm(dqkv, w_ref[:, 0:1024], 1, 1)
    n1 = x * inv1
    norm_acc[0] += fold8(dm1 * n1)
    dx_ref[...] = dh + norm_bwd(dm1, n1, inv1, gain1)

    @pl.when(step == steps - 1)
    def _():
        top = lax.broadcasted_iota(jnp.int32, (128, 1), 0)
        rows1 = jnp.sum(norm_acc[0], axis=0, keepdims=True)
        rows2 = jnp.sum(norm_acc[1], axis=0, keepdims=True)
        both = jnp.where(top == 0, rows1, 0.0) + jnp.where(top == 1, rows2, 0.0)
        for c in range(0, D, 128):
            width = min(128, D - c)
            acc[c:c + width, C_NORM:C_NORM + 128] += both[:, c:c + width].T
        head_q = jnp.sum(head_acc[0], axis=0, keepdims=True)
        head_k = jnp.sum(head_acc[1], axis=0, keepdims=True)
        head_row = jnp.where(low, head_q, pltpu.roll(head_k, 64, 1))
        acc[:, C_HEAD:C_HEAD + 128] += jnp.broadcast_to(head_row, (D, 128))
        store_acc = pltpu.make_async_copy(acc, acc_out, sems.at[0])
        store_acc.start()
        if last:
            for f in range(0, FF, 512):
                for s in range(0, D, 64):
                    tbuf[:, s:s + 64] = accd[s:s + 64, f:f + 512].T
                store = pltpu.make_async_copy(tbuf, accd_out.at[pl.ds(f, 512), :], sems.at[1])
                store.start()
                store.wait()
        else:
            store_accd = pltpu.make_async_copy(accd, accd_out, sems.at[1])
            store_accd.start()
            store_accd.wait()
        store_acc.wait()


def layer_chunk(x, dy, cs, w_pack, w_down, gains, head_gains, start, carry, last, total):
    steps = x.shape[0] // SEQ
    first = carry is None
    whole = lambda shape: pl.BlockSpec(shape, lambda i: (0,) * len(shape), pipeline_mode=pl.Buffered(1))
    here = lambda cols: pl.BlockSpec((SEQ, cols), lambda i: (i + start, 0))
    anyspec = pl.BlockSpec(memory_space=pl.ANY)
    in_specs = [pl.BlockSpec((SEQ, D), lambda i: (i, 0)), here(D), here(128), whole(w_pack.shape), whole(w_down.shape), whole(gains.shape), whole(head_gains.shape)]
    args = [x, dy, cs, w_pack, w_down, gains, head_gains]
    aliases = {}
    if not first:
        in_specs += [anyspec] * 3
        args += list(carry)
        aliases = {7: 2, 9: 0} if last else {7: 2, 8: 3, 9: 0}
    out_shape = [
        jax.ShapeDtypeStruct((total, D), BF),
        jax.ShapeDtypeStruct((steps * SEQ, D), F32),
        jax.ShapeDtypeStruct((D, G_COLS), F32),
        jax.ShapeDtypeStruct((FF, D) if last else (D, FF), F32),
    ]
    y, dx, acc, accd = pl.pallas_call(
        functools.partial(layer_kernel, first, last, steps),
        grid=(steps,),
        in_specs=in_specs,
        out_specs=[here(D), pl.BlockSpec((SEQ, D), lambda i: (i, 0)), anyspec, anyspec],
        out_shape=out_shape,
        scratch_shapes=[
            pltpu.VMEM((D, G_COLS), F32),
            pltpu.VMEM((D, FF), F32),
            pltpu.VMEM((2, 8, D), F32),
            pltpu.VMEM((2, 8, 128), F32),
            pltpu.VMEM((D, X_COLS), BF),
            pltpu.VMEM((HEADS * 128, D), BF),
            pltpu.VMEM((SEQ, X_COLS), BF),
            pltpu.VMEM((KV, GRP * SEQ, SEQ), F32),
            pltpu.VMEM((512, D), F32),
            pltpu.SemaphoreType.DMA((2,)),
        ],
        input_output_aliases=aliases,
        compiler_params=pltpu.CompilerParams(dimension_semantics=('arbitrary',), vmem_limit_bytes=60 << 20),
        cost_estimate=pl.CostEstimate(flops=steps * 6_000_000_000, bytes_accessed=steps * 2_500_000 + 45_000_000, transcendentals=steps * 1_000_000),
        name='layer_chunk',
    )(*args)
    return dx, (acc, accd, y)


def solution(mesh):
    row_spec = P(AXIS_NAME, None)
    vec_spec = P(AXIS_NAME)
    full_spec = P(None)
    batch_spec = P(AXIS_NAME, None, None)
    weight_specs = (vec_spec, row_spec, row_spec, row_spec, full_spec, full_spec, row_spec, vec_spec, row_spec, row_spec, row_spec)

    def device_step(tokens, positions, table_shard, attn_norm, w_query, w_key, w_value, q_norm, k_norm, w_out, mlp_norm, w_gate, w_up, w_down, dy_out):
        batch_len, seq_len = tokens.shape
        devices = lax.axis_size(AXIS_NAME)
        rows_local = table_shard.shape[0]
        shard = w_query.shape[0]
        all_ids = lax.all_gather(tokens, AXIS_NAME)
        norms = jnp.concatenate([attn_norm[:, None], mlp_norm[:, None], jnp.zeros((shard, W_COLS - C_NORM - 2), BF)], axis=1)
        pad = jnp.zeros((shard, 64), BF)
        packed = jnp.concatenate([w_query, w_key, w_value, pad, w_out, pad, w_gate, w_up, norms], axis=1)
        w_pack = lax.all_gather(packed, AXIS_NAME, tiled=True)
        w_down_full = lax.all_gather(w_down, AXIS_NAME, tiled=True)
        gains = w_pack[:, C_NORM:C_NORM + 2].T.astype(F32)
        head_gains = jnp.stack([q_norm, k_norm]).astype(F32)
        swapped = jnp.concatenate([head_gains[:, 32:], head_gains[:, :32]], axis=1)
        head_gains = jnp.concatenate([head_gains, swapped], axis=1)

        inv_freq = jnp.exp(jnp.arange(HEAD // 2, dtype=F32) * (-2.0 * math.log(ROPE_THETA) / HEAD))
        angles = positions.reshape(-1, 1).astype(F32) * inv_freq
        cos_t, sin_t = jnp.cos(angles), jnp.sin(angles)
        cs = jnp.concatenate([cos_t, cos_t, -sin_t, sin_t], axis=1)
        dy = dy_out.reshape(-1, D)

        local_ids = all_ids - lax.axis_index(AXIS_NAME) * rows_local
        is_owner = (local_ids >= 0) & (local_ids < rows_local)
        safe_ids = jnp.clip(local_ids, 0, rows_local - 1)
        targets = jnp.where(is_owner, local_ids, rows_local)
        xs = []
        start = 0
        for size in CHUNKS:
            ids = safe_ids[:, start:start + size].reshape(-1)
            own = is_owner[:, start:start + size].reshape(-1)
            picked = jnp.where(own[:, None], jnp.take(table_shard, ids, axis=0), jnp.zeros((), BF))
            xs.append(lax.psum_scatter(picked, AXIS_NAME, scatter_dimension=0, tiled=True))
            start += size
        carry = None
        start = 0
        all_rows, all_targets = [], []
        for idx, size in enumerate(CHUNKS):
            x_chunk = xs[idx]
            if idx >= 2:
                x_chunk, all_rows[idx - 2] = lax.optimization_barrier((x_chunk, all_rows[idx - 2]))
            dx, carry = layer_chunk(x_chunk, dy, cs, w_pack, w_down_full, gains, head_gains, start, carry, idx == len(CHUNKS) - 1, batch_len * seq_len)
            all_rows.append(lax.all_gather(dx, AXIS_NAME, tiled=True))
            all_targets.append(targets[:, start:start + size].reshape(-1))
            start += size
        acc, d_w_down, y = carry
        d_table = jax.ops.segment_sum(jnp.concatenate(all_rows, axis=0), jnp.concatenate(all_targets), num_segments=rows_local)
        g_pack = lax.optimization_barrier(lax.psum_scatter(acc, AXIS_NAME, scatter_dimension=0, tiled=True))
        d_w_down = lax.psum_scatter(d_w_down, AXIS_NAME, scatter_dimension=0, tiled=True)
        kv_cols = w_key.shape[1]
        return (y.reshape(batch_len, seq_len, D), d_table, g_pack[:, C_NORM], g_pack[:, :D], g_pack[:, D:D + kv_cols], g_pack[:, D + kv_cols:D + 2 * kv_cols],
                g_pack[0, C_HEAD:C_HEAD + HEAD], g_pack[0, C_HEAD + HEAD:C_HEAD + 2 * HEAD], g_pack[:, C_OUT:C_OUT + D], g_pack[:, C_NORM + 1],
                g_pack[:, C_GATE:C_GATE + FF], g_pack[:, C_UP:C_UP + FF], d_w_down)

    return jax.shard_map(device_step, mesh=mesh, in_specs=(row_spec, row_spec, row_spec) + weight_specs + (batch_spec,), out_specs=(batch_spec, row_spec) + weight_specs, check_vma=False)
```

```python
import functools
import math
import jax
import jax.numpy as jnp
from jax import lax
from jax.experimental import pallas as pl
from jax.experimental.pallas import tpu as pltpu
from jax.sharding import PartitionSpec as P

NORM_EPS = 1e-6
ROPE_THETA = 1.0e6
AXIS_NAME = 'fsdp'
SEQ = 256
D = 576
FF = 1536
HEAD = 64
HEADS = 9
KV = 3
GRP = 3
C_OUT, C_GATE, C_UP, C_NORM, C_HEAD = 1024, 1664, 3200, 4736, 4864
W_COLS, G_COLS = 4864, 4992
X_K, X_V, X_COLS = HEADS * 128, (HEADS + KV) * 128, (HEADS + 2 * KV) * 128
FF_STEP = 512
CHUNKS = (4, 4, 4)
BF, F32 = jnp.bfloat16, jnp.float32


def mm(lhs, rhs, lhs_dim=1, rhs_dim=0):
    return lax.dot_general(lhs, rhs, (((lhs_dim,), (rhs_dim,)), ((), ())), preferred_element_type=F32)


def fold8(values):
    return jnp.sum(values.reshape(values.shape[0] // 8, 8, values.shape[1]), axis=0)


def norm_bwd(grad_out, normed, inv_rms, norm_gain):
    grad_normed = grad_out * norm_gain
    return inv_rms * (grad_normed - normed * jnp.mean(grad_normed * normed, axis=-1, keepdims=True))


def head_norm_rope(head_ext, gain_ext, cs):
    head_f = head_ext.astype(F32)
    inv = lax.rsqrt(jnp.sum(head_f * head_f, axis=-1, keepdims=True) * (1.0 / 128) + NORM_EPS)
    turned = head_f * inv * gain_ext * cs
    return turned + pltpu.roll(turned, 64, 1), inv


def head_norm_rope_bwd(grad_ext, head_ext, inv, gain_low, cs_bwd, low):
    turned = grad_ext * cs_bwd
    grad_t = turned + pltpu.roll(turned, 64, 1)
    normed = jnp.where(low, head_ext.astype(F32), 0.0) * inv
    grad_normed = grad_t * gain_low
    mean_term = jnp.sum(grad_normed * normed, axis=-1, keepdims=True) * (1.0 / HEAD)
    return inv * (grad_normed - normed * mean_term), fold8(grad_t * normed)


def pack_pairs(heads):
    tiles = []
    for idx in range(0, len(heads), 2):
        tile = heads[idx]
        if idx + 1 < len(heads):
            tile = tile + pltpu.roll(heads[idx + 1], 64, 1)
        tiles.append(tile.astype(BF))
    return tiles


def layer_kernel(first, last, steps, *refs):
    (x_ref, dy_ref, cs_ref, w_ref, wd_ref, gains_ref, head_gains_ref) = refs[:7]
    refs = refs[7:]
    if not first:
        acc_in, accd_in, _ = refs[:3]
        refs = refs[3:]
    (y_ref, dx_ref, acc_out, accd_out) = refs[:4]
    (acc, accd, norm_acc, head_acc, wx, wox, qkv_s, probs_s, tbuf, sems) = refs[4:]
    step = pl.program_id(0)
    low = lax.broadcasted_iota(jnp.int32, (1, 128), 1) < 64

    @pl.when(step == 0)
    def _():
        if first:
            acc[...] = jnp.zeros_like(acc)
            accd[...] = jnp.zeros_like(accd)
        else:
            load_acc = pltpu.make_async_copy(acc_in, acc, sems.at[0])
            load_accd = pltpu.make_async_copy(accd_in, accd, sems.at[1])
            load_acc.start()
            load_accd.start()
        norm_acc[...] = jnp.zeros_like(norm_acc)
        head_acc[...] = jnp.zeros_like(head_acc)
        for h in range(HEADS + 2 * KV):
            tile = w_ref[:, (h // 2) * 128:(h // 2) * 128 + 128].astype(F32)
            moved = pltpu.roll(tile, 64, 1)
            if h >= HEADS + KV:
                both = jnp.where(low, moved if h % 2 else tile, 0.0)
            else:
                twice = jnp.where(low, moved, tile) if h % 2 else jnp.where(low, tile, moved)
                both = jnp.where(low, twice, pltpu.roll(twice, 32, 1))
            wx[:, h * 128:h * 128 + 128] = both.astype(BF)
        for h in range(HEADS):
            wox[h * 128:h * 128 + 64, :] = w_ref[h * 64:h * 64 + 64, C_OUT:C_OUT + D]
            wox[h * 128 + 64:h * 128 + 128, :] = jnp.zeros((64, D), BF)
        if not first:
            load_acc.wait()
            load_accd.wait()

    gain1 = gains_ref[0:1, :]
    gain2 = gains_ref[1:2, :]
    gain_q, gain_k = head_gains_ref[0:1, :], head_gains_ref[1:2, :]
    low_q, low_k = jnp.where(low, gain_q, 0.0), jnp.where(low, gain_k, 0.0)
    cs = cs_ref[...]
    cs_bwd = jnp.where(low, cs, -cs)
    causal = ((lax.broadcasted_iota(jnp.int32, (GRP * SEQ, SEQ), 0) & (SEQ - 1))
              >= lax.broadcasted_iota(jnp.int32, (GRP * SEQ, SEQ), 1))

    x = x_ref[...].astype(F32)
    inv1 = lax.rsqrt(jnp.mean(x * x, axis=-1, keepdims=True) + NORM_EPS)
    m1 = (x * inv1 * gain1).astype(BF)
    qkv_s[...] = mm(m1, wx[...]).astype(BF)
    saved = []
    heads = []
    for g in range(KV):
        ke = qkv_s[:, X_K + g * 128:X_K + g * 128 + 128]
        v0 = qkv_s[:, X_V + g * 128:X_V + g * 128 + 128]
        k_rot, k_inv = head_norm_rope(ke, gain_k, cs)
        k0 = jnp.where(low, k_rot, 0.0).astype(BF)
        k_swap = jnp.where(low, k_rot, pltpu.roll(k_rot, 32, 1)).astype(BF)
        qs, q_swaps, q_invs = [], [], []
        for r in range(GRP):
            h = g * GRP + r
            q_rot, q_inv = head_norm_rope(qkv_s[:, h * 128:h * 128 + 128], gain_q, cs)
            qs.append(q_rot.astype(BF))
            q_swaps.append(jnp.where(low, q_rot, pltpu.roll(q_rot, 32, 1)).astype(BF))
            q_invs.append(q_inv)
        scores = mm(jnp.concatenate(qs, axis=0), k0, 1, 1) * (HEAD ** -0.5)
        scores = jnp.where(causal, scores, -1e30)
        expd = jnp.exp(scores - jnp.max(scores, axis=-1, keepdims=True))
        probs = expd / jnp.sum(expd, axis=-1, keepdims=True)
        probs_s[g] = probs
        o = mm(probs.astype(BF), v0)
        for r in range(GRP):
            heads.append(o[r * SEQ:(r + 1) * SEQ])
        saved.append((k_swap, jnp.concatenate(q_swaps, axis=0), q_invs, k_inv))
    attn = jnp.concatenate(pack_pairs(heads), axis=1)
    hidden_b = (x + mm(attn[:, :D], w_ref[:, C_OUT:C_OUT + D])).astype(BF)
    hidden = hidden_b.astype(F32)
    inv2 = lax.rsqrt(jnp.mean(hidden * hidden, axis=-1, keepdims=True) + NORM_EPS)
    m2 = (hidden * inv2 * gain2).astype(BF)

    dy = dy_ref[...]
    m2_t = m2.T
    dy_t = dy.T
    y = hidden
    dm2 = jnp.zeros((SEQ, D), F32)
    for f in range(0, FF, FF_STEP):
        wg = w_ref[:, C_GATE + f:C_GATE + f + FF_STEP]
        wu = w_ref[:, C_UP + f:C_UP + f + FF_STEP]
        wd = wd_ref[f:f + FF_STEP, :]
        gate = mm(m2, wg)
        up = mm(m2, wu)
        dact = mm(dy, wd, 1, 1)
        sig = 1.0 / (1.0 + jnp.exp(-gate))
        silu = gate * sig
        act = (silu * up).astype(BF)
        y = y + mm(act, wd)
        dgate = (dact * up * sig * (1.0 + gate * (1.0 - sig))).astype(BF)
        dup = (dact * silu).astype(BF)
        dm2 = dm2 + mm(dgate, wg, 1, 1) + mm(dup, wu, 1, 1)
        acc[:, C_GATE + f:C_GATE + f + FF_STEP] += mm(m2_t, dgate)
        acc[:, C_UP + f:C_UP + f + FF_STEP] += mm(m2_t, dup)
        accd[:, f:f + FF_STEP] += mm(dy_t, act)
    y_ref[...] = y.astype(BF)
    n2 = hidden * inv2
    norm_acc[1] += fold8(dm2 * n2)
    dh = dy.astype(F32) + norm_bwd(dm2, n2, inv2, gain2)
    dh_b = dh.astype(BF)
    acc[:, C_OUT:C_OUT + D] += mm(attn.T, dh_b)[:D]

    do = mm(dh_b, wox[...], 1, 1).astype(BF)
    dqs, dks, dvs = [], [], []
    for g in range(KV):
        k_swap, q_swap, q_invs, k_inv = saved[g]
        v0 = qkv_s[:, X_V + g * 128:X_V + g * 128 + 128]
        do_g = jnp.concatenate([do[:, h * 128:h * 128 + 128] for h in range(g * GRP, (g + 1) * GRP)], axis=0)
        probs = probs_s[g]
        dprobs = mm(do_g, v0, 1, 1)
        dvs.append(mm(do_g.T, probs.astype(BF)).T)
        dscores = probs * (dprobs - jnp.sum(dprobs * probs, axis=-1, keepdims=True)) * (HEAD ** -0.5)
        dscores = dscores.astype(BF)
        dq = mm(dscores, k_swap)
        dk = mm(q_swap.T, dscores).T
        dk, dk_gain = head_norm_rope_bwd(dk, qkv_s[:, X_K + g * 128:X_K + g * 128 + 128], k_inv, low_k, cs_bwd, low)
        dks.append(dk)
        head_acc[1] += dk_gain
        for r in range(GRP):
            h = g * GRP + r
            dq_h, dq_gain = head_norm_rope_bwd(dq[r * SEQ:(r + 1) * SEQ], qkv_s[:, h * 128:h * 128 + 128], q_invs[r], low_q, cs_bwd, low)
            dqs.append(dq_h)
            head_acc[0] += dq_gain
    dqkv = jnp.concatenate(pack_pairs(dqs + dks + dvs), axis=1)
    acc[:, 0:1024] += mm(m1.T, dqkv)
    dm1 = mm(dqkv, w_ref[:, 0:1024], 1, 1)
    n1 = x * inv1
    norm_acc[0] += fold8(dm1 * n1)
    dx = jnp.concatenate([dh + norm_bwd(dm1, n1, inv1, gain1), jnp.zeros((SEQ, 64), F32)], axis=1)
    for j in range(5):
        dx_ref[pl.ds(j, SEQ, stride=5), :] = dx[:, j * 128:j * 128 + 128]

    @pl.when(step == steps - 1)
    def _():
        top = lax.broadcasted_iota(jnp.int32, (128, 1), 0)
        rows1 = jnp.sum(norm_acc[0], axis=0, keepdims=True)
        rows2 = jnp.sum(norm_acc[1], axis=0, keepdims=True)
        both = jnp.where(top == 0, rows1, 0.0) + jnp.where(top == 1, rows2, 0.0)
        for c in range(0, D, 128):
            width = min(128, D - c)
            acc[c:c + width, C_NORM:C_NORM + 128] += both[:, c:c + width].T
        head_q = jnp.sum(head_acc[0], axis=0, keepdims=True)
        head_k = jnp.sum(head_acc[1], axis=0, keepdims=True)
        head_row = jnp.where(low, head_q, pltpu.roll(head_k, 64, 1))
        acc[:, C_HEAD:C_HEAD + 128] += jnp.broadcast_to(head_row, (D, 128))
        store_acc = pltpu.make_async_copy(acc, acc_out, sems.at[0])
        store_acc.start()
        if last:
            for f in range(0, FF, 512):
                for s in range(0, D, 64):
                    tbuf[:, s:s + 64] = accd[s:s + 64, f:f + 512].T
                store = pltpu.make_async_copy(tbuf, accd_out.at[pl.ds(f, 512), :], sems.at[1])
                store.start()
                store.wait()
        else:
            store_accd = pltpu.make_async_copy(accd, accd_out, sems.at[1])
            store_accd.start()
            store_accd.wait()
        store_acc.wait()


ROW_WORDS = 5
GROUP_ROWS = 16
PAD_ROWS = 16


def gather_kernel(blocks, ids_ref, tab_ref, *refs):
    outs, (lin, buf) = refs[:-2], refs[-2:]
    step = pl.program_id(0)
    rows = tab_ref.shape[1]

    @pl.when(step == 0)
    def _():
        def build(b, _):
            at = pl.multiple_of(b * 128, 128)
            for j in range(ROW_WORDS):
                part = tab_ref[j * 128:min(j * 128 + 128, D), pl.ds(at, 128)].astype(F32)
                if part.shape[0] < 128:
                    part = jnp.concatenate([part, jnp.zeros((128 - part.shape[0], 128), F32)], axis=0)
                lin[pl.ds(at * ROW_WORDS + j, 128, stride=ROW_WORDS), :] = part.T
            return 0

        lax.fori_loop(0, rows // 128, build, 0)
        lin[rows * ROW_WORDS:(rows + PAD_ROWS) * ROW_WORDS, :] = jnp.zeros((PAD_ROWS * ROW_WORDS, 128), F32)

    def pick(k, _):
        base = k * GROUP_ROWS
        got = [lin[pl.ds(ids_ref[step * SEQ + base + u], ROW_WORDS), :] for u in range(GROUP_ROWS)]
        for u in range(GROUP_ROWS):
            buf[pl.ds((base + u) * ROW_WORDS, ROW_WORDS), :] = got[u]
        return 0

    lax.fori_loop(0, SEQ // GROUP_ROWS, pick, 0)
    first = 0
    for out, count in zip(outs, blocks):
        @pl.when((step >= first) & (step < first + count))
        def _():
            for j in range(ROW_WORDS):
                width = min(128, D - j * 128)
                out[:, j * 128:j * 128 + width] = buf[pl.ds(j, SEQ, stride=ROW_WORDS), :][:, :width].astype(BF)

        first += count


def gather_rows(ids, table_t, blocks):
    starts = [sum(blocks[:c]) for c in range(len(blocks))]
    rows = table_t.shape[1]
    out_spec = lambda c: pl.BlockSpec((SEQ, D), lambda i, ids: (jnp.clip(i - starts[c], 0, blocks[c] - 1), 0))
    return pl.pallas_call(
        functools.partial(gather_kernel, blocks),
        grid_spec=pltpu.PrefetchScalarGridSpec(
            num_scalar_prefetch=1,
            grid=(sum(blocks),),
            in_specs=[pl.BlockSpec(table_t.shape, lambda i, ids: (0, 0), pipeline_mode=pl.Buffered(1))],
            out_specs=[out_spec(c) for c in range(len(blocks))],
            scratch_shapes=[pltpu.VMEM(((rows + PAD_ROWS) * ROW_WORDS, 128), F32), pltpu.VMEM((SEQ * ROW_WORDS, 128), F32)],
        ),
        out_shape=[jax.ShapeDtypeStruct((count * SEQ, D), BF) for count in blocks],
        compiler_params=pltpu.CompilerParams(dimension_semantics=('arbitrary',), vmem_limit_bytes=48 << 20),
        cost_estimate=pl.CostEstimate(flops=40_000_000_000, bytes_accessed=40_000_000, transcendentals=0),
        name='gather_rows',
    )(ids, table_t)


def scatter_kernel(first, last, blocks, ids_ref, clash_ref, rows_ref, *refs):
    if not first:
        acc_in, refs = refs[0], refs[1:]
    out_ref, acc, sem = refs[:3]
    tbuf = refs[3] if last else None
    step = pl.program_id(0)
    rows = acc.shape[0] // ROW_WORDS - PAD_ROWS

    @pl.when(step == 0)
    def _():
        if first:
            acc[...] = jnp.zeros_like(acc)
        else:
            load = pltpu.make_async_copy(acc_in, acc, sem)
            load.start()
            load.wait()

    groups = SCATTER_ROWS // GROUP_ROWS

    def add(k, _):
        base = k * GROUP_ROWS
        spots = [pl.ds(ids_ref[step * SCATTER_ROWS + base + u], ROW_WORDS) for u in range(GROUP_ROWS)]
        from_row = lambda u: rows_ref[pl.ds((base + u) * ROW_WORDS, ROW_WORDS), :]
        clash = clash_ref[step * groups + k]

        @pl.when(clash == 0)
        def _():
            sums = [acc[spots[u], :] + from_row(u) for u in range(GROUP_ROWS)]
            for u in range(GROUP_ROWS):
                acc[spots[u], :] = sums[u]

        @pl.when(clash != 0)
        def _():
            for u in range(GROUP_ROWS):
                acc[spots[u], :] += from_row(u)

        return 0

    lax.fori_loop(0, groups, add, 0)

    @pl.when(step == blocks - 1)
    def _():
        if last:
            def flush(b, _):
                slot = lax.rem(b, 2)
                at = pl.multiple_of(b * 128, 128)
                store = pltpu.make_async_copy(tbuf.at[slot], out_ref.at[:, pl.ds(at, 128)], sem)

                @pl.when(b >= 1)
                def _():
                    store.wait()

                for j in range(ROW_WORDS):
                    width = min(128, D - j * 128)
                    part = acc[pl.ds(at * ROW_WORDS + j, 128, stride=ROW_WORDS), :].T
                    tbuf[slot, j * 128:j * 128 + width, :] = part[:width]
                store.start()
                return 0

            lax.fori_loop(0, rows // 128, flush, 0)
            pltpu.make_async_copy(tbuf.at[0], out_ref.at[:, pl.ds(0, 128)], sem).wait()
        else:
            store = pltpu.make_async_copy(acc, out_ref, sem)
            store.start()
            store.wait()


SCATTER_ROWS = 512


def scatter_rows(ids, clash, rows_in, table_rows, carry, last):
    first = carry is None
    blocks = rows_in.shape[0] // (SCATTER_ROWS * ROW_WORDS)
    acc_shape = ((table_rows + PAD_ROWS) * ROW_WORDS, 128)
    anyspec = pl.BlockSpec(memory_space=pl.ANY)
    scratch = [pltpu.VMEM(acc_shape, F32), pltpu.SemaphoreType.DMA]
    if last:
        scratch.append(pltpu.VMEM((2, D, 128), F32))
    return pl.pallas_call(
        functools.partial(scatter_kernel, first, last, blocks),
        grid_spec=pltpu.PrefetchScalarGridSpec(
            num_scalar_prefetch=2,
            grid=(blocks,),
            in_specs=[pl.BlockSpec((SCATTER_ROWS * ROW_WORDS, 128), lambda i, *_: (i, 0))] + ([] if first else [anyspec]),
            out_specs=anyspec,
            scratch_shapes=scratch,
        ),
        out_shape=jax.ShapeDtypeStruct((D, table_rows) if last else acc_shape, F32),
        input_output_aliases={} if first or last else {3: 0},
        compiler_params=pltpu.CompilerParams(dimension_semantics=('arbitrary',), vmem_limit_bytes=40 << 20),
        cost_estimate=pl.CostEstimate(flops=20_000_000_000, bytes_accessed=60_000_000, transcendentals=0),
        name='scatter_rows',
    )(*([ids, clash, rows_in] + ([] if first else [carry])))


def layer_chunk(x, dy, cs, w_pack, w_down, gains, head_gains, start, carry, last, total):
    steps = x.shape[0] // SEQ
    first = carry is None
    whole = lambda shape: pl.BlockSpec(shape, lambda i: (0,) * len(shape), pipeline_mode=pl.Buffered(1))
    here = lambda cols: pl.BlockSpec((SEQ, cols), lambda i: (i + start, 0))
    anyspec = pl.BlockSpec(memory_space=pl.ANY)
    in_specs = [pl.BlockSpec((SEQ, D), lambda i: (i, 0)), here(D), here(128), whole(w_pack.shape), whole(w_down.shape), whole(gains.shape), whole(head_gains.shape)]
    args = [x, dy, cs, w_pack, w_down, gains, head_gains]
    aliases = {}
    if not first:
        in_specs += [anyspec] * 3
        args += list(carry)
        aliases = {7: 2, 9: 0} if last else {7: 2, 8: 3, 9: 0}
    out_shape = [
        jax.ShapeDtypeStruct((total, D), BF),
        jax.ShapeDtypeStruct((steps * SEQ * 5, 128), F32),
        jax.ShapeDtypeStruct((D, G_COLS), F32),
        jax.ShapeDtypeStruct((FF, D) if last else (D, FF), F32),
    ]
    y, dx, acc, accd = pl.pallas_call(
        functools.partial(layer_kernel, first, last, steps),
        grid=(steps,),
        in_specs=in_specs,
        out_specs=[here(D), pl.BlockSpec((SEQ * 5, 128), lambda i: (i, 0)), anyspec, anyspec],
        out_shape=out_shape,
        scratch_shapes=[
            pltpu.VMEM((D, G_COLS), F32),
            pltpu.VMEM((D, FF), F32),
            pltpu.VMEM((2, 8, D), F32),
            pltpu.VMEM((2, 8, 128), F32),
            pltpu.VMEM((D, X_COLS), BF),
            pltpu.VMEM((HEADS * 128, D), BF),
            pltpu.VMEM((SEQ, X_COLS), BF),
            pltpu.VMEM((KV, GRP * SEQ, SEQ), F32),
            pltpu.VMEM((512, D), F32),
            pltpu.SemaphoreType.DMA((2,)),
        ],
        input_output_aliases=aliases,
        compiler_params=pltpu.CompilerParams(dimension_semantics=('arbitrary',), vmem_limit_bytes=60 << 20),
        cost_estimate=pl.CostEstimate(flops=steps * 6_000_000_000, bytes_accessed=steps * 2_500_000 + 45_000_000, transcendentals=steps * 1_000_000),
        name='layer_chunk',
    )(*args)
    return dx, (acc, accd, y)


def solution(mesh):
    row_spec = P(AXIS_NAME, None)
    vec_spec = P(AXIS_NAME)
    full_spec = P(None)
    batch_spec = P(AXIS_NAME, None, None)
    weight_specs = (vec_spec, row_spec, row_spec, row_spec, full_spec, full_spec, row_spec, vec_spec, row_spec, row_spec, row_spec)

    def device_step(tokens, positions, table_shard, attn_norm, w_query, w_key, w_value, q_norm, k_norm, w_out, mlp_norm, w_gate, w_up, w_down, dy_out):
        batch_len, seq_len = tokens.shape
        devices = lax.axis_size(AXIS_NAME)
        rows_local = table_shard.shape[0]
        shard = w_query.shape[0]
        all_ids = lax.all_gather(tokens, AXIS_NAME)
        norms = jnp.concatenate([attn_norm[:, None], mlp_norm[:, None], jnp.zeros((shard, W_COLS - C_NORM - 2), BF)], axis=1)
        pad = jnp.zeros((shard, 64), BF)
        packed = jnp.concatenate([w_query, w_key, w_value, pad, w_out, pad, w_gate, w_up, norms], axis=1)
        w_pack = lax.all_gather(packed, AXIS_NAME, tiled=True)
        w_down_full = lax.all_gather(w_down, AXIS_NAME, tiled=True)
        gains = w_pack[:, C_NORM:C_NORM + 2].T.astype(F32)
        head_gains = jnp.stack([q_norm, k_norm]).astype(F32)
        swapped = jnp.concatenate([head_gains[:, 32:], head_gains[:, :32]], axis=1)
        head_gains = jnp.concatenate([head_gains, swapped], axis=1)

        inv_freq = jnp.exp(jnp.arange(HEAD // 2, dtype=F32) * (-2.0 * math.log(ROPE_THETA) / HEAD))
        angles = positions.reshape(-1, 1).astype(F32) * inv_freq
        cos_t, sin_t = jnp.cos(angles), jnp.sin(angles)
        cs = jnp.concatenate([cos_t, cos_t, -sin_t, sin_t], axis=1)
        dy = dy_out.reshape(-1, D)

        local_ids = all_ids - lax.axis_index(AXIS_NAME) * rows_local
        is_owner = (local_ids >= 0) & (local_ids < rows_local)
        starts = [sum(CHUNKS[:c]) for c in range(len(CHUNKS))]
        by_chunk = lambda values: [values[:, s:s + n].reshape(-1) for s, n in zip(starts, CHUNKS)]
        take_from = by_chunk(jnp.where(is_owner, local_ids, rows_local) * ROW_WORDS)
        spare = lax.broadcasted_iota(jnp.int32, all_ids.shape, 2) % GROUP_ROWS + rows_local
        add_to = jnp.where(is_owner, local_ids, spare)
        grouped = add_to.reshape(all_ids.shape[:2] + (seq_len // GROUP_ROWS, GROUP_ROWS))
        pairs = (grouped[..., :, None] == grouped[..., None, :]) & (jnp.arange(GROUP_ROWS)[:, None] > jnp.arange(GROUP_ROWS)[None, :])
        clashes = by_chunk(jnp.any(pairs, axis=(-1, -2)).astype(jnp.int32))
        add_to = by_chunk(add_to * ROW_WORDS)

        picked = gather_rows(jnp.concatenate(take_from), table_shard.T, tuple(devices * n for n in CHUNKS))
        xs = [lax.psum_scatter(rows, AXIS_NAME, scatter_dimension=0, tiled=True) for rows in picked]
        carry = None
        rows_of = []
        for idx in range(len(CHUNKS)):
            x_chunk = xs[idx]
            dx, carry = layer_chunk(x_chunk, dy, cs, w_pack, w_down_full, gains, head_gains, starts[idx], carry, idx == len(CHUNKS) - 1, batch_len * seq_len)
            rows_of.append(lax.all_gather(dx, AXIS_NAME, tiled=True))
        acc, d_w_down, y = carry
        d_table = None
        for idx in range(len(CHUNKS)):
            d_table = scatter_rows(add_to[idx], clashes[idx], rows_of[idx], rows_local, d_table, idx == len(CHUNKS) - 1)
        d_table = d_table.T
        g_pack = lax.optimization_barrier(lax.psum_scatter(acc, AXIS_NAME, scatter_dimension=0, tiled=True))
        d_w_down = lax.psum_scatter(d_w_down, AXIS_NAME, scatter_dimension=0, tiled=True)
        kv_cols = w_key.shape[1]
        return (y.reshape(batch_len, seq_len, D), d_table, g_pack[:, C_NORM], g_pack[:, :D], g_pack[:, D:D + kv_cols], g_pack[:, D + kv_cols:D + 2 * kv_cols],
                g_pack[0, C_HEAD:C_HEAD + HEAD], g_pack[0, C_HEAD + HEAD:C_HEAD + 2 * HEAD], g_pack[:, C_OUT:C_OUT + D], g_pack[:, C_NORM + 1],
                g_pack[:, C_GATE:C_GATE + FF], g_pack[:, C_UP:C_UP + FF], d_w_down)

    return jax.shard_map(device_step, mesh=mesh, in_specs=(row_spec, row_spec, row_spec) + weight_specs + (batch_spec,), out_specs=(batch_spec, row_spec) + weight_specs, check_vma=False)
```

```python
import functools
import math
import jax
import jax.numpy as jnp
from jax import lax
from jax.experimental import pallas as pl
from jax.experimental.pallas import tpu as pltpu
from jax.sharding import PartitionSpec as P

NORM_EPS = 1e-6
ROPE_THETA = 1.0e6
AXIS_NAME = 'fsdp'
SEQ = 256
HALF_SEQ = SEQ // 2
LANES = 128
D = 576
FF = 1536
HEAD = 64
HEADS = 9
KV = 3
GRP = 3
C_OUT, C_GATE, C_UP, C_NORM, C_HEAD = 1024, 1664, 3200, 4736, 4864
W_COLS, G_COLS = 4864, 4992
X_K, X_V, X_COLS = HEADS * LANES, (HEADS + KV) * LANES, (HEADS + 2 * KV) * LANES
FF_STEP = 512
CHUNKS = (4, 4, 4)
PAIR_WORDS = 9
BF, F32 = jnp.bfloat16, jnp.float32


def mm(lhs, rhs, lhs_dim=1, rhs_dim=0):
    return lax.dot_general(lhs, rhs, (((lhs_dim,), (rhs_dim,)), ((), ())), preferred_element_type=F32)


def fold8(values):
    return jnp.sum(values.reshape(values.shape[0] // 8, 8, values.shape[1]), axis=0)


def norm_bwd(grad_out, normed, inv_rms, norm_gain):
    grad_normed = grad_out * norm_gain
    return inv_rms * (grad_normed - normed * jnp.mean(grad_normed * normed, axis=-1, keepdims=True))


def head_norm_rope(head_ext, gain_ext, cs):
    head_f = head_ext.astype(F32)
    inv = lax.rsqrt(jnp.sum(head_f * head_f, axis=-1, keepdims=True) * (1.0 / LANES) + NORM_EPS)
    turned = head_f * inv * gain_ext * cs
    return turned + pltpu.roll(turned, 64, 1), inv


def head_norm_rope_bwd(grad_ext, head_ext, inv, gain_low, cs_bwd, low):
    turned = grad_ext * cs_bwd
    grad_t = turned + pltpu.roll(turned, 64, 1)
    normed = jnp.where(low, head_ext.astype(F32), 0.0) * inv
    grad_normed = grad_t * gain_low
    mean_term = jnp.sum(grad_normed * normed, axis=-1, keepdims=True) * (1.0 / HEAD)
    return inv * (grad_normed - normed * mean_term), fold8(grad_t * normed)


def pack_pairs(heads):
    tiles = []
    for idx in range(0, len(heads), 2):
        tile = heads[idx]
        if idx + 1 < len(heads):
            tile = tile + pltpu.roll(heads[idx + 1], 64, 1)
        tiles.append(tile.astype(BF))
    return tiles


def layer_kernel(first, last, steps, *refs):
    (x_ref, dy_ref, cs_ref, w_ref, wd_ref, gains_ref, head_gains_ref, core_ref) = refs[:8]
    refs = refs[8:]
    if not first:
        acc_in, accd_in, _ = refs[:3]
        refs = refs[3:]
    y_ref, dx_ref = refs[:2]
    outs = refs[2:6] if last else refs[2:4]
    (acc, accd, norm_acc, head_acc, wx, wox, qkv_s, probs_s, tbuf, sems) = refs[2 + len(outs):]
    step = pl.program_id(0)
    low = lax.broadcasted_iota(jnp.int32, (1, LANES), 1) < 64

    @pl.when(step == 0)
    def _():
        if first:
            acc[...] = jnp.zeros_like(acc)
            accd[...] = jnp.zeros_like(accd)
        else:
            load_acc = pltpu.make_async_copy(acc_in, acc, sems.at[0])
            load_accd = pltpu.make_async_copy(accd_in, accd, sems.at[1])
            load_acc.start()
            load_accd.start()
        norm_acc[...] = jnp.zeros_like(norm_acc)
        head_acc[...] = jnp.zeros_like(head_acc)
        for h in range(HEADS + 2 * KV):
            tile = w_ref[:, (h // 2) * LANES:(h // 2) * LANES + LANES].astype(F32)
            moved = pltpu.roll(tile, 64, 1)
            if h >= HEADS + KV:
                both = jnp.where(low, moved if h % 2 else tile, 0.0)
            else:
                twice = jnp.where(low, moved, tile) if h % 2 else jnp.where(low, tile, moved)
                both = jnp.where(low, twice, pltpu.roll(twice, 32, 1))
            wx[:, h * LANES:h * LANES + LANES] = both.astype(BF)
        for h in range(HEADS):
            wox[h * LANES:h * LANES + 64, :] = w_ref[h * 64:h * 64 + 64, C_OUT:C_OUT + D]
            wox[h * LANES + 64:h * LANES + LANES, :] = jnp.zeros((64, D), BF)
        if not first:
            load_acc.wait()
            load_accd.wait()

    gain1 = gains_ref[0:1, :]
    gain2 = gains_ref[1:2, :]
    gain_q, gain_k = head_gains_ref[0:1, :], head_gains_ref[1:2, :]
    low_q, low_k = jnp.where(low, gain_q, 0.0), jnp.where(low, gain_k, 0.0)
    cs = cs_ref[...]
    cs_bwd = jnp.where(low, cs, -cs)
    causal = ((lax.broadcasted_iota(jnp.int32, (GRP * SEQ, SEQ), 0) & (SEQ - 1))
              >= lax.broadcasted_iota(jnp.int32, (GRP * SEQ, SEQ), 1))

    pairs = x_ref[...].astype(F32)
    tails = pairs[:, 512:640]
    x = jnp.concatenate([
        jnp.concatenate([pairs[:, :512], tails[:, :64]], axis=1),
        jnp.concatenate([pairs[:, 640:], pltpu.roll(tails, 64, 1)[:, :64]], axis=1)], axis=0)
    inv1 = lax.rsqrt(jnp.mean(x * x, axis=-1, keepdims=True) + NORM_EPS)
    m1 = (x * inv1 * gain1).astype(BF)
    qkv_s[...] = mm(m1, wx[...]).astype(BF)
    saved = []
    heads = []
    for g in range(KV):
        ke = qkv_s[:, X_K + g * LANES:X_K + g * LANES + LANES]
        v0 = qkv_s[:, X_V + g * LANES:X_V + g * LANES + LANES]
        k_rot, k_inv = head_norm_rope(ke, gain_k, cs)
        k0 = jnp.where(low, k_rot, 0.0).astype(BF)
        k_swap = jnp.where(low, k_rot, pltpu.roll(k_rot, 32, 1)).astype(BF)
        qs, q_swaps, q_invs = [], [], []
        for r in range(GRP):
            h = g * GRP + r
            q_rot, q_inv = head_norm_rope(qkv_s[:, h * LANES:h * LANES + LANES], gain_q, cs)
            qs.append(q_rot.astype(BF))
            q_swaps.append(jnp.where(low, q_rot, pltpu.roll(q_rot, 32, 1)).astype(BF))
            q_invs.append(q_inv)
        scores = mm(jnp.concatenate(qs, axis=0), k0, 1, 1) * (HEAD ** -0.5)
        scores = jnp.where(causal, scores, -1e30)
        expd = jnp.exp(scores - jnp.max(scores, axis=-1, keepdims=True))
        probs = expd / jnp.sum(expd, axis=-1, keepdims=True)
        probs_s[g] = probs
        o = mm(probs.astype(BF), v0)
        for r in range(GRP):
            heads.append(o[r * SEQ:(r + 1) * SEQ])
        saved.append((k_swap, jnp.concatenate(q_swaps, axis=0), q_invs, k_inv))
    attn = jnp.concatenate(pack_pairs(heads), axis=1)
    hidden_b = (x + mm(attn[:, :D], w_ref[:, C_OUT:C_OUT + D])).astype(BF)
    hidden = hidden_b.astype(F32)
    inv2 = lax.rsqrt(jnp.mean(hidden * hidden, axis=-1, keepdims=True) + NORM_EPS)
    m2 = (hidden * inv2 * gain2).astype(BF)

    dy = dy_ref[...]
    m2_t = m2.T
    dy_t = dy.T
    y = hidden
    dm2 = jnp.zeros((SEQ, D), F32)
    for f in range(0, FF, FF_STEP):
        wg = w_ref[:, C_GATE + f:C_GATE + f + FF_STEP]
        wu = w_ref[:, C_UP + f:C_UP + f + FF_STEP]
        wd = wd_ref[f:f + FF_STEP, :]
        gate = mm(m2, wg)
        up = mm(m2, wu)
        dact = mm(dy, wd, 1, 1)
        sig = 1.0 / (1.0 + jnp.exp(-gate))
        silu = gate * sig
        act = (silu * up).astype(BF)
        y = y + mm(act, wd)
        dgate = (dact * up * sig * (1.0 + gate * (1.0 - sig))).astype(BF)
        dup = (dact * silu).astype(BF)
        dm2 = dm2 + mm(dgate, wg, 1, 1) + mm(dup, wu, 1, 1)
        acc[:, C_GATE + f:C_GATE + f + FF_STEP] += mm(m2_t, dgate)
        acc[:, C_UP + f:C_UP + f + FF_STEP] += mm(m2_t, dup)
        accd[:, f:f + FF_STEP] += mm(dy_t, act)
    y_ref[...] = y.astype(BF)
    n2 = hidden * inv2
    norm_acc[1] += fold8(dm2 * n2)
    dh = dy.astype(F32) + norm_bwd(dm2, n2, inv2, gain2)
    dh_b = dh.astype(BF)
    acc[:, C_OUT:C_OUT + D] += mm(attn.T, dh_b)[:D]

    do = mm(dh_b, wox[...], 1, 1).astype(BF)
    dqs, dks, dvs = [], [], []
    for g in range(KV):
        k_swap, q_swap, q_invs, k_inv = saved[g]
        v0 = qkv_s[:, X_V + g * LANES:X_V + g * LANES + LANES]
        do_g = jnp.concatenate([do[:, h * LANES:h * LANES + LANES] for h in range(g * GRP, (g + 1) * GRP)], axis=0)
        probs = probs_s[g]
        dprobs = mm(do_g, v0, 1, 1)
        dvs.append(mm(do_g.T, probs.astype(BF)).T)
        dscores = probs * (dprobs - jnp.sum(dprobs * probs, axis=-1, keepdims=True)) * (HEAD ** -0.5)
        dscores = dscores.astype(BF)
        dq = mm(dscores, k_swap)
        dk = mm(q_swap.T, dscores).T
        dk, dk_gain = head_norm_rope_bwd(dk, qkv_s[:, X_K + g * LANES:X_K + g * LANES + LANES], k_inv, low_k, cs_bwd, low)
        dks.append(dk)
        head_acc[1] += dk_gain
        for r in range(GRP):
            h = g * GRP + r
            dq_h, dq_gain = head_norm_rope_bwd(dq[r * SEQ:(r + 1) * SEQ], qkv_s[:, h * LANES:h * LANES + LANES], q_invs[r], low_q, cs_bwd, low)
            dqs.append(dq_h)
            head_acc[0] += dq_gain
    dqkv = jnp.concatenate(pack_pairs(dqs + dks + dvs), axis=1)
    acc[:, 0:1024] += mm(m1.T, dqkv)
    dm1 = mm(dqkv, w_ref[:, 0:1024], 1, 1)
    n1 = x * inv1
    norm_acc[0] += fold8(dm1 * n1)
    dx = dh + norm_bwd(dm1, n1, inv1, gain1)
    upper, lower = dx[:HALF_SEQ], dx[HALF_SEQ:]
    for j in range(4):
        dx_ref[pl.ds(j, HALF_SEQ, stride=PAIR_WORDS), :] = upper[:, j * LANES:j * LANES + LANES]
        dx_ref[pl.ds(5 + j, HALF_SEQ, stride=PAIR_WORDS), :] = lower[:, j * LANES:j * LANES + LANES]
    dx_ref[pl.ds(4, HALF_SEQ, stride=PAIR_WORDS), :] = jnp.concatenate([upper[:, 512:], lower[:, 512:]], axis=1)

    @pl.when(step == steps - 1)
    def _():
        top = lax.broadcasted_iota(jnp.int32, (LANES, 1), 0)
        rows1 = jnp.sum(norm_acc[0], axis=0, keepdims=True)
        rows2 = jnp.sum(norm_acc[1], axis=0, keepdims=True)
        both = jnp.where(top == 0, rows1, 0.0) + jnp.where(top == 1, rows2, 0.0)
        for c in range(0, D, LANES):
            width = min(LANES, D - c)
            acc[c:c + width, C_NORM:C_NORM + LANES] += both[:, c:c + width].T
        head_q = jnp.sum(head_acc[0], axis=0, keepdims=True)
        head_k = jnp.sum(head_acc[1], axis=0, keepdims=True)
        head_row = jnp.where(low, head_q, pltpu.roll(head_k, 64, 1))
        acc[:, C_HEAD:C_HEAD + LANES] += jnp.broadcast_to(head_row, (D, LANES))
        if last:
            mine = core_ref[0]
            for f in range(0, FF, 192):
                for t in range(0, D, LANES):
                    width = min(LANES, D - t)
                    tbuf[f:f + 192, t:t + width] = accd[t:t + width, f:f + 192].T
            stores = []
            for d in range(8):
                for src, keep, send in ((acc.at[pl.ds(d * 72, 72), :], outs[0], outs[1]), (tbuf.at[pl.ds(d * 192, 192), :], outs[2], outs[3])):
                    stores.append(pltpu.make_async_copy(src, keep.at[d // 2], sems.at[0]))

                    @pl.when(mine == d % 2)
                    def _():
                        stores[-1].start()

                    @pl.when(mine != d % 2)
                    def _():
                        pltpu.make_async_copy(src, send.at[d // 2], sems.at[0]).start()
        else:
            stores = [pltpu.make_async_copy(acc, outs[0], sems.at[0]), pltpu.make_async_copy(accd, outs[1], sems.at[0])]
            for store in stores:
                store.start()
        for store in stores:
            store.wait()


ROW_WORDS = 5
ACC_WORDS = 6
GROUP_ROWS = 16
PAD_ROWS = 16


def gather_kernel(blocks, ids_ref, tab_ref, *refs):
    outs, (lin, buf) = refs[:-2], refs[-2:]
    step = pl.program_id(0)
    rows = tab_ref.shape[1]

    @pl.when(step == 0)
    def _():
        def build(b, _):
            at = pl.multiple_of(b * LANES, LANES)
            for j in range(ROW_WORDS):
                part = tab_ref[j * LANES:min(j * LANES + LANES, D), pl.ds(at, LANES)].astype(F32)
                if part.shape[0] < LANES:
                    part = jnp.concatenate([part, jnp.zeros((LANES - part.shape[0], LANES), F32)], axis=0)
                lin[pl.ds(at * ROW_WORDS + j, LANES, stride=ROW_WORDS), :] = part.T
            return 0

        lax.fori_loop(0, rows // LANES, build, 0)
        lin[rows * ROW_WORDS:(rows + PAD_ROWS) * ROW_WORDS, :] = jnp.zeros((PAD_ROWS * ROW_WORDS, LANES), F32)

    def pick(k, _):
        base = k * GROUP_ROWS
        got = [lin[pl.ds(ids_ref[step * SEQ + base + u], ROW_WORDS), :] for u in range(GROUP_ROWS)]
        for u in range(GROUP_ROWS):
            buf[pl.ds((base + u) * ROW_WORDS, ROW_WORDS), :] = got[u]
        return 0

    lax.fori_loop(0, SEQ // GROUP_ROWS, pick, 0)
    first = 0
    half = HALF_SEQ * ROW_WORDS
    for out, count in zip(outs, blocks):
        @pl.when((step >= first) & (step < first + count))
        def _():
            for j in range(4):
                out[:, j * LANES:j * LANES + LANES] = buf[pl.ds(j, HALF_SEQ, stride=ROW_WORDS), :].astype(BF)
                out[:, 640 + j * LANES:768 + j * LANES] = buf[pl.ds(half + j, HALF_SEQ, stride=ROW_WORDS), :].astype(BF)
            tails = buf[pl.ds(4, HALF_SEQ, stride=ROW_WORDS), :] + pltpu.roll(buf[pl.ds(half + 4, HALF_SEQ, stride=ROW_WORDS), :], 64, 1)
            out[:, 512:640] = tails.astype(BF)

        first += count


def gather_rows(ids, table_t, blocks):
    starts = [sum(blocks[:c]) for c in range(len(blocks))]
    rows = table_t.shape[1]
    out_spec = lambda c: pl.BlockSpec((HALF_SEQ, 2 * D), lambda i, ids: (jnp.clip(i - starts[c], 0, blocks[c] - 1), 0))
    return pl.pallas_call(
        functools.partial(gather_kernel, blocks),
        grid_spec=pltpu.PrefetchScalarGridSpec(
            num_scalar_prefetch=1,
            grid=(sum(blocks),),
            in_specs=[pl.BlockSpec(table_t.shape, lambda i, ids: (0, 0), pipeline_mode=pl.Buffered(1))],
            out_specs=[out_spec(c) for c in range(len(blocks))],
            scratch_shapes=[pltpu.VMEM(((rows + PAD_ROWS) * ROW_WORDS, LANES), F32), pltpu.VMEM((SEQ * ROW_WORDS, LANES), F32)],
        ),
        out_shape=[jax.ShapeDtypeStruct((count * HALF_SEQ, 2 * D), BF) for count in blocks],
        compiler_params=pltpu.CompilerParams(dimension_semantics=('arbitrary',), vmem_limit_bytes=48 << 20),
        cost_estimate=pl.CostEstimate(flops=40_000_000_000, bytes_accessed=40_000_000, transcendentals=0),
        name='gather_rows',
    )(ids, table_t)


def scatter_kernel(first, last, blocks, ids_ref, clash_ref, rows_ref, *refs):
    if not first:
        acc_in, refs = refs[0], refs[1:]
    out_ref, acc, sem = refs[:3]
    tbuf = refs[3] if last else None
    step = pl.program_id(0)
    rows = acc.shape[0] // ACC_WORDS - PAD_ROWS

    @pl.when(step == 0)
    def _():
        if first:
            acc[...] = jnp.zeros_like(acc)
        else:
            load = pltpu.make_async_copy(acc_in, acc, sem.at[0])
            load.start()
            load.wait()

    groups = SCATTER_ROWS // GROUP_ROWS

    def add(k, _):
        spots = [pl.ds(ids_ref[step * SCATTER_ROWS + u * LANES + k], ROW_WORDS) for u in range(GROUP_ROWS)]
        from_row = lambda u: rows_ref[pl.ds((u // 2 * LANES + k) * PAIR_WORDS + (u % 2) * 4, ROW_WORDS), :]
        clash = clash_ref[step * groups + k]

        @pl.when(clash == 0)
        def _():
            sums = [acc[spots[u], :] + from_row(u) for u in range(GROUP_ROWS)]
            for u in range(GROUP_ROWS):
                acc[spots[u], :] = sums[u]

        @pl.when(clash != 0)
        def _():
            for u in range(GROUP_ROWS):
                acc[spots[u], :] += from_row(u)

        return 0

    lax.fori_loop(0, groups, add, 0)

    @pl.when(step == blocks - 1)
    def _():
        if last:
            wide = FLUSH_ROWS

            def flush(b, _):
                slot = lax.rem(b, 2)
                at = pl.multiple_of(b * wide, wide)
                store = pltpu.make_async_copy(tbuf.at[slot], out_ref.at[:, pl.ds(at, wide)], sem.at[slot])

                @pl.when(b >= 2)
                def _():
                    store.wait()

                word = lambda w, r: acc[pl.ds((at + r) * ACC_WORDS + w, LANES, stride=ACC_WORDS), :]
                for r in range(0, wide, LANES):
                    for j in range(4):
                        tbuf[slot, j * LANES:j * LANES + LANES, r:r + LANES] = word(1 + j, r).T
                    tail = word(5, r) + pltpu.roll(word(0, r), 64, 1)
                    tbuf[slot, 512:D, r:r + LANES] = tail.T[:64]
                store.start()
                return 0

            lax.fori_loop(0, rows // wide, flush, 0)
            for slot in range(2):
                pltpu.make_async_copy(tbuf.at[slot], out_ref.at[:, pl.ds(0, wide)], sem.at[slot]).wait()
        else:
            store = pltpu.make_async_copy(acc, out_ref, sem.at[0])
            store.start()
            store.wait()


SCATTER_ROWS = LANES * GROUP_ROWS
FLUSH_ROWS = 512


def scatter_rows(ids, clash, rows_in, table_rows, carry, last):
    first = carry is None
    blocks = rows_in.shape[0] // (SCATTER_ROWS // 2 * PAIR_WORDS)
    acc_shape = ((table_rows + PAD_ROWS) * ACC_WORDS, LANES)
    anyspec = pl.BlockSpec(memory_space=pl.ANY)
    scratch = [pltpu.VMEM(acc_shape, F32), pltpu.SemaphoreType.DMA((2,))]
    if last:
        scratch.append(pltpu.VMEM((2, D, FLUSH_ROWS), F32))
    return pl.pallas_call(
        functools.partial(scatter_kernel, first, last, blocks),
        grid_spec=pltpu.PrefetchScalarGridSpec(
            num_scalar_prefetch=2,
            grid=(blocks,),
            in_specs=[pl.BlockSpec((SCATTER_ROWS // 2 * PAIR_WORDS, LANES), lambda i, *_: (i, 0))] + ([] if first else [anyspec]),
            out_specs=anyspec,
            scratch_shapes=scratch,
        ),
        out_shape=jax.ShapeDtypeStruct((D, table_rows) if last else acc_shape, F32),
        input_output_aliases={} if first or last else {3: 0},
        compiler_params=pltpu.CompilerParams(dimension_semantics=('arbitrary',), vmem_limit_bytes=48 << 20),
        cost_estimate=pl.CostEstimate(flops=20_000_000_000, bytes_accessed=60_000_000, transcendentals=0),
        name='scatter_rows',
    )(*([ids, clash, rows_in] + ([] if first else [carry])))


def layer_chunk(x, dy, cs, w_pack, w_down, gains, head_gains, core, start, carry, last, total):
    steps = x.shape[0] // (HALF_SEQ)
    first = carry is None
    whole = lambda shape: pl.BlockSpec(shape, lambda i: (0,) * len(shape), pipeline_mode=pl.Buffered(1))
    here = lambda cols: pl.BlockSpec((SEQ, cols), lambda i: (i + start, 0))
    anyspec = pl.BlockSpec(memory_space=pl.ANY)
    in_specs = [pl.BlockSpec((HALF_SEQ, 2 * D), lambda i: (i, 0)), here(D), here(LANES), whole(w_pack.shape), whole(w_down.shape), whole(gains.shape), whole(head_gains.shape), pl.BlockSpec(memory_space=pltpu.SMEM)]
    args = [x, dy, cs, w_pack, w_down, gains, head_gains, core]
    aliases = {}
    if not first:
        in_specs += [anyspec] * 3
        args += list(carry)
        aliases = {10: 0} if last else {8: 2, 9: 3, 10: 0}
    out_shape = [
        jax.ShapeDtypeStruct((total, D), BF),
        jax.ShapeDtypeStruct((steps * HALF_SEQ * PAIR_WORDS, LANES), F32),
    ]
    grad_shapes = [(4, 72, G_COLS)] * 2 + [(4, 192, D)] * 2 if last else [(D, G_COLS), (D, FF)]
    out_shape += [jax.ShapeDtypeStruct(shape, F32) for shape in grad_shapes]
    y, dx, *grads = pl.pallas_call(
        functools.partial(layer_kernel, first, last, steps),
        grid=(steps,),
        in_specs=in_specs,
        out_specs=[here(D), pl.BlockSpec((HALF_SEQ * PAIR_WORDS, LANES), lambda i: (i, 0))] + [anyspec] * len(grad_shapes),
        out_shape=out_shape,
        scratch_shapes=[
            pltpu.VMEM((D, G_COLS), F32),
            pltpu.VMEM((D, FF), F32),
            pltpu.VMEM((2, 8, D), F32),
            pltpu.VMEM((2, 8, LANES), F32),
            pltpu.VMEM((D, X_COLS), BF),
            pltpu.VMEM((HEADS * LANES, D), BF),
            pltpu.VMEM((SEQ, X_COLS), BF),
            pltpu.VMEM((KV, GRP * SEQ, SEQ), F32),
            pltpu.VMEM((FF, D) if last else (8, LANES), F32),
            pltpu.SemaphoreType.DMA((2,)),
        ],
        input_output_aliases=aliases,
        compiler_params=pltpu.CompilerParams(dimension_semantics=('arbitrary',), vmem_limit_bytes=60 << 20),
        cost_estimate=pl.CostEstimate(flops=steps * 6_000_000_000, bytes_accessed=steps * 2_500_000 + 45_000_000, transcendentals=steps * 1_000_000),
        name='layer_chunk',
    )(*args)
    return dx, (*grads, y)


def swap_with(bit, values):
    return lax.ppermute(values, AXIS_NAME, [(i, i ^ bit) for i in range(8)])


def reduce_grads(grads):
    index = lax.axis_index(AXIS_NAME)
    x, y = (index // 2) % 2, index // 4
    parts = [(grads[i], swap_with(1, grads[i + 1])) for i in (0, 2)]
    summed = [(kept + got).reshape(2, 2, *kept.shape[1:]) for kept, got in parts]
    at = lambda values, axis, idx: lax.dynamic_index_in_dim(values, idx, axis, keepdims=False)
    results = []
    for grads in summed:
        axis, cut = (-1, 2560) if grads.shape[-1] == G_COLS else (-2, 96)
        size = grads.shape[axis]
        one, two = lax.slice_in_dim(grads, 0, cut, axis=axis), lax.slice_in_dim(grads, cut, size, axis=axis)
        one_got = swap_with(2, at(one, 1, 1 - x))
        two_got = swap_with(4, at(two, 0, 1 - y))
        results.append((at(one, 1, x), one_got, at(two, 0, y), two_got, axis))
    finals = []
    for one, one_got, two, two_got, axis in results:
        one, two = one + one_got, two + two_got
        finals.append((at(one, 0, y), swap_with(4, at(one, 0, 1 - y)), at(two, 0, x), swap_with(2, at(two, 0, 1 - x)), axis))
    return [jnp.concatenate([one + one_got, two + two_got], axis=axis) for one, one_got, two, two_got, axis in finals]


def solution(mesh):
    row_spec = P(AXIS_NAME, None)
    vec_spec = P(AXIS_NAME)
    full_spec = P(None)
    batch_spec = P(AXIS_NAME, None, None)
    weight_specs = (vec_spec, row_spec, row_spec, row_spec, full_spec, full_spec, row_spec, vec_spec, row_spec, row_spec, row_spec)

    def device_step(tokens, positions, table_shard, attn_norm, w_query, w_key, w_value, q_norm, k_norm, w_out, mlp_norm, w_gate, w_up, w_down, dy_out):
        batch_len, seq_len = tokens.shape
        devices = lax.axis_size(AXIS_NAME)
        rows_local = table_shard.shape[0]
        shard = w_query.shape[0]
        all_ids = lax.all_gather(tokens, AXIS_NAME)
        norms = jnp.concatenate([attn_norm[:, None], mlp_norm[:, None], jnp.zeros((shard, W_COLS - C_NORM - 2), BF)], axis=1)
        pad = jnp.zeros((shard, 64), BF)
        packed = jnp.concatenate([w_query, w_key, w_value, pad, w_out, pad, w_gate, w_up, norms], axis=1)
        w_pack = lax.all_gather(packed, AXIS_NAME, tiled=True)
        w_down_full = lax.all_gather(w_down, AXIS_NAME, tiled=True)
        gains = w_pack[:, C_NORM:C_NORM + 2].T.astype(F32)
        head_gains = jnp.stack([q_norm, k_norm]).astype(F32)
        swapped = jnp.concatenate([head_gains[:, 32:], head_gains[:, :32]], axis=1)
        head_gains = jnp.concatenate([head_gains, swapped], axis=1)

        inv_freq = jnp.exp(jnp.arange(HEAD // 2, dtype=F32) * (-2.0 * math.log(ROPE_THETA) / HEAD))
        angles = positions.reshape(-1, 1).astype(F32) * inv_freq
        cos_t, sin_t = jnp.cos(angles), jnp.sin(angles)
        cs = jnp.concatenate([cos_t, cos_t, -sin_t, sin_t], axis=1)
        dy = dy_out.reshape(-1, D)

        starts = [sum(CHUNKS[:c]) for c in range(len(CHUNKS))]
        take_from, add_to, clashes = [], [], []
        for first, size in zip(starts, CHUNKS):
            local_ids = all_ids[:, first:first + size].reshape(-1, LANES) - lax.axis_index(AXIS_NAME) * rows_local
            is_owner = (local_ids >= 0) & (local_ids < rows_local)
            line = lax.broadcasted_iota(jnp.int32, local_ids.shape, 0)
            take_from.append((jnp.where(is_owner, local_ids, rows_local) * ROW_WORDS).reshape(-1))
            spot = jnp.where(is_owner, local_ids, rows_local + line % GROUP_ROWS)
            add_to.append((spot * ACC_WORDS + 1 - line % 2).reshape(-1))
            groups = spot.reshape(-1, GROUP_ROWS, LANES)
            twice = jnp.concatenate([groups, groups], axis=1)
            same = [jnp.any(groups == twice[:, shift:shift + GROUP_ROWS], axis=1) for shift in range(1, GROUP_ROWS // 2 + 1)]
            clashes.append(functools.reduce(jnp.logical_or, same).astype(jnp.int32).reshape(-1))

        table_t = table_shard.T
        picked = gather_rows(take_from[0], table_t, (devices * CHUNKS[0],))
        picked += gather_rows(jnp.concatenate(take_from[1:]), table_t, tuple(devices * n for n in CHUNKS[1:]))
        xs = [lax.psum_scatter(rows, AXIS_NAME, scatter_dimension=0, tiled=True) for rows in picked]
        core = lax.rem(lax.axis_index(AXIS_NAME), 2).reshape(1)
        carry = None
        rows_of = []
        for idx in range(len(CHUNKS)):
            x_chunk = xs[idx]
            dx, carry = layer_chunk(x_chunk, dy, cs, w_pack, w_down_full, gains, head_gains, core, starts[idx], carry, idx == len(CHUNKS) - 1, batch_len * seq_len)
            rows_of.append(lax.all_gather(dx, AXIS_NAME, tiled=True))
        *grads, y = carry
        d_table = None
        for idx in range(len(CHUNKS)):
            d_table = scatter_rows(add_to[idx], clashes[idx], rows_of[idx], rows_local, d_table, idx == len(CHUNKS) - 1)
        d_table = d_table.T
        g_pack, d_w_down = reduce_grads(grads)
        kv_cols = w_key.shape[1]
        return (y.reshape(batch_len, seq_len, D), d_table, g_pack[:, C_NORM], g_pack[:, :D], g_pack[:, D:D + kv_cols], g_pack[:, D + kv_cols:D + 2 * kv_cols],
                g_pack[0, C_HEAD:C_HEAD + HEAD], g_pack[0, C_HEAD + HEAD:C_HEAD + 2 * HEAD], g_pack[:, C_OUT:C_OUT + D], g_pack[:, C_NORM + 1],
                g_pack[:, C_GATE:C_GATE + FF], g_pack[:, C_UP:C_UP + FF], d_w_down)

    return jax.shard_map(device_step, mesh=mesh, in_specs=(row_spec, row_spec, row_spec) + weight_specs + (batch_spec,), out_specs=(batch_spec, row_spec) + weight_specs, check_vma=False)
```

```python
import functools
import math
import jax
import jax.numpy as jnp
from jax import lax
from jax.experimental import pallas as pl
from jax.experimental.pallas import tpu as pltpu
from jax.sharding import PartitionSpec as P

NORM_EPS = 1e-6
ROPE_THETA = 1.0e6
AXIS_NAME = 'fsdp'
SEQ = 256
HALF_SEQ = SEQ // 2
SEQS = 2
LANES = 128
D = 576
FF = 1536
HEAD = 64
HEADS = 9
KV = 3
GRP = 3
C_OUT, C_GATE, C_UP, C_NORM, C_HEAD = 1024, 1664, 3200, 4736, 4864
W_COLS, G_COLS = 4864, 4992
X_K, X_V, X_COLS = HEADS * LANES, (HEADS + KV) * LANES, (HEADS + 2 * KV) * LANES
FF_STEP = 512
CHUNKS = (4, 4, 4)
PAIR_WORDS = 9
BF, F32 = jnp.bfloat16, jnp.float32


def mm(lhs, rhs, lhs_dim=1, rhs_dim=0):
    return lax.dot_general(lhs, rhs, (((lhs_dim,), (rhs_dim,)), ((), ())), preferred_element_type=F32)


def fold8(values):
    return jnp.sum(values.reshape(values.shape[0] // 8, 8, values.shape[1]), axis=0)


def norm_bwd(grad_out, normed, inv_rms, norm_gain):
    grad_normed = grad_out * norm_gain
    return inv_rms * (grad_normed - normed * jnp.mean(grad_normed * normed, axis=-1, keepdims=True))


def head_norm_rope(head_ext, gain_ext, cs):
    head_f = head_ext.astype(F32)
    inv = lax.rsqrt(jnp.sum(head_f * head_f, axis=-1, keepdims=True) * (1.0 / LANES) + NORM_EPS)
    turned = head_f * inv * gain_ext * cs
    return turned + pltpu.roll(turned, 64, 1), inv


def head_norm_rope_bwd(grad_ext, head_ext, inv, gain_low, cs_bwd, low):
    turned = grad_ext * cs_bwd
    grad_t = turned + pltpu.roll(turned, 64, 1)
    normed = jnp.where(low, head_ext.astype(F32), 0.0) * inv
    grad_normed = grad_t * gain_low
    mean_term = jnp.sum(grad_normed * normed, axis=-1, keepdims=True) * (1.0 / HEAD)
    return inv * (grad_normed - normed * mean_term), fold8(grad_t * normed)


def pack_pairs(heads):
    tiles = []
    for idx in range(0, len(heads), 2):
        tile = heads[idx]
        if idx + 1 < len(heads):
            tile = tile + pltpu.roll(heads[idx + 1], 64, 1)
        tiles.append(tile.astype(BF))
    return tiles


def layer_kernel(first, last, steps, *refs):
    (x_ref, dy_ref, cs_ref, w_ref, wd_ref, gains_ref, head_gains_ref, core_ref) = refs[:8]
    refs = refs[8:]
    if not first:
        acc_in, accd_in, _ = refs[:3]
        refs = refs[3:]
    y_ref, dx_ref = refs[:2]
    outs = refs[2:6] if last else refs[2:4]
    (acc, accd, norm_acc, head_acc, wx, wox, qkv_s, upper_s, lower_s, tbuf, sems) = refs[2 + len(outs):]
    step = pl.program_id(0)
    low = lax.broadcasted_iota(jnp.int32, (1, LANES), 1) < 64

    @pl.when(step == 0)
    def _():
        if first:
            acc[...] = jnp.zeros_like(acc)
            accd[...] = jnp.zeros_like(accd)
        else:
            load_acc = pltpu.make_async_copy(acc_in, acc, sems.at[0])
            load_accd = pltpu.make_async_copy(accd_in, accd, sems.at[1])
            load_acc.start()
            load_accd.start()
        norm_acc[...] = jnp.zeros_like(norm_acc)
        head_acc[...] = jnp.zeros_like(head_acc)
        for h in range(HEADS + 2 * KV):
            tile = w_ref[:, (h // 2) * LANES:(h // 2) * LANES + LANES].astype(F32)
            moved = pltpu.roll(tile, 64, 1)
            if h >= HEADS + KV:
                both = jnp.where(low, moved if h % 2 else tile, 0.0)
            else:
                twice = jnp.where(low, moved, tile) if h % 2 else jnp.where(low, tile, moved)
                both = jnp.where(low, twice, pltpu.roll(twice, 32, 1))
            wx[:, h * LANES:h * LANES + LANES] = both.astype(BF)
        for h in range(HEADS):
            wox[h * LANES:h * LANES + 64, :] = w_ref[h * 64:h * 64 + 64, C_OUT:C_OUT + D]
            wox[h * LANES + 64:h * LANES + LANES, :] = jnp.zeros((64, D), BF)
        if not first:
            load_acc.wait()
            load_accd.wait()

    gain1 = gains_ref[0:1, :]
    gain2 = gains_ref[1:2, :]
    gain_q, gain_k = head_gains_ref[0:1, :], head_gains_ref[1:2, :]
    low_q, low_k = jnp.where(low, gain_q, 0.0), jnp.where(low, gain_k, 0.0)
    scale = HEAD ** -0.5
    stacked = GRP * HALF_SEQ
    row = lax.broadcasted_iota(jnp.int32, (stacked, SEQ), 0) & (HALF_SEQ - 1)
    lower_mask = lax.broadcasted_iota(jnp.int32, (stacked, SEQ), 1) - HALF_SEQ <= row
    upper_mask = lower_mask[:, HALF_SEQ:]

    def halves(tiles):
        return jnp.concatenate([t[:HALF_SEQ] for t in tiles], axis=0), jnp.concatenate([t[HALF_SEQ:] for t in tiles], axis=0)

    def joined(upper, lower, r):
        return jnp.concatenate([part[r * HALF_SEQ:(r + 1) * HALF_SEQ] for part in (upper, lower)], axis=0)

    def softmax(scores, mask):
        scores = jnp.where(mask, scores, -1e30)
        expd = jnp.exp(scores - jnp.max(scores, axis=-1, keepdims=True))
        return expd * (1.0 / jnp.sum(expd, axis=-1, keepdims=True))

    parts = []
    for s in range(SEQS):
        pairs = x_ref[s * HALF_SEQ:(s + 1) * HALF_SEQ, :].astype(F32)
        tails = pairs[:, 512:640]
        parts.append(jnp.concatenate([pairs[:, :512], tails[:, :64]], axis=1))
        parts.append(jnp.concatenate([pairs[:, 640:], pltpu.roll(tails, 64, 1)[:, :64]], axis=1))
    x = jnp.concatenate(parts, axis=0)
    inv1 = lax.rsqrt(jnp.mean(x * x, axis=-1, keepdims=True) + NORM_EPS)
    m1 = (x * inv1 * gain1).astype(BF)
    qkv_s[...] = mm(m1, wx[...]).astype(BF)
    saved, packed = [], []
    for s in range(SEQS):
        rows = slice(s * SEQ, (s + 1) * SEQ)
        cs = cs_ref[rows, :]
        heads = []
        for g in range(KV):
            ke = qkv_s[rows, X_K + g * LANES:X_K + (g + 1) * LANES]
            v0 = qkv_s[rows, X_V + g * LANES:X_V + (g + 1) * LANES]
            k_rot, k_inv = head_norm_rope(ke, gain_k, cs)
            k0 = jnp.where(low, k_rot, 0.0).astype(BF)
            k_swap = (jnp.where(low, k_rot, pltpu.roll(k_rot, 32, 1)) * scale).astype(BF)
            qs, q_swaps, q_invs = [], [], []
            for r in range(GRP):
                h = g * GRP + r
                q_rot, q_inv = head_norm_rope(qkv_s[rows, h * LANES:(h + 1) * LANES], gain_q, cs * scale)
                qs.append(q_rot.astype(BF))
                q_swaps.append(jnp.where(low, q_rot, pltpu.roll(q_rot, 32, 1)).astype(BF))
                q_invs.append(q_inv)
            q_upper, q_lower = halves(qs)
            upper = softmax(mm(q_upper, k0[:HALF_SEQ], 1, 1), upper_mask)
            lower = softmax(mm(q_lower, k0, 1, 1), lower_mask)
            upper_s[s * KV + g] = upper
            lower_s[s * KV + g] = lower
            o_upper, o_lower = mm(upper.astype(BF), v0[:HALF_SEQ]), mm(lower.astype(BF), v0)
            heads += [joined(o_upper, o_lower, r) for r in range(GRP)]
            saved.append((k_swap, halves(q_swaps), q_invs, k_inv))
        packed.append(jnp.concatenate(pack_pairs(heads), axis=1))
    attn = jnp.concatenate(packed, axis=0)
    hidden_b = (x + mm(attn[:, :D], w_ref[:, C_OUT:C_OUT + D])).astype(BF)
    hidden = hidden_b.astype(F32)
    inv2 = lax.rsqrt(jnp.mean(hidden * hidden, axis=-1, keepdims=True) + NORM_EPS)
    m2 = (hidden * inv2 * gain2).astype(BF)

    dy = dy_ref[...]
    m2_t = m2.T
    dy_t = dy.T
    y = hidden
    dm2 = jnp.zeros((SEQS * SEQ, D), F32)
    for f in range(0, FF, FF_STEP):
        wg = w_ref[:, C_GATE + f:C_GATE + f + FF_STEP]
        wu = w_ref[:, C_UP + f:C_UP + f + FF_STEP]
        wd = wd_ref[f:f + FF_STEP, :]
        gate = mm(m2, wg)
        up = mm(m2, wu)
        dact = mm(dy, wd, 1, 1)
        sig = 1.0 / (1.0 + jnp.exp(-gate))
        silu = gate * sig
        act = (silu * up).astype(BF)
        y = y + mm(act, wd)
        dgate = (dact * up * sig * (1.0 + gate * (1.0 - sig))).astype(BF)
        dup = (dact * silu).astype(BF)
        dm2 = dm2 + mm(dgate, wg, 1, 1) + mm(dup, wu, 1, 1)
        acc[:, C_GATE + f:C_GATE + f + FF_STEP] += mm(m2_t, dgate)
        acc[:, C_UP + f:C_UP + f + FF_STEP] += mm(m2_t, dup)
        accd[:, f:f + FF_STEP] += mm(dy_t, act)
    y_ref[...] = y.astype(BF)
    n2 = hidden * inv2
    norm_acc[1] += fold8(dm2 * n2)
    dh = dy.astype(F32) + norm_bwd(dm2, n2, inv2, gain2)
    dh_b = dh.astype(BF)
    acc[:, C_OUT:C_OUT + D] += mm(attn.T, dh_b)[:D]

    do = mm(dh_b, wox[...], 1, 1).astype(BF)
    packed = []
    for s in range(SEQS):
        rows = slice(s * SEQ, (s + 1) * SEQ)
        cs = cs_ref[rows, :]
        cs_bwd = jnp.where(low, cs, -cs)
        dqs, dks, dvs = [], [], []
        for g in range(KV):
            k_swap, (swap_upper, swap_lower), q_invs, k_inv = saved[s * KV + g]
            v0 = qkv_s[rows, X_V + g * LANES:X_V + (g + 1) * LANES]
            do_upper, do_lower = halves([do[rows, h * LANES:(h + 1) * LANES] for h in range(g * GRP, (g + 1) * GRP)])
            upper, lower = upper_s[s * KV + g], lower_s[s * KV + g]
            d_upper, d_lower = mm(do_upper, v0[:HALF_SEQ], 1, 1), mm(do_lower, v0, 1, 1)
            ds_upper = (upper * (d_upper - jnp.sum(d_upper * upper, axis=-1, keepdims=True))).astype(BF)
            ds_lower = (lower * (d_lower - jnp.sum(d_lower * lower, axis=-1, keepdims=True))).astype(BF)

            def over_queries(left_upper, left_lower, right_upper, right_lower):
                short, full = mm(left_upper.T, right_upper), mm(left_lower.T, right_lower)
                return jnp.concatenate([(full[:, :HALF_SEQ] + short).T, full[:, HALF_SEQ:].T], axis=0)

            dvs.append(over_queries(do_upper, do_lower, upper.astype(BF), lower.astype(BF)))
            dk = over_queries(swap_upper, swap_lower, ds_upper, ds_lower)
            dk, dk_gain = head_norm_rope_bwd(dk, qkv_s[rows, X_K + g * LANES:X_K + (g + 1) * LANES], k_inv, low_k, cs_bwd, low)
            dks.append(dk)
            head_acc[1] += dk_gain
            dq_upper, dq_lower = mm(ds_upper, k_swap[:HALF_SEQ]), mm(ds_lower, k_swap)
            for r in range(GRP):
                h = g * GRP + r
                dq_h, dq_gain = head_norm_rope_bwd(joined(dq_upper, dq_lower, r), qkv_s[rows, h * LANES:(h + 1) * LANES], q_invs[r], low_q, cs_bwd, low)
                dqs.append(dq_h)
                head_acc[0] += dq_gain
        packed.append(jnp.concatenate(pack_pairs(dqs + dks + dvs), axis=1))
    dqkv = jnp.concatenate(packed, axis=0)
    acc[:, 0:1024] += mm(m1.T, dqkv)
    dm1 = mm(dqkv, w_ref[:, 0:1024], 1, 1)
    n1 = x * inv1
    norm_acc[0] += fold8(dm1 * n1)
    dx = dh + norm_bwd(dm1, n1, inv1, gain1)
    for s in range(SEQS):
        upper, lower = dx[s * SEQ:s * SEQ + HALF_SEQ], dx[s * SEQ + HALF_SEQ:(s + 1) * SEQ]
        base = s * HALF_SEQ * PAIR_WORDS
        for j in range(4):
            dx_ref[pl.ds(base + j, HALF_SEQ, stride=PAIR_WORDS), :] = upper[:, j * LANES:(j + 1) * LANES]
            dx_ref[pl.ds(base + 5 + j, HALF_SEQ, stride=PAIR_WORDS), :] = lower[:, j * LANES:(j + 1) * LANES]
        dx_ref[pl.ds(base + 4, HALF_SEQ, stride=PAIR_WORDS), :] = jnp.concatenate([upper[:, 512:], lower[:, 512:]], axis=1)

    @pl.when(step == steps - 1)
    def _():
        top = lax.broadcasted_iota(jnp.int32, (LANES, 1), 0)
        rows1 = jnp.sum(norm_acc[0], axis=0, keepdims=True)
        rows2 = jnp.sum(norm_acc[1], axis=0, keepdims=True)
        both = jnp.where(top == 0, rows1, 0.0) + jnp.where(top == 1, rows2, 0.0)
        for c in range(0, D, LANES):
            width = min(LANES, D - c)
            acc[c:c + width, C_NORM:C_NORM + LANES] += both[:, c:c + width].T
        head_q = jnp.sum(head_acc[0], axis=0, keepdims=True)
        head_k = jnp.sum(head_acc[1], axis=0, keepdims=True)
        head_row = jnp.where(low, head_q, pltpu.roll(head_k, 64, 1))
        acc[:, C_HEAD:C_HEAD + LANES] += jnp.broadcast_to(head_row, (D, LANES))
        if last:
            mine = core_ref[0]

            def send_block(d, src, keep, send, sem):
                @pl.when(mine == d % 2)
                def _():
                    pltpu.make_async_copy(src, keep.at[d // 2], sem).start()

                @pl.when(mine != d % 2)
                def _():
                    pltpu.make_async_copy(src, send.at[d // 2], sem).start()

                return pltpu.make_async_copy(src, keep.at[d // 2], sem)

            stores = [send_block(d, acc.at[pl.ds(d * 72, 72), :], outs[0], outs[1], sems.at[0]) for d in range(8)]
            for part in range(0, 8, 4):
                moved = []
                for d in range(4):
                    f = (part + d) * 192
                    for t in range(0, D, LANES):
                        width = min(LANES, D - t)
                        tbuf[d * 192:d * 192 + 192, t:t + width] = accd[t:t + width, f:f + 192].T
                    moved.append(send_block(part + d, tbuf.at[pl.ds(d * 192, 192), :], outs[2], outs[3], sems.at[1]))
                for store in moved:
                    store.wait()
        else:
            stores = [pltpu.make_async_copy(acc, outs[0], sems.at[0]), pltpu.make_async_copy(accd, outs[1], sems.at[0])]
            for store in stores:
                store.start()
        for store in stores:
            store.wait()


ROW_WORDS = 5
ACC_WORDS = 6
GROUP_ROWS = 16
PAD_ROWS = 16


def gather_kernel(blocks, ids_ref, tab_ref, *refs):
    outs, (lin, buf) = refs[:-2], refs[-2:]
    step = pl.program_id(0)
    rows = tab_ref.shape[1]

    @pl.when(step == 0)
    def _():
        def build(b, _):
            at = pl.multiple_of(b * LANES, LANES)
            for j in range(ROW_WORDS):
                part = tab_ref[j * LANES:min(j * LANES + LANES, D), pl.ds(at, LANES)].astype(F32)
                if part.shape[0] < LANES:
                    part = jnp.concatenate([part, jnp.zeros((LANES - part.shape[0], LANES), F32)], axis=0)
                lin[pl.ds(at * ROW_WORDS + j, LANES, stride=ROW_WORDS), :] = part.T
            return 0

        lax.fori_loop(0, rows // LANES, build, 0)
        lin[rows * ROW_WORDS:(rows + PAD_ROWS) * ROW_WORDS, :] = jnp.zeros((PAD_ROWS * ROW_WORDS, LANES), F32)

    def pick(k, _):
        base = k * GROUP_ROWS
        got = [lin[pl.ds(ids_ref[step * SEQ + base + u], ROW_WORDS), :] for u in range(GROUP_ROWS)]
        for u in range(GROUP_ROWS):
            buf[pl.ds((base + u) * ROW_WORDS, ROW_WORDS), :] = got[u]
        return 0

    lax.fori_loop(0, SEQ // GROUP_ROWS, pick, 0)
    first = 0
    half = HALF_SEQ * ROW_WORDS
    for out, count in zip(outs, blocks):
        @pl.when((step >= first) & (step < first + count))
        def _():
            for j in range(4):
                out[:, j * LANES:j * LANES + LANES] = buf[pl.ds(j, HALF_SEQ, stride=ROW_WORDS), :].astype(BF)
                out[:, 640 + j * LANES:768 + j * LANES] = buf[pl.ds(half + j, HALF_SEQ, stride=ROW_WORDS), :].astype(BF)
            tails = buf[pl.ds(4, HALF_SEQ, stride=ROW_WORDS), :] + pltpu.roll(buf[pl.ds(half + 4, HALF_SEQ, stride=ROW_WORDS), :], 64, 1)
            out[:, 512:640] = tails.astype(BF)

        first += count


def gather_rows(ids, table_t, blocks):
    starts = [sum(blocks[:c]) for c in range(len(blocks))]
    rows = table_t.shape[1]
    out_spec = lambda c: pl.BlockSpec((HALF_SEQ, 2 * D), lambda i, ids: (jnp.clip(i - starts[c], 0, blocks[c] - 1), 0))
    return pl.pallas_call(
        functools.partial(gather_kernel, blocks),
        grid_spec=pltpu.PrefetchScalarGridSpec(
            num_scalar_prefetch=1,
            grid=(sum(blocks),),
            in_specs=[pl.BlockSpec(table_t.shape, lambda i, ids: (0, 0), pipeline_mode=pl.Buffered(1))],
            out_specs=[out_spec(c) for c in range(len(blocks))],
            scratch_shapes=[pltpu.VMEM(((rows + PAD_ROWS) * ROW_WORDS, LANES), F32), pltpu.VMEM((SEQ * ROW_WORDS, LANES), F32)],
        ),
        out_shape=[jax.ShapeDtypeStruct((count * HALF_SEQ, 2 * D), BF) for count in blocks],
        compiler_params=pltpu.CompilerParams(dimension_semantics=('arbitrary',), vmem_limit_bytes=48 << 20),
        cost_estimate=pl.CostEstimate(flops=40_000_000_000, bytes_accessed=40_000_000, transcendentals=0),
        name='gather_rows',
    )(ids, table_t)


def scatter_kernel(first, last, blocks, ids_ref, clash_ref, rows_ref, *refs):
    if not first:
        acc_in, refs = refs[0], refs[1:]
    out_ref, acc, sem = refs[:3]
    tbuf = refs[3] if last else None
    step = pl.program_id(0)
    rows = acc.shape[0] // ACC_WORDS - PAD_ROWS

    @pl.when(step == 0)
    def _():
        if first:
            acc[...] = jnp.zeros_like(acc)
        else:
            load = pltpu.make_async_copy(acc_in, acc, sem.at[0])
            load.start()
            load.wait()

    groups = SCATTER_ROWS // GROUP_ROWS

    def add(k, _):
        spots = [pl.ds(ids_ref[step * SCATTER_ROWS + u * LANES + k], ROW_WORDS) for u in range(GROUP_ROWS)]
        from_row = lambda u: rows_ref[pl.ds((u // 2 * LANES + k) * PAIR_WORDS + (u % 2) * 4, ROW_WORDS), :]
        clash = clash_ref[step * groups + k]

        @pl.when(clash == 0)
        def _():
            sums = [acc[spots[u], :] + from_row(u) for u in range(GROUP_ROWS)]
            for u in range(GROUP_ROWS):
                acc[spots[u], :] = sums[u]

        @pl.when(clash != 0)
        def _():
            for u in range(GROUP_ROWS):
                acc[spots[u], :] += from_row(u)

        return 0

    lax.fori_loop(0, groups, add, 0)

    @pl.when(step == blocks - 1)
    def _():
        if last:
            wide = FLUSH_ROWS

            def flush(b, _):
                slot = lax.rem(b, 2)
                at = pl.multiple_of(b * wide, wide)
                store = pltpu.make_async_copy(tbuf.at[slot], out_ref.at[:, pl.ds(at, wide)], sem.at[slot])

                @pl.when(b >= 2)
                def _():
                    store.wait()

                word = lambda w, r: acc[pl.ds((at + r) * ACC_WORDS + w, LANES, stride=ACC_WORDS), :]
                for r in range(0, wide, LANES):
                    for j in range(4):
                        tbuf[slot, j * LANES:j * LANES + LANES, r:r + LANES] = word(1 + j, r).T
                    tail = word(5, r) + pltpu.roll(word(0, r), 64, 1)
                    tbuf[slot, 512:D, r:r + LANES] = tail.T[:64]
                store.start()
                return 0

            lax.fori_loop(0, rows // wide, flush, 0)
            for slot in range(2):
                pltpu.make_async_copy(tbuf.at[slot], out_ref.at[:, pl.ds(0, wide)], sem.at[slot]).wait()
        else:
            store = pltpu.make_async_copy(acc, out_ref, sem.at[0])
            store.start()
            store.wait()


SCATTER_ROWS = LANES * GROUP_ROWS
FLUSH_ROWS = 512


def scatter_rows(ids, clash, rows_in, table_rows, carry, last):
    first = carry is None
    blocks = rows_in.shape[0] // (SCATTER_ROWS // 2 * PAIR_WORDS)
    acc_shape = ((table_rows + PAD_ROWS) * ACC_WORDS, LANES)
    anyspec = pl.BlockSpec(memory_space=pl.ANY)
    scratch = [pltpu.VMEM(acc_shape, F32), pltpu.SemaphoreType.DMA((2,))]
    if last:
        scratch.append(pltpu.VMEM((2, D, FLUSH_ROWS), F32))
    return pl.pallas_call(
        functools.partial(scatter_kernel, first, last, blocks),
        grid_spec=pltpu.PrefetchScalarGridSpec(
            num_scalar_prefetch=2,
            grid=(blocks,),
            in_specs=[pl.BlockSpec((SCATTER_ROWS // 2 * PAIR_WORDS, LANES), lambda i, *_: (i, 0))] + ([] if first else [anyspec]),
            out_specs=anyspec,
            scratch_shapes=scratch,
        ),
        out_shape=jax.ShapeDtypeStruct((D, table_rows) if last else acc_shape, F32),
        input_output_aliases={} if first or last else {3: 0},
        compiler_params=pltpu.CompilerParams(dimension_semantics=('arbitrary',), vmem_limit_bytes=48 << 20),
        cost_estimate=pl.CostEstimate(flops=20_000_000_000, bytes_accessed=60_000_000, transcendentals=0),
        name='scatter_rows',
    )(*([ids, clash, rows_in] + ([] if first else [carry])))


def layer_chunk(x, dy, cs, w_pack, w_down, gains, head_gains, core, start, carry, last, total):
    steps = x.shape[0] // (SEQS * HALF_SEQ)
    start = start // SEQS
    first = carry is None
    whole = lambda shape: pl.BlockSpec(shape, lambda i: (0,) * len(shape), pipeline_mode=pl.Buffered(1))
    here = lambda cols: pl.BlockSpec((SEQS * SEQ, cols), lambda i: (i + start, 0))
    anyspec = pl.BlockSpec(memory_space=pl.ANY)
    in_specs = [pl.BlockSpec((SEQS * HALF_SEQ, 2 * D), lambda i: (i, 0)), here(D), here(LANES), whole(w_pack.shape), whole(w_down.shape), whole(gains.shape), whole(head_gains.shape), pl.BlockSpec(memory_space=pltpu.SMEM)]
    args = [x, dy, cs, w_pack, w_down, gains, head_gains, core]
    aliases = {}
    if not first:
        in_specs += [anyspec] * 3
        args += list(carry)
        aliases = {10: 0} if last else {8: 2, 9: 3, 10: 0}
    out_shape = [
        jax.ShapeDtypeStruct((total, D), BF),
        jax.ShapeDtypeStruct((steps * SEQS * HALF_SEQ * PAIR_WORDS, LANES), F32),
    ]
    grad_shapes = [(4, 72, G_COLS)] * 2 + [(4, 192, D)] * 2 if last else [(D, G_COLS), (D, FF)]
    out_shape += [jax.ShapeDtypeStruct(shape, F32) for shape in grad_shapes]
    y, dx, *grads = pl.pallas_call(
        functools.partial(layer_kernel, first, last, steps),
        grid=(steps,),
        in_specs=in_specs,
        out_specs=[here(D), pl.BlockSpec((SEQS * HALF_SEQ * PAIR_WORDS, LANES), lambda i: (i, 0))] + [anyspec] * len(grad_shapes),
        out_shape=out_shape,
        scratch_shapes=[
            pltpu.VMEM((D, G_COLS), F32),
            pltpu.VMEM((D, FF), F32),
            pltpu.VMEM((2, 8, D), F32),
            pltpu.VMEM((2, 8, LANES), F32),
            pltpu.VMEM((D, X_COLS), BF),
            pltpu.VMEM((HEADS * LANES, D), BF),
            pltpu.VMEM((SEQS * SEQ, X_COLS), BF),
            pltpu.VMEM((SEQS * KV, GRP * HALF_SEQ, HALF_SEQ), F32),
            pltpu.VMEM((SEQS * KV, GRP * HALF_SEQ, SEQ), F32),
            pltpu.VMEM((FF // 2, D) if last else (8, LANES), F32),
            pltpu.SemaphoreType.DMA((2,)),
        ],
        input_output_aliases=aliases,
        compiler_params=pltpu.CompilerParams(dimension_semantics=('arbitrary',), vmem_limit_bytes=62 << 20),
        cost_estimate=pl.CostEstimate(flops=steps * SEQS * 6_000_000_000, bytes_accessed=steps * SEQS * 2_500_000 + 45_000_000, transcendentals=steps * SEQS * 1_000_000),
        name='layer_chunk',
    )(*args)
    return dx, (*grads, y)


def swap_with(bit, values):
    return lax.ppermute(values, AXIS_NAME, [(i, i ^ bit) for i in range(8)])


def gather_by_swaps(shard):
    index = lax.axis_index(AXIS_NAME)
    for bit in (1, 2, 4):
        got = swap_with(bit, shard)
        second = (index // bit) % 2 == 1
        shard = jnp.where(second, jnp.concatenate([got, shard], axis=0), jnp.concatenate([shard, got], axis=0))
    return shard


def reduce_grads(grads):
    index = lax.axis_index(AXIS_NAME)
    x, y = (index // 2) % 2, index // 4
    parts = [(grads[i], swap_with(1, grads[i + 1])) for i in (0, 2)]
    summed = [(kept + got).reshape(2, 2, *kept.shape[1:]) for kept, got in parts]
    at = lambda values, axis, idx: lax.dynamic_index_in_dim(values, idx, axis, keepdims=False)
    results = []
    for grads in summed:
        axis, cut = (-1, 2560) if grads.shape[-1] == G_COLS else (-2, 96)
        size = grads.shape[axis]
        one, two = lax.slice_in_dim(grads, 0, cut, axis=axis), lax.slice_in_dim(grads, cut, size, axis=axis)
        one_got = swap_with(2, at(one, 1, 1 - x))
        two_got = swap_with(4, at(two, 0, 1 - y))
        results.append((at(one, 1, x), one_got, at(two, 0, y), two_got, axis))
    finals = []
    for one, one_got, two, two_got, axis in results:
        one, two = one + one_got, two + two_got
        finals.append((at(one, 0, y), swap_with(4, at(one, 0, 1 - y)), at(two, 0, x), swap_with(2, at(two, 0, 1 - x)), axis))
    return [jnp.concatenate([one + one_got, two + two_got], axis=axis) for one, one_got, two, two_got, axis in finals]


def solution(mesh):
    row_spec = P(AXIS_NAME, None)
    vec_spec = P(AXIS_NAME)
    full_spec = P(None)
    batch_spec = P(AXIS_NAME, None, None)
    weight_specs = (vec_spec, row_spec, row_spec, row_spec, full_spec, full_spec, row_spec, vec_spec, row_spec, row_spec, row_spec)

    def device_step(tokens, positions, table_shard, attn_norm, w_query, w_key, w_value, q_norm, k_norm, w_out, mlp_norm, w_gate, w_up, w_down, dy_out):
        batch_len, seq_len = tokens.shape
        devices = lax.axis_size(AXIS_NAME)
        rows_local = table_shard.shape[0]
        shard = w_query.shape[0]
        all_ids = lax.all_gather(tokens, AXIS_NAME)
        norms = jnp.concatenate([attn_norm[:, None], mlp_norm[:, None], jnp.zeros((shard, W_COLS - C_NORM - 2), BF)], axis=1)
        pad = jnp.zeros((shard, 64), BF)
        packed = jnp.concatenate([w_query, w_key, w_value, pad, w_out, pad, w_gate, w_up, norms], axis=1)
        w_pack = lax.all_gather(packed, AXIS_NAME, tiled=True)
        w_down_full = gather_by_swaps(w_down)
        gains = w_pack[:, C_NORM:C_NORM + 2].T.astype(F32)
        head_gains = jnp.stack([q_norm, k_norm]).astype(F32)
        swapped = jnp.concatenate([head_gains[:, 32:], head_gains[:, :32]], axis=1)
        head_gains = jnp.concatenate([head_gains, swapped], axis=1)

        inv_freq = jnp.exp(jnp.arange(HEAD // 2, dtype=F32) * (-2.0 * math.log(ROPE_THETA) / HEAD))
        angles = positions.reshape(-1, 1).astype(F32) * inv_freq
        cos_t, sin_t = jnp.cos(angles), jnp.sin(angles)
        cs = jnp.concatenate([cos_t, cos_t, -sin_t, sin_t], axis=1)
        dy = dy_out.reshape(-1, D)

        starts = [sum(CHUNKS[:c]) for c in range(len(CHUNKS))]
        take_from, add_to, clashes = [], [], []
        for first, size in zip(starts, CHUNKS):
            local_ids = all_ids[:, first:first + size].reshape(-1, LANES) - lax.axis_index(AXIS_NAME) * rows_local
            is_owner = (local_ids >= 0) & (local_ids < rows_local)
            line = lax.broadcasted_iota(jnp.int32, local_ids.shape, 0)
            take_from.append((jnp.where(is_owner, local_ids, rows_local) * ROW_WORDS).reshape(-1))
            spot = jnp.where(is_owner, local_ids, rows_local + line % GROUP_ROWS)
            add_to.append((spot * ACC_WORDS + 1 - line % 2).reshape(-1))
            groups = spot.reshape(-1, GROUP_ROWS, LANES)
            twice = jnp.concatenate([groups, groups], axis=1)
            same = [jnp.any(groups == twice[:, shift:shift + GROUP_ROWS], axis=1) for shift in range(1, GROUP_ROWS // 2 + 1)]
            clashes.append(functools.reduce(jnp.logical_or, same).astype(jnp.int32).reshape(-1))

        table_t = table_shard.T
        picked = gather_rows(take_from[0], table_t, (devices * CHUNKS[0],))
        picked += gather_rows(jnp.concatenate(take_from[1:]), table_t, tuple(devices * n for n in CHUNKS[1:]))
        xs = [lax.psum_scatter(rows, AXIS_NAME, scatter_dimension=0, tiled=True) for rows in picked]
        core = lax.rem(lax.axis_index(AXIS_NAME), 2).reshape(1)
        carry = None
        rows_of = []
        for idx in range(len(CHUNKS)):
            x_chunk = xs[idx]
            dx, carry = layer_chunk(x_chunk, dy, cs, w_pack, w_down_full, gains, head_gains, core, starts[idx], carry, idx == len(CHUNKS) - 1, batch_len * seq_len)
            rows_of.append(lax.all_gather(dx, AXIS_NAME, tiled=True))
        *grads, y = carry
        d_table = None
        for idx in range(len(CHUNKS)):
            d_table = scatter_rows(add_to[idx], clashes[idx], rows_of[idx], rows_local, d_table, idx == len(CHUNKS) - 1)
        d_table = d_table.T
        g_pack, d_w_down = reduce_grads(grads)
        kv_cols = w_key.shape[1]
        return (y.reshape(batch_len, seq_len, D), d_table, g_pack[:, C_NORM], g_pack[:, :D], g_pack[:, D:D + kv_cols], g_pack[:, D + kv_cols:D + 2 * kv_cols],
                g_pack[0, C_HEAD:C_HEAD + HEAD], g_pack[0, C_HEAD + HEAD:C_HEAD + 2 * HEAD], g_pack[:, C_OUT:C_OUT + D], g_pack[:, C_NORM + 1],
                g_pack[:, C_GATE:C_GATE + FF], g_pack[:, C_UP:C_UP + FF], d_w_down)

    return jax.shard_map(device_step, mesh=mesh, in_specs=(row_spec, row_spec, row_spec) + weight_specs + (batch_spec,), out_specs=(batch_spec, row_spec) + weight_specs, check_vma=False)
```

```python
import functools
import math
import jax
import jax.numpy as jnp
from jax import lax
from jax.experimental import pallas as pl
from jax.experimental.pallas import tpu as pltpu
from jax.sharding import PartitionSpec as P

NORM_EPS = 1e-6
ROPE_THETA = 1.0e6
AXIS_NAME = 'fsdp'
SEQ = 256
HALF_SEQ = SEQ // 2
SEQS = 1
LANES = 128
D = 576
FF = 1536
HEAD = 64
HEADS = 9
KV = 3
GRP = 3
C_OUT, C_GATE, C_UP, C_NORM, C_HEAD = 1024, 1664, 3200, 4736, 4864
W_COLS, G_COLS = 4864, 4992
X_K, X_V, X_COLS = HEADS * LANES, (HEADS + KV) * LANES, (HEADS + 2 * KV) * LANES
FF_STEP = 512
CHUNKS = (4, 4, 4)
PAIR_WORDS = 9
BF, F32 = jnp.bfloat16, jnp.float32


def mm(lhs, rhs, lhs_dim=1, rhs_dim=0):
    return lax.dot_general(lhs, rhs, (((lhs_dim,), (rhs_dim,)), ((), ())), preferred_element_type=F32)


def fold8(values):
    return jnp.sum(values.reshape(values.shape[0] // 8, 8, values.shape[1]), axis=0)


def norm_bwd(grad_out, normed, inv_rms, norm_gain):
    grad_normed = grad_out * norm_gain
    return inv_rms * (grad_normed - normed * jnp.mean(grad_normed * normed, axis=-1, keepdims=True))


def head_norm_rope(head_ext, gain_ext, cs):
    head_f = head_ext.astype(F32)
    inv = lax.rsqrt(jnp.sum(head_f * head_f, axis=-1, keepdims=True) * (1.0 / LANES) + NORM_EPS)
    turned = head_f * inv * gain_ext * cs
    return turned + pltpu.roll(turned, 64, 1), inv


def head_norm_rope_bwd(grad_ext, head_ext, inv, gain_low, cs_bwd, low):
    turned = grad_ext * cs_bwd
    grad_t = turned + pltpu.roll(turned, 64, 1)
    normed = jnp.where(low, head_ext.astype(F32), 0.0) * inv
    grad_normed = grad_t * gain_low
    mean_term = jnp.sum(grad_normed * normed, axis=-1, keepdims=True) * (1.0 / HEAD)
    return inv * (grad_normed - normed * mean_term), fold8(grad_t * normed)


def pack_pairs(heads):
    tiles = []
    for idx in range(0, len(heads), 2):
        tile = heads[idx]
        if idx + 1 < len(heads):
            tile = tile + pltpu.roll(heads[idx + 1], 64, 1)
        tiles.append(tile.astype(BF))
    return tiles


def layer_kernel(first, last, steps, *refs):
    (x_ref, dy_ref, cs_ref, w_ref, wd_ref, gains_ref, head_gains_ref, core_ref) = refs[:8]
    refs = refs[8:]
    if not first:
        acc_in, accd_in, _ = refs[:3]
        refs = refs[3:]
    y_ref, dx_ref = refs[:2]
    outs = refs[2:6] if last else refs[2:4]
    (acc, accd, norm_acc, head_acc, wx, wox, qkv_s, upper_s, lower_s, tbuf, sems) = refs[2 + len(outs):]
    step = pl.program_id(0)
    low = lax.broadcasted_iota(jnp.int32, (1, LANES), 1) < 64

    @pl.when(step == 0)
    def _():
        if first:
            acc[...] = jnp.zeros_like(acc)
            accd[...] = jnp.zeros_like(accd)
        else:
            load_acc = pltpu.make_async_copy(acc_in, acc, sems.at[0])
            load_accd = pltpu.make_async_copy(accd_in, accd, sems.at[1])
            load_acc.start()
            load_accd.start()
        norm_acc[...] = jnp.zeros_like(norm_acc)
        head_acc[...] = jnp.zeros_like(head_acc)
        for h in range(HEADS + 2 * KV):
            tile = w_ref[:, (h // 2) * LANES:(h // 2) * LANES + LANES].astype(F32)
            moved = pltpu.roll(tile, 64, 1)
            if h >= HEADS + KV:
                both = jnp.where(low, moved if h % 2 else tile, 0.0)
            else:
                twice = jnp.where(low, moved, tile) if h % 2 else jnp.where(low, tile, moved)
                both = jnp.where(low, twice, pltpu.roll(twice, 32, 1))
            wx[:, h * LANES:h * LANES + LANES] = both.astype(BF)
        for h in range(HEADS):
            wox[h * LANES:h * LANES + 64, :] = w_ref[h * 64:h * 64 + 64, C_OUT:C_OUT + D]
            wox[h * LANES + 64:h * LANES + LANES, :] = jnp.zeros((64, D), BF)
        if not first:
            load_acc.wait()
            load_accd.wait()

    gain1 = gains_ref[0:1, :]
    gain2 = gains_ref[1:2, :]
    gain_q, gain_k = head_gains_ref[0:1, :], head_gains_ref[1:2, :]
    low_q, low_k = jnp.where(low, gain_q, 0.0), jnp.where(low, gain_k, 0.0)
    scale = HEAD ** -0.5
    stacked = GRP * HALF_SEQ
    row = lax.broadcasted_iota(jnp.int32, (stacked, SEQ), 0) & (HALF_SEQ - 1)
    lower_mask = lax.broadcasted_iota(jnp.int32, (stacked, SEQ), 1) - HALF_SEQ <= row
    upper_mask = lower_mask[:, HALF_SEQ:]

    def halves(tiles):
        return jnp.concatenate([t[:HALF_SEQ] for t in tiles], axis=0), jnp.concatenate([t[HALF_SEQ:] for t in tiles], axis=0)

    def joined(upper, lower, r):
        return jnp.concatenate([part[r * HALF_SEQ:(r + 1) * HALF_SEQ] for part in (upper, lower)], axis=0)

    def softmax(scores, mask):
        scores = jnp.where(mask, scores, -1e30)
        expd = jnp.exp(scores - jnp.max(scores, axis=-1, keepdims=True))
        return expd * (1.0 / jnp.sum(expd, axis=-1, keepdims=True))

    parts = []
    for s in range(SEQS):
        pairs = x_ref[s * HALF_SEQ:(s + 1) * HALF_SEQ, :].astype(F32)
        tails = pairs[:, 512:640]
        parts.append(jnp.concatenate([pairs[:, :512], tails[:, :64]], axis=1))
        parts.append(jnp.concatenate([pairs[:, 640:], pltpu.roll(tails, 64, 1)[:, :64]], axis=1))
    x = jnp.concatenate(parts, axis=0)
    inv1 = lax.rsqrt(jnp.mean(x * x, axis=-1, keepdims=True) + NORM_EPS)
    m1 = (x * inv1 * gain1).astype(BF)
    qkv_s[...] = mm(m1, wx[...]).astype(BF)
    saved, packed = [], []
    for s in range(SEQS):
        rows = slice(s * SEQ, (s + 1) * SEQ)
        cs = cs_ref[rows, :]
        heads = []
        for g in range(KV):
            ke = qkv_s[rows, X_K + g * LANES:X_K + (g + 1) * LANES]
            v0 = qkv_s[rows, X_V + g * LANES:X_V + (g + 1) * LANES]
            k_rot, k_inv = head_norm_rope(ke, gain_k, cs)
            k0 = jnp.where(low, k_rot, 0.0).astype(BF)
            k_swap = (jnp.where(low, k_rot, pltpu.roll(k_rot, 32, 1)) * scale).astype(BF)
            qs, q_swaps, q_invs = [], [], []
            for r in range(GRP):
                h = g * GRP + r
                q_rot, q_inv = head_norm_rope(qkv_s[rows, h * LANES:(h + 1) * LANES], gain_q, cs * scale)
                qs.append(q_rot.astype(BF))
                q_swaps.append(jnp.where(low, q_rot, pltpu.roll(q_rot, 32, 1)).astype(BF))
                q_invs.append(q_inv)
            q_upper, q_lower = halves(qs)
            upper = softmax(mm(q_upper, k0[:HALF_SEQ], 1, 1), upper_mask)
            lower = softmax(mm(q_lower, k0, 1, 1), lower_mask)
            upper_s[s * KV + g] = upper
            lower_s[s * KV + g] = lower
            o_upper, o_lower = mm(upper.astype(BF), v0[:HALF_SEQ]), mm(lower.astype(BF), v0)
            heads += [joined(o_upper, o_lower, r) for r in range(GRP)]
            saved.append((k_swap, halves(q_swaps), q_invs, k_inv))
        packed.append(jnp.concatenate(pack_pairs(heads), axis=1))
    attn = jnp.concatenate(packed, axis=0)
    hidden_b = (x + mm(attn[:, :D], w_ref[:, C_OUT:C_OUT + D])).astype(BF)
    hidden = hidden_b.astype(F32)
    inv2 = lax.rsqrt(jnp.mean(hidden * hidden, axis=-1, keepdims=True) + NORM_EPS)
    m2 = (hidden * inv2 * gain2).astype(BF)

    dy = dy_ref[...]
    m2_t = m2.T
    dy_t = dy.T
    y = hidden
    dm2 = jnp.zeros((SEQS * SEQ, D), F32)
    for f in range(0, FF, FF_STEP):
        wg = w_ref[:, C_GATE + f:C_GATE + f + FF_STEP]
        wu = w_ref[:, C_UP + f:C_UP + f + FF_STEP]
        wd = wd_ref[f:f + FF_STEP, :]
        gate = mm(m2, wg)
        up = mm(m2, wu)
        dact = mm(dy, wd, 1, 1)
        sig = 1.0 / (1.0 + jnp.exp(-gate))
        silu = gate * sig
        act = (silu * up).astype(BF)
        y = y + mm(act, wd)
        dgate = (dact * up * sig * (1.0 + gate * (1.0 - sig))).astype(BF)
        dup = (dact * silu).astype(BF)
        dm2 = dm2 + mm(dgate, wg, 1, 1) + mm(dup, wu, 1, 1)
        acc[:, C_GATE + f:C_GATE + f + FF_STEP] += mm(m2_t, dgate)
        acc[:, C_UP + f:C_UP + f + FF_STEP] += mm(m2_t, dup)
        accd[:, f:f + FF_STEP] += mm(dy_t, act)
    y_ref[...] = y.astype(BF)
    n2 = hidden * inv2
    norm_acc[1] += fold8(dm2 * n2)
    dh = dy.astype(F32) + norm_bwd(dm2, n2, inv2, gain2)
    dh_b = dh.astype(BF)
    acc[:, C_OUT:C_OUT + D] += mm(attn.T, dh_b)[:D]

    do = mm(dh_b, wox[...], 1, 1).astype(BF)
    packed = []
    for s in range(SEQS):
        rows = slice(s * SEQ, (s + 1) * SEQ)
        cs = cs_ref[rows, :]
        cs_bwd = jnp.where(low, cs, -cs)
        dqs, dks, dvs = [], [], []
        for g in range(KV):
            k_swap, (swap_upper, swap_lower), q_invs, k_inv = saved[s * KV + g]
            v0 = qkv_s[rows, X_V + g * LANES:X_V + (g + 1) * LANES]
            do_upper, do_lower = halves([do[rows, h * LANES:(h + 1) * LANES] for h in range(g * GRP, (g + 1) * GRP)])
            upper, lower = upper_s[s * KV + g], lower_s[s * KV + g]
            d_upper, d_lower = mm(do_upper, v0[:HALF_SEQ], 1, 1), mm(do_lower, v0, 1, 1)
            ds_upper = (upper * (d_upper - jnp.sum(d_upper * upper, axis=-1, keepdims=True))).astype(BF)
            ds_lower = (lower * (d_lower - jnp.sum(d_lower * lower, axis=-1, keepdims=True))).astype(BF)

            def over_queries(left_upper, left_lower, right_upper, right_lower):
                short, full = mm(left_upper.T, right_upper), mm(left_lower.T, right_lower)
                return jnp.concatenate([(full[:, :HALF_SEQ] + short).T, full[:, HALF_SEQ:].T], axis=0)

            dvs.append(over_queries(do_upper, do_lower, upper.astype(BF), lower.astype(BF)))
            dk = over_queries(swap_upper, swap_lower, ds_upper, ds_lower)
            dk, dk_gain = head_norm_rope_bwd(dk, qkv_s[rows, X_K + g * LANES:X_K + (g + 1) * LANES], k_inv, low_k, cs_bwd, low)
            dks.append(dk)
            head_acc[1] += dk_gain
            dq_upper, dq_lower = mm(ds_upper, k_swap[:HALF_SEQ]), mm(ds_lower, k_swap)
            for r in range(GRP):
                h = g * GRP + r
                dq_h, dq_gain = head_norm_rope_bwd(joined(dq_upper, dq_lower, r), qkv_s[rows, h * LANES:(h + 1) * LANES], q_invs[r], low_q, cs_bwd, low)
                dqs.append(dq_h)
                head_acc[0] += dq_gain
        packed.append(jnp.concatenate(pack_pairs(dqs + dks + dvs), axis=1))
    dqkv = jnp.concatenate(packed, axis=0)
    acc[:, 0:1024] += mm(m1.T, dqkv)
    dm1 = mm(dqkv, w_ref[:, 0:1024], 1, 1)
    n1 = x * inv1
    norm_acc[0] += fold8(dm1 * n1)
    dx = dh + norm_bwd(dm1, n1, inv1, gain1)
    for s in range(SEQS):
        upper, lower = dx[s * SEQ:s * SEQ + HALF_SEQ], dx[s * SEQ + HALF_SEQ:(s + 1) * SEQ]
        base = s * HALF_SEQ * PAIR_WORDS
        for j in range(4):
            dx_ref[pl.ds(base + j, HALF_SEQ, stride=PAIR_WORDS), :] = upper[:, j * LANES:(j + 1) * LANES]
            dx_ref[pl.ds(base + 5 + j, HALF_SEQ, stride=PAIR_WORDS), :] = lower[:, j * LANES:(j + 1) * LANES]
        dx_ref[pl.ds(base + 4, HALF_SEQ, stride=PAIR_WORDS), :] = jnp.concatenate([upper[:, 512:], lower[:, 512:]], axis=1)

    @pl.when(step == steps - 1)
    def _():
        top = lax.broadcasted_iota(jnp.int32, (LANES, 1), 0)
        rows1 = jnp.sum(norm_acc[0], axis=0, keepdims=True)
        rows2 = jnp.sum(norm_acc[1], axis=0, keepdims=True)
        both = jnp.where(top == 0, rows1, 0.0) + jnp.where(top == 1, rows2, 0.0)
        for c in range(0, D, LANES):
            width = min(LANES, D - c)
            acc[c:c + width, C_NORM:C_NORM + LANES] += both[:, c:c + width].T
        head_q = jnp.sum(head_acc[0], axis=0, keepdims=True)
        head_k = jnp.sum(head_acc[1], axis=0, keepdims=True)
        head_row = jnp.where(low, head_q, pltpu.roll(head_k, 64, 1))
        acc[:, C_HEAD:C_HEAD + LANES] += jnp.broadcast_to(head_row, (D, LANES))
        if last:
            mine = core_ref[0]

            def send_block(d, src, keep, send, sem):
                @pl.when(mine == d % 2)
                def _():
                    pltpu.make_async_copy(src, keep.at[d // 2], sem).start()

                @pl.when(mine != d % 2)
                def _():
                    pltpu.make_async_copy(src, send.at[d // 2], sem).start()

                return pltpu.make_async_copy(src, keep.at[d // 2], sem)

            stores = [send_block(d, acc.at[pl.ds(d * 72, 72), :], outs[0], outs[1], sems.at[0]) for d in range(8)]
            for part in range(0, 8, 4):
                moved = []
                for d in range(4):
                    f = (part + d) * 192
                    for t in range(0, D, LANES):
                        width = min(LANES, D - t)
                        tbuf[d * 192:d * 192 + 192, t:t + width] = accd[t:t + width, f:f + 192].T
                    moved.append(send_block(part + d, tbuf.at[pl.ds(d * 192, 192), :], outs[2], outs[3], sems.at[1]))
                for store in moved:
                    store.wait()
        else:
            stores = [pltpu.make_async_copy(acc, outs[0], sems.at[0]), pltpu.make_async_copy(accd, outs[1], sems.at[0])]
            for store in stores:
                store.start()
        for store in stores:
            store.wait()


ROW_WORDS = 5
ACC_WORDS = 6
GROUP_ROWS = 16
PAD_ROWS = 16


def gather_kernel(blocks, ids_ref, tab_ref, *refs):
    outs, (lin, buf) = refs[:-2], refs[-2:]
    step = pl.program_id(0)
    rows = tab_ref.shape[1]

    @pl.when(step == 0)
    def _():
        def build(b, _):
            at = pl.multiple_of(b * LANES, LANES)
            for j in range(ROW_WORDS):
                part = tab_ref[j * LANES:min(j * LANES + LANES, D), pl.ds(at, LANES)].astype(F32)
                if part.shape[0] < LANES:
                    part = jnp.concatenate([part, jnp.zeros((LANES - part.shape[0], LANES), F32)], axis=0)
                lin[pl.ds(at * ROW_WORDS + j, LANES, stride=ROW_WORDS), :] = part.T
            return 0

        lax.fori_loop(0, rows // LANES, build, 0)
        lin[rows * ROW_WORDS:(rows + PAD_ROWS) * ROW_WORDS, :] = jnp.zeros((PAD_ROWS * ROW_WORDS, LANES), F32)

    def pick(k, _):
        base = k * GROUP_ROWS
        got = [lin[pl.ds(ids_ref[step * SEQ + base + u], ROW_WORDS), :] for u in range(GROUP_ROWS)]
        for u in range(GROUP_ROWS):
            buf[pl.ds((base + u) * ROW_WORDS, ROW_WORDS), :] = got[u]
        return 0

    lax.fori_loop(0, SEQ // GROUP_ROWS, pick, 0)
    first = 0
    half = HALF_SEQ * ROW_WORDS
    for out, count in zip(outs, blocks):
        @pl.when((step >= first) & (step < first + count))
        def _():
            for j in range(4):
                out[:, j * LANES:j * LANES + LANES] = buf[pl.ds(j, HALF_SEQ, stride=ROW_WORDS), :].astype(BF)
                out[:, 640 + j * LANES:768 + j * LANES] = buf[pl.ds(half + j, HALF_SEQ, stride=ROW_WORDS), :].astype(BF)
            tails = buf[pl.ds(4, HALF_SEQ, stride=ROW_WORDS), :] + pltpu.roll(buf[pl.ds(half + 4, HALF_SEQ, stride=ROW_WORDS), :], 64, 1)
            out[:, 512:640] = tails.astype(BF)

        first += count


def gather_rows(ids, table_t, blocks):
    starts = [sum(blocks[:c]) for c in range(len(blocks))]
    rows = table_t.shape[1]
    out_spec = lambda c: pl.BlockSpec((HALF_SEQ, 2 * D), lambda i, ids: (jnp.clip(i - starts[c], 0, blocks[c] - 1), 0))
    return pl.pallas_call(
        functools.partial(gather_kernel, blocks),
        grid_spec=pltpu.PrefetchScalarGridSpec(
            num_scalar_prefetch=1,
            grid=(sum(blocks),),
            in_specs=[pl.BlockSpec(table_t.shape, lambda i, ids: (0, 0), pipeline_mode=pl.Buffered(1))],
            out_specs=[out_spec(c) for c in range(len(blocks))],
            scratch_shapes=[pltpu.VMEM(((rows + PAD_ROWS) * ROW_WORDS, LANES), F32), pltpu.VMEM((SEQ * ROW_WORDS, LANES), F32)],
        ),
        out_shape=[jax.ShapeDtypeStruct((count * HALF_SEQ, 2 * D), BF) for count in blocks],
        compiler_params=pltpu.CompilerParams(dimension_semantics=('arbitrary',), vmem_limit_bytes=48 << 20),
        cost_estimate=pl.CostEstimate(flops=40_000_000_000, bytes_accessed=40_000_000, transcendentals=0),
        name='gather_rows',
    )(ids, table_t)


def scatter_kernel(first, last, blocks, ids_ref, clash_ref, rows_ref, *refs):
    if not first:
        acc_in, refs = refs[0], refs[1:]
    out_ref, acc, sem = refs[:3]
    tbuf = refs[3] if last else None
    step = pl.program_id(0)
    rows = acc.shape[0] // ACC_WORDS - PAD_ROWS

    @pl.when(step == 0)
    def _():
        if first:
            acc[...] = jnp.zeros_like(acc)
        else:
            load = pltpu.make_async_copy(acc_in, acc, sem.at[0])
            load.start()
            load.wait()

    groups = SCATTER_ROWS // GROUP_ROWS

    def add(k, _):
        spots = [pl.ds(ids_ref[step * SCATTER_ROWS + u * LANES + k], ROW_WORDS) for u in range(GROUP_ROWS)]
        from_row = lambda u: rows_ref[pl.ds((u // 2 * LANES + k) * PAIR_WORDS + (u % 2) * 4, ROW_WORDS), :]
        clash = clash_ref[step * groups + k]

        @pl.when(clash == 0)
        def _():
            sums = [acc[spots[u], :] + from_row(u) for u in range(GROUP_ROWS)]
            for u in range(GROUP_ROWS):
                acc[spots[u], :] = sums[u]

        @pl.when(clash != 0)
        def _():
            for u in range(GROUP_ROWS):
                acc[spots[u], :] += from_row(u)

        return 0

    lax.fori_loop(0, groups, add, 0)

    @pl.when(step == blocks - 1)
    def _():
        if last:
            wide = FLUSH_ROWS

            def flush(b, _):
                slot = lax.rem(b, 2)
                at = pl.multiple_of(b * wide, wide)
                store = pltpu.make_async_copy(tbuf.at[slot], out_ref.at[:, pl.ds(at, wide)], sem.at[slot])

                @pl.when(b >= 2)
                def _():
                    store.wait()

                word = lambda w, r: acc[pl.ds((at + r) * ACC_WORDS + w, LANES, stride=ACC_WORDS), :]
                for r in range(0, wide, LANES):
                    for j in range(4):
                        tbuf[slot, j * LANES:j * LANES + LANES, r:r + LANES] = word(1 + j, r).T
                    tail = word(5, r) + pltpu.roll(word(0, r), 64, 1)
                    tbuf[slot, 512:D, r:r + LANES] = tail.T[:64]
                store.start()
                return 0

            lax.fori_loop(0, rows // wide, flush, 0)
            for slot in range(2):
                pltpu.make_async_copy(tbuf.at[slot], out_ref.at[:, pl.ds(0, wide)], sem.at[slot]).wait()
        else:
            store = pltpu.make_async_copy(acc, out_ref, sem.at[0])
            store.start()
            store.wait()


SCATTER_ROWS = LANES * GROUP_ROWS
FLUSH_ROWS = 512


def scatter_rows(ids, clash, rows_in, table_rows, carry, last):
    first = carry is None
    blocks = rows_in.shape[0] // (SCATTER_ROWS // 2 * PAIR_WORDS)
    acc_shape = ((table_rows + PAD_ROWS) * ACC_WORDS, LANES)
    anyspec = pl.BlockSpec(memory_space=pl.ANY)
    scratch = [pltpu.VMEM(acc_shape, F32), pltpu.SemaphoreType.DMA((2,))]
    if last:
        scratch.append(pltpu.VMEM((2, D, FLUSH_ROWS), F32))
    return pl.pallas_call(
        functools.partial(scatter_kernel, first, last, blocks),
        grid_spec=pltpu.PrefetchScalarGridSpec(
            num_scalar_prefetch=2,
            grid=(blocks,),
            in_specs=[pl.BlockSpec((SCATTER_ROWS // 2 * PAIR_WORDS, LANES), lambda i, *_: (i, 0))] + ([] if first else [anyspec]),
            out_specs=anyspec,
            scratch_shapes=scratch,
        ),
        out_shape=jax.ShapeDtypeStruct((D, table_rows) if last else acc_shape, F32),
        input_output_aliases={} if first or last else {3: 0},
        compiler_params=pltpu.CompilerParams(dimension_semantics=('arbitrary',), vmem_limit_bytes=48 << 20),
        cost_estimate=pl.CostEstimate(flops=20_000_000_000, bytes_accessed=60_000_000, transcendentals=0),
        name='scatter_rows',
    )(*([ids, clash, rows_in] + ([] if first else [carry])))


def layer_chunk(x, dy, cs, w_pack, w_down, gains, head_gains, core, start, carry, last, total):
    steps = x.shape[0] // (SEQS * HALF_SEQ)
    start = start // SEQS
    first = carry is None
    whole = lambda shape: pl.BlockSpec(shape, lambda i: (0,) * len(shape), pipeline_mode=pl.Buffered(1))
    here = lambda cols: pl.BlockSpec((SEQS * SEQ, cols), lambda i: (i + start, 0))
    anyspec = pl.BlockSpec(memory_space=pl.ANY)
    in_specs = [pl.BlockSpec((SEQS * HALF_SEQ, 2 * D), lambda i: (i, 0)), here(D), here(LANES), whole(w_pack.shape), whole(w_down.shape), whole(gains.shape), whole(head_gains.shape), pl.BlockSpec(memory_space=pltpu.SMEM)]
    args = [x, dy, cs, w_pack, w_down, gains, head_gains, core]
    aliases = {}
    if not first:
        in_specs += [anyspec] * 3
        args += list(carry)
        aliases = {10: 0} if last else {8: 2, 9: 3, 10: 0}
    out_shape = [
        jax.ShapeDtypeStruct((total, D), BF),
        jax.ShapeDtypeStruct((steps * SEQS * HALF_SEQ * PAIR_WORDS, LANES), F32),
    ]
    grad_shapes = [(4, 72, G_COLS)] * 2 + [(4, 192, D)] * 2 if last else [(D, G_COLS), (D, FF)]
    out_shape += [jax.ShapeDtypeStruct(shape, F32) for shape in grad_shapes]
    y, dx, *grads = pl.pallas_call(
        functools.partial(layer_kernel, first, last, steps),
        grid=(steps,),
        in_specs=in_specs,
        out_specs=[here(D), pl.BlockSpec((SEQS * HALF_SEQ * PAIR_WORDS, LANES), lambda i: (i, 0))] + [anyspec] * len(grad_shapes),
        out_shape=out_shape,
        scratch_shapes=[
            pltpu.VMEM((D, G_COLS), F32),
            pltpu.VMEM((D, FF), F32),
            pltpu.VMEM((2, 8, D), F32),
            pltpu.VMEM((2, 8, LANES), F32),
            pltpu.VMEM((D, X_COLS), BF),
            pltpu.VMEM((HEADS * LANES, D), BF),
            pltpu.VMEM((SEQS * SEQ, X_COLS), BF),
            pltpu.VMEM((SEQS * KV, GRP * HALF_SEQ, HALF_SEQ), F32),
            pltpu.VMEM((SEQS * KV, GRP * HALF_SEQ, SEQ), F32),
            pltpu.VMEM((FF // 2, D) if last else (8, LANES), F32),
            pltpu.SemaphoreType.DMA((2,)),
        ],
        input_output_aliases=aliases,
        compiler_params=pltpu.CompilerParams(dimension_semantics=('arbitrary',), vmem_limit_bytes=62 << 20),
        cost_estimate=pl.CostEstimate(flops=steps * SEQS * 6_000_000_000, bytes_accessed=steps * SEQS * 2_500_000 + 45_000_000, transcendentals=steps * SEQS * 1_000_000),
        name='layer_chunk',
    )(*args)
    return dx, (*grads, y)


def swap_with(bit, values):
    return lax.ppermute(values, AXIS_NAME, [(i, i ^ bit) for i in range(8)])


def gather_by_swaps(shard):
    index = lax.axis_index(AXIS_NAME)
    for bit in (1, 2, 4):
        got = swap_with(bit, shard)
        second = (index // bit) % 2 == 1
        shard = jnp.where(second, jnp.concatenate([got, shard], axis=0), jnp.concatenate([shard, got], axis=0))
    return shard


def reduce_by_swaps(kept, sent, axis, cut):
    index = lax.axis_index(AXIS_NAME)
    x, y = (index // 2) % 2, index // 4
    at = lambda values, axis, idx: lax.dynamic_index_in_dim(values, idx, axis, keepdims=False)
    got = swap_with(1, sent)
    summed = (kept + got).reshape(2, 2, *kept.shape[1:])
    one, two = lax.slice_in_dim(summed, 0, cut, axis=axis), lax.slice_in_dim(summed, cut, summed.shape[axis], axis=axis)
    one_got, two_got = swap_with(2, at(one, 1, 1 - x)), swap_with(4, at(two, 0, 1 - y))
    one, two = at(one, 1, x) + one_got, at(two, 0, y) + two_got
    one_got, two_got = swap_with(4, at(one, 0, 1 - y)), swap_with(2, at(two, 0, 1 - x))
    return jnp.concatenate([at(one, 0, y) + one_got, at(two, 0, x) + two_got], axis=axis)


def solution(mesh):
    row_spec = P(AXIS_NAME, None)
    vec_spec = P(AXIS_NAME)
    full_spec = P(None)
    batch_spec = P(AXIS_NAME, None, None)
    weight_specs = (vec_spec, row_spec, row_spec, row_spec, full_spec, full_spec, row_spec, vec_spec, row_spec, row_spec, row_spec)

    def device_step(tokens, positions, table_shard, attn_norm, w_query, w_key, w_value, q_norm, k_norm, w_out, mlp_norm, w_gate, w_up, w_down, dy_out):
        batch_len, seq_len = tokens.shape
        devices = lax.axis_size(AXIS_NAME)
        rows_local = table_shard.shape[0]
        shard = w_query.shape[0]
        all_ids = lax.all_gather(tokens, AXIS_NAME)
        norms = jnp.concatenate([attn_norm[:, None], mlp_norm[:, None], jnp.zeros((shard, W_COLS - C_NORM - 2), BF)], axis=1)
        pad = jnp.zeros((shard, 64), BF)
        packed = jnp.concatenate([w_query, w_key, w_value, pad, w_out, pad, w_gate, w_up, norms], axis=1)
        w_pack = lax.all_gather(packed, AXIS_NAME, tiled=True)
        w_down_full = gather_by_swaps(w_down)
        gains = w_pack[:, C_NORM:C_NORM + 2].T.astype(F32)
        head_gains = jnp.stack([q_norm, k_norm]).astype(F32)
        swapped = jnp.concatenate([head_gains[:, 32:], head_gains[:, :32]], axis=1)
        head_gains = jnp.concatenate([head_gains, swapped], axis=1)

        inv_freq = jnp.exp(jnp.arange(HEAD // 2, dtype=F32) * (-2.0 * math.log(ROPE_THETA) / HEAD))
        angles = positions.reshape(-1, 1).astype(F32) * inv_freq
        cos_t, sin_t = jnp.cos(angles), jnp.sin(angles)
        cs = jnp.concatenate([cos_t, cos_t, -sin_t, sin_t], axis=1)
        dy = dy_out.reshape(-1, D)

        starts = [sum(CHUNKS[:c]) for c in range(len(CHUNKS))]
        take_from, add_to, clashes = [], [], []
        for first, size in zip(starts, CHUNKS):
            local_ids = all_ids[:, first:first + size].reshape(-1, LANES) - lax.axis_index(AXIS_NAME) * rows_local
            is_owner = (local_ids >= 0) & (local_ids < rows_local)
            line = lax.broadcasted_iota(jnp.int32, local_ids.shape, 0)
            take_from.append((jnp.where(is_owner, local_ids, rows_local) * ROW_WORDS).reshape(-1))
            spot = jnp.where(is_owner, local_ids, rows_local + line % GROUP_ROWS)
            add_to.append((spot * ACC_WORDS + 1 - line % 2).reshape(-1))
            groups = spot.reshape(-1, GROUP_ROWS, LANES)
            twice = jnp.concatenate([groups, groups], axis=1)
            same = [jnp.any(groups == twice[:, shift:shift + GROUP_ROWS], axis=1) for shift in range(1, GROUP_ROWS // 2 + 1)]
            clashes.append(functools.reduce(jnp.logical_or, same).astype(jnp.int32).reshape(-1))

        table_t = table_shard.T
        parity = lax.axis_index(AXIS_NAME) % 2
        *mids, last_ids = take_from[1:]
        by_core = last_ids.reshape(devices // 2, 2, -1)
        kept = jnp.where(parity == 0, by_core[:, 0], by_core[:, 1]).reshape(-1)
        sent = jnp.where(parity == 0, by_core[:, 1], by_core[:, 0]).reshape(-1)
        picked = gather_rows(take_from[0], table_t, (devices * CHUNKS[0],))
        half_rows = devices // 2 * CHUNKS[-1]
        picked += gather_rows(jnp.concatenate(mids + [kept, sent]), table_t, tuple(devices * n for n in CHUNKS[1:-1]) + (half_rows, half_rows))
        *picked, kept, sent = picked
        xs = [lax.psum_scatter(rows, AXIS_NAME, scatter_dimension=0, tiled=True) for rows in picked]
        pair_rows = CHUNKS[-1] * HALF_SEQ
        split = lambda rows: rows.reshape(devices // 2, pair_rows, 2 * D)
        xs.append(reduce_by_swaps(split(kept), split(sent), -2, pair_rows // 2))
        core = lax.rem(lax.axis_index(AXIS_NAME), 2).reshape(1)
        carry = None
        rows_of = []
        for idx in range(len(CHUNKS)):
            x_chunk = xs[idx]
            dx, carry = layer_chunk(x_chunk, dy, cs, w_pack, w_down_full, gains, head_gains, core, starts[idx], carry, idx == len(CHUNKS) - 1, batch_len * seq_len)
            rows_of.append(lax.all_gather(dx, AXIS_NAME, tiled=True))
        *grads, y = carry
        d_table = None
        for idx in range(len(CHUNKS)):
            d_table = scatter_rows(add_to[idx], clashes[idx], rows_of[idx], rows_local, d_table, idx == len(CHUNKS) - 1)
        d_table = d_table.T
        g_pack = reduce_by_swaps(grads[0], grads[1], -1, 2560)
        d_w_down = reduce_by_swaps(grads[2], grads[3], -2, 96)
        kv_cols = w_key.shape[1]
        return (y.reshape(batch_len, seq_len, D), d_table, g_pack[:, C_NORM], g_pack[:, :D], g_pack[:, D:D + kv_cols], g_pack[:, D + kv_cols:D + 2 * kv_cols],
                g_pack[0, C_HEAD:C_HEAD + HEAD], g_pack[0, C_HEAD + HEAD:C_HEAD + 2 * HEAD], g_pack[:, C_OUT:C_OUT + D], g_pack[:, C_NORM + 1],
                g_pack[:, C_GATE:C_GATE + FF], g_pack[:, C_UP:C_UP + FF], d_w_down)

    return jax.shard_map(device_step, mesh=mesh, in_specs=(row_spec, row_spec, row_spec) + weight_specs + (batch_spec,), out_specs=(batch_spec, row_spec) + weight_specs, check_vma=False)
```

```python
import functools
import math
import jax
import jax.numpy as jnp
from jax import lax
from jax.experimental import pallas as pl
from jax.experimental.pallas import tpu as pltpu
from jax.sharding import PartitionSpec as P

NORM_EPS = 1e-6
ROPE_THETA = 1.0e6
AXIS_NAME = 'fsdp'
SEQ = 256
HALF_SEQ = SEQ // 2
SEQS = 1
LANES = 128
D = 576
FF = 1536
HEAD = 64
HEADS = 9
KV = 3
GRP = 3
C_OUT, C_GATE, C_UP, C_NORM, C_HEAD = 1024, 1664, 3200, 4736, 4864
W_COLS, G_COLS = 4864, 4992
X_K, X_V, X_COLS = HEADS * LANES, (HEADS + KV) * LANES, (HEADS + 2 * KV) * LANES
FF_STEP = 512
CHUNKS = (4, 4, 4)
PAIR_WORDS = 9
BF, F32 = jnp.bfloat16, jnp.float32


def mm(lhs, rhs, lhs_dim=1, rhs_dim=0):
    return lax.dot_general(lhs, rhs, (((lhs_dim,), (rhs_dim,)), ((), ())), preferred_element_type=F32)


def fold8(values):
    return jnp.sum(values.reshape(values.shape[0] // 8, 8, values.shape[1]), axis=0)


def norm_bwd(grad_out, normed, inv_rms, norm_gain):
    grad_normed = grad_out * norm_gain
    return inv_rms * (grad_normed - normed * jnp.mean(grad_normed * normed, axis=-1, keepdims=True))


def head_norm_rope(head_ext, gain_ext, cs):
    head_f = head_ext.astype(F32)
    inv = lax.rsqrt(jnp.sum(head_f * head_f, axis=-1, keepdims=True) * (1.0 / LANES) + NORM_EPS)
    turned = head_f * inv * gain_ext * cs
    return turned + pltpu.roll(turned, HEAD, 1), inv


def head_norm_rope_bwd(grad_ext, head_ext, inv, gain_low, cs_bwd, low):
    turned = grad_ext * cs_bwd
    grad_t = turned + pltpu.roll(turned, HEAD, 1)
    normed = jnp.where(low, head_ext.astype(F32), 0.0) * inv
    grad_normed = grad_t * gain_low
    mean_term = jnp.sum(grad_normed * normed, axis=-1, keepdims=True) * (1.0 / HEAD)
    return inv * (grad_normed - normed * mean_term), fold8(grad_t * normed)


def pack_pairs(heads):
    tiles = []
    for idx in range(0, len(heads), 2):
        tile = heads[idx]
        if idx + 1 < len(heads):
            tile = tile + pltpu.roll(heads[idx + 1], HEAD, 1)
        tiles.append(tile.astype(BF))
    return tiles


def layer_kernel(first, last, steps, *refs):
    (x_ref, dy_ref, cs_ref, w_ref, wd_ref, gains_ref, head_gains_ref, core_ref) = refs[:8]
    refs = refs[8:]
    if not first:
        acc_in, accd_in, _ = refs[:3]
        refs = refs[3:]
    y_ref, dx_ref = refs[:2]
    outs = refs[2:6] if last else refs[2:4]
    (acc, accd, norm_acc, head_acc, wx, wox, qkv_s, upper_s, lower_s, cs_s, tbuf, sems) = refs[2 + len(outs):]
    step = pl.program_id(0)
    low = lax.broadcasted_iota(jnp.int32, (1, LANES), 1) < HEAD

    @pl.when(step == 0)
    def _():
        if first:
            acc[...] = jnp.zeros_like(acc)
            accd[...] = jnp.zeros_like(accd)
        else:
            load_acc = pltpu.make_async_copy(acc_in, acc, sems.at[0])
            load_accd = pltpu.make_async_copy(accd_in, accd, sems.at[1])
            load_acc.start()
            load_accd.start()
        norm_acc[...] = jnp.zeros_like(norm_acc)
        head_acc[...] = jnp.zeros_like(head_acc)
        for h in range(HEADS + 2 * KV):
            tile = w_ref[:, (h // 2) * LANES:(h // 2) * LANES + LANES].astype(F32)
            moved = pltpu.roll(tile, HEAD, 1)
            if h >= HEADS + KV:
                both = jnp.where(low, moved if h % 2 else tile, 0.0)
            else:
                twice = jnp.where(low, moved, tile) if h % 2 else jnp.where(low, tile, moved)
                both = jnp.where(low, twice, pltpu.roll(twice, 32, 1))
            wx[:, h * LANES:h * LANES + LANES] = both.astype(BF)
        for h in range(HEADS):
            wox[h * LANES:h * LANES + HEAD, :] = w_ref[h * HEAD:h * HEAD + HEAD, C_OUT:C_OUT + D]
            wox[h * LANES + HEAD:h * LANES + LANES, :] = jnp.zeros((HEAD, D), BF)
        if not first:
            load_acc.wait()
            load_accd.wait()

    gain1 = gains_ref[0:1, :]
    gain2 = gains_ref[1:2, :]
    gain_q, gain_k = head_gains_ref[0:1, :], head_gains_ref[1:2, :]
    low_q, low_k = jnp.where(low, gain_q, 0.0), jnp.where(low, gain_k, 0.0)
    scale = HEAD ** -0.5
    stacked = GRP * HALF_SEQ
    row = lax.broadcasted_iota(jnp.int32, (stacked, SEQ), 0) & (HALF_SEQ - 1)
    lower_mask = lax.broadcasted_iota(jnp.int32, (stacked, SEQ), 1) - HALF_SEQ <= row
    upper_mask = lower_mask[:, HALF_SEQ:]

    def halves(tiles):
        return jnp.concatenate([t[:HALF_SEQ] for t in tiles], axis=0), jnp.concatenate([t[HALF_SEQ:] for t in tiles], axis=0)

    def joined(upper, lower, r):
        return jnp.concatenate([part[r * HALF_SEQ:(r + 1) * HALF_SEQ] for part in (upper, lower)], axis=0)

    def softmax(scores, mask):
        scores = jnp.where(mask, scores, -1e30)
        expd = jnp.exp(scores - jnp.max(scores, axis=-1, keepdims=True))
        return expd * (1.0 / jnp.sum(expd, axis=-1, keepdims=True))

    cos_t, sin_t = cs_ref[:HEAD // 2, :], cs_ref[HEAD // 2:, :]
    cs_s[...] = jnp.concatenate([cos_t, cos_t, -sin_t, sin_t], axis=0).T

    parts = []
    for s in range(SEQS):
        pairs = x_ref[s * HALF_SEQ:(s + 1) * HALF_SEQ, :].astype(F32)
        tails = pairs[:, 512:640]
        parts.append(jnp.concatenate([pairs[:, :512], tails[:, :HEAD]], axis=1))
        parts.append(jnp.concatenate([pairs[:, 640:], pltpu.roll(tails, HEAD, 1)[:, :HEAD]], axis=1))
    x = jnp.concatenate(parts, axis=0)
    inv1 = lax.rsqrt(jnp.mean(x * x, axis=-1, keepdims=True) + NORM_EPS)
    m1 = (x * inv1 * gain1).astype(BF)
    qkv_s[...] = mm(m1, wx[...]).astype(BF)
    saved, packed = [], []
    for s in range(SEQS):
        rows = slice(s * SEQ, (s + 1) * SEQ)
        cs = cs_s[...]
        heads = []
        for g in range(KV):
            ke = qkv_s[rows, X_K + g * LANES:X_K + (g + 1) * LANES]
            v0 = qkv_s[rows, X_V + g * LANES:X_V + (g + 1) * LANES]
            k_rot, k_inv = head_norm_rope(ke, gain_k, cs)
            k0 = jnp.where(low, k_rot, 0.0).astype(BF)
            k_swap = (jnp.where(low, k_rot, pltpu.roll(k_rot, 32, 1)) * scale).astype(BF)
            qs, q_swaps, q_invs = [], [], []
            for r in range(GRP):
                h = g * GRP + r
                q_rot, q_inv = head_norm_rope(qkv_s[rows, h * LANES:(h + 1) * LANES], gain_q, cs * scale)
                qs.append(q_rot.astype(BF))
                q_swaps.append(jnp.where(low, q_rot, pltpu.roll(q_rot, 32, 1)).astype(BF))
                q_invs.append(q_inv)
            q_upper, q_lower = halves(qs)
            upper = softmax(mm(q_upper, k0[:HALF_SEQ], 1, 1), upper_mask)
            lower = softmax(mm(q_lower, k0, 1, 1), lower_mask)
            upper_s[s * KV + g] = upper
            lower_s[s * KV + g] = lower
            o_upper, o_lower = mm(upper.astype(BF), v0[:HALF_SEQ]), mm(lower.astype(BF), v0)
            heads += [joined(o_upper, o_lower, r) for r in range(GRP)]
            saved.append((k_swap, halves(q_swaps), q_invs, k_inv))
        packed.append(jnp.concatenate(pack_pairs(heads), axis=1))
    attn = jnp.concatenate(packed, axis=0)
    hidden_b = (x + mm(attn[:, :D], w_ref[:, C_OUT:C_OUT + D])).astype(BF)
    hidden = hidden_b.astype(F32)
    inv2 = lax.rsqrt(jnp.mean(hidden * hidden, axis=-1, keepdims=True) + NORM_EPS)
    m2 = (hidden * inv2 * gain2).astype(BF)

    dy_t = dy_ref[...]
    dy = dy_t.T
    m2_t = m2.T
    y = hidden
    dm2 = jnp.zeros((SEQS * SEQ, D), F32)
    for f in range(0, FF, FF_STEP):
        wg = w_ref[:, C_GATE + f:C_GATE + f + FF_STEP]
        wu = w_ref[:, C_UP + f:C_UP + f + FF_STEP]
        wd = wd_ref[f:f + FF_STEP, :]
        gate = mm(m2, wg)
        up = mm(m2, wu)
        dact = mm(dy, wd, 1, 1)
        sig = 1.0 / (1.0 + jnp.exp(-gate))
        silu = gate * sig
        act = (silu * up).astype(BF)
        y = y + mm(act, wd)
        dgate = (dact * up * sig * (1.0 + gate * (1.0 - sig))).astype(BF)
        dup = (dact * silu).astype(BF)
        dm2 = dm2 + mm(dgate, wg, 1, 1) + mm(dup, wu, 1, 1)
        acc[:, C_GATE + f:C_GATE + f + FF_STEP] += mm(m2_t, dgate)
        acc[:, C_UP + f:C_UP + f + FF_STEP] += mm(m2_t, dup)
        accd[:, f:f + FF_STEP] += mm(dy_t, act)
    y_ref[...] = y.astype(BF)
    n2 = hidden * inv2
    norm_acc[1] += fold8(dm2 * n2)
    dh = dy.astype(F32) + norm_bwd(dm2, n2, inv2, gain2)
    dh_b = dh.astype(BF)
    acc[:, C_OUT:C_OUT + D] += mm(attn.T, dh_b)[:D]

    do = mm(dh_b, wox[...], 1, 1).astype(BF)
    packed = []
    for s in range(SEQS):
        rows = slice(s * SEQ, (s + 1) * SEQ)
        cs = cs_s[...]
        cs_bwd = jnp.where(low, cs, -cs)
        dqs, dks, dvs = [], [], []
        for g in range(KV):
            k_swap, (swap_upper, swap_lower), q_invs, k_inv = saved[s * KV + g]
            v0 = qkv_s[rows, X_V + g * LANES:X_V + (g + 1) * LANES]
            do_upper, do_lower = halves([do[rows, h * LANES:(h + 1) * LANES] for h in range(g * GRP, (g + 1) * GRP)])
            upper, lower = upper_s[s * KV + g], lower_s[s * KV + g]
            d_upper, d_lower = mm(do_upper, v0[:HALF_SEQ], 1, 1), mm(do_lower, v0, 1, 1)
            ds_upper = (upper * (d_upper - jnp.sum(d_upper * upper, axis=-1, keepdims=True))).astype(BF)
            ds_lower = (lower * (d_lower - jnp.sum(d_lower * lower, axis=-1, keepdims=True))).astype(BF)

            def over_queries(left_upper, left_lower, right_upper, right_lower):
                short, full = mm(left_upper.T, right_upper), mm(left_lower.T, right_lower)
                return jnp.concatenate([(full[:, :HALF_SEQ] + short).T, full[:, HALF_SEQ:].T], axis=0)

            dvs.append(over_queries(do_upper, do_lower, upper.astype(BF), lower.astype(BF)))
            dk = over_queries(swap_upper, swap_lower, ds_upper, ds_lower)
            dk, dk_gain = head_norm_rope_bwd(dk, qkv_s[rows, X_K + g * LANES:X_K + (g + 1) * LANES], k_inv, low_k, cs_bwd, low)
            dks.append(dk)
            head_acc[1] += dk_gain
            dq_upper, dq_lower = mm(ds_upper, k_swap[:HALF_SEQ]), mm(ds_lower, k_swap)
            for r in range(GRP):
                h = g * GRP + r
                dq_h, dq_gain = head_norm_rope_bwd(joined(dq_upper, dq_lower, r), qkv_s[rows, h * LANES:(h + 1) * LANES], q_invs[r], low_q, cs_bwd, low)
                dqs.append(dq_h)
                head_acc[0] += dq_gain
        packed.append(jnp.concatenate(pack_pairs(dqs + dks + dvs), axis=1))
    dqkv = jnp.concatenate(packed, axis=0)
    acc[:, 0:1024] += mm(m1.T, dqkv)
    dm1 = mm(dqkv, w_ref[:, 0:1024], 1, 1)
    n1 = x * inv1
    norm_acc[0] += fold8(dm1 * n1)
    dx = dh + norm_bwd(dm1, n1, inv1, gain1)
    for s in range(SEQS):
        upper, lower = dx[s * SEQ:s * SEQ + HALF_SEQ], dx[s * SEQ + HALF_SEQ:(s + 1) * SEQ]
        base = s * HALF_SEQ * PAIR_WORDS
        for j in range(4):
            dx_ref[pl.ds(base + j, HALF_SEQ, stride=PAIR_WORDS), :] = upper[:, j * LANES:(j + 1) * LANES]
            dx_ref[pl.ds(base + 5 + j, HALF_SEQ, stride=PAIR_WORDS), :] = lower[:, j * LANES:(j + 1) * LANES]
        dx_ref[pl.ds(base + 4, HALF_SEQ, stride=PAIR_WORDS), :] = jnp.concatenate([upper[:, 512:], lower[:, 512:]], axis=1)

    @pl.when(step == steps - 1)
    def _():
        top = lax.broadcasted_iota(jnp.int32, (LANES, 1), 0)
        rows1 = jnp.sum(norm_acc[0], axis=0, keepdims=True)
        rows2 = jnp.sum(norm_acc[1], axis=0, keepdims=True)
        both = jnp.where(top == 0, rows1, 0.0) + jnp.where(top == 1, rows2, 0.0)
        for c in range(0, D, LANES):
            width = min(LANES, D - c)
            acc[c:c + width, C_NORM:C_NORM + LANES] += both[:, c:c + width].T
        head_q = jnp.sum(head_acc[0], axis=0, keepdims=True)
        head_k = jnp.sum(head_acc[1], axis=0, keepdims=True)
        head_row = jnp.where(low, head_q, pltpu.roll(head_k, HEAD, 1))
        acc[:, C_HEAD:C_HEAD + LANES] += jnp.broadcast_to(head_row, (D, LANES))
        if last:
            mine = core_ref[0]

            def send_block(d, src, keep, send, sem):
                @pl.when(mine == d % 2)
                def _():
                    pltpu.make_async_copy(src, keep.at[d // 2], sem).start()

                @pl.when(mine != d % 2)
                def _():
                    pltpu.make_async_copy(src, send.at[d // 2], sem).start()

                return pltpu.make_async_copy(src, keep.at[d // 2], sem)

            stores = [send_block(d, acc.at[pl.ds(d * 72, 72), :], outs[0], outs[1], sems.at[0]) for d in range(8)]
            for part in range(0, 8, 4):
                moved = []
                for d in range(4):
                    f = (part + d) * 192
                    for t in range(0, D, LANES):
                        width = min(LANES, D - t)
                        tbuf[d * 192:d * 192 + 192, t:t + width] = accd[t:t + width, f:f + 192].T
                    moved.append(send_block(part + d, tbuf.at[pl.ds(d * 192, 192), :], outs[2], outs[3], sems.at[1]))
                for store in moved:
                    store.wait()
        else:
            stores = [pltpu.make_async_copy(acc, outs[0], sems.at[0]), pltpu.make_async_copy(accd, outs[1], sems.at[0])]
            for store in stores:
                store.start()
        for store in stores:
            store.wait()


ROW_WORDS = 5
ACC_WORDS = 6
GROUP_ROWS = 16
PAD_ROWS = 16


def gather_kernel(blocks, ids_ref, tab_ref, *refs):
    outs, (lin, buf) = refs[:-2], refs[-2:]
    step = pl.program_id(0)
    rows = tab_ref.shape[1]

    @pl.when(step == 0)
    def _():
        def build(b, _):
            at = pl.multiple_of(b * LANES, LANES)
            for j in range(ROW_WORDS):
                part = tab_ref[j * LANES:min(j * LANES + LANES, D), pl.ds(at, LANES)].astype(F32)
                if part.shape[0] < LANES:
                    part = jnp.concatenate([part, jnp.zeros((LANES - part.shape[0], LANES), F32)], axis=0)
                lin[pl.ds(at * ROW_WORDS + j, LANES, stride=ROW_WORDS), :] = part.T
            return 0

        lax.fori_loop(0, rows // LANES, build, 0)
        lin[rows * ROW_WORDS:(rows + PAD_ROWS) * ROW_WORDS, :] = jnp.zeros((PAD_ROWS * ROW_WORDS, LANES), F32)

    def pick(k, _):
        base = k * GROUP_ROWS
        got = [lin[pl.ds(ids_ref[step * SEQ + base + u], ROW_WORDS), :] for u in range(GROUP_ROWS)]
        for u in range(GROUP_ROWS):
            buf[pl.ds((base + u) * ROW_WORDS, ROW_WORDS), :] = got[u]
        return 0

    lax.fori_loop(0, SEQ // GROUP_ROWS, pick, 0)
    first = 0
    half = HALF_SEQ * ROW_WORDS
    for out, count in zip(outs, blocks):
        @pl.when((step >= first) & (step < first + count))
        def _():
            for j in range(4):
                out[:, j * LANES:j * LANES + LANES] = buf[pl.ds(j, HALF_SEQ, stride=ROW_WORDS), :].astype(BF)
                out[:, 640 + j * LANES:768 + j * LANES] = buf[pl.ds(half + j, HALF_SEQ, stride=ROW_WORDS), :].astype(BF)
            tails = buf[pl.ds(4, HALF_SEQ, stride=ROW_WORDS), :] + pltpu.roll(buf[pl.ds(half + 4, HALF_SEQ, stride=ROW_WORDS), :], HEAD, 1)
            out[:, 512:640] = tails.astype(BF)

        first += count


def gather_rows(ids, table_t, blocks):
    starts = [sum(blocks[:c]) for c in range(len(blocks))]
    rows = table_t.shape[1]
    out_spec = lambda c: pl.BlockSpec((HALF_SEQ, 2 * D), lambda i, ids: (jnp.clip(i - starts[c], 0, blocks[c] - 1), 0))
    return pl.pallas_call(
        functools.partial(gather_kernel, blocks),
        grid_spec=pltpu.PrefetchScalarGridSpec(
            num_scalar_prefetch=1,
            grid=(sum(blocks),),
            in_specs=[pl.BlockSpec(table_t.shape, lambda i, ids: (0, 0), pipeline_mode=pl.Buffered(1))],
            out_specs=[out_spec(c) for c in range(len(blocks))],
            scratch_shapes=[pltpu.VMEM(((rows + PAD_ROWS) * ROW_WORDS, LANES), F32), pltpu.VMEM((SEQ * ROW_WORDS, LANES), F32)],
        ),
        out_shape=[jax.ShapeDtypeStruct((count * HALF_SEQ, 2 * D), BF) for count in blocks],
        compiler_params=pltpu.CompilerParams(dimension_semantics=('arbitrary',), vmem_limit_bytes=48 << 20),
        cost_estimate=pl.CostEstimate(flops=40_000_000_000, bytes_accessed=40_000_000, transcendentals=0),
        name='gather_rows',
    )(ids, table_t)


def scatter_kernel(first, last, blocks, ids_ref, clash_ref, rows_ref, *refs):
    if not first:
        acc_in, refs = refs[0], refs[1:]
    out_ref, acc, sem = refs[:3]
    tbuf = refs[3] if last else None
    step = pl.program_id(0)
    rows = acc.shape[0] // ACC_WORDS - PAD_ROWS

    @pl.when(step == 0)
    def _():
        if first:
            acc[...] = jnp.zeros_like(acc)
        else:
            load = pltpu.make_async_copy(acc_in, acc, sem.at[0])
            load.start()
            load.wait()

    groups = SCATTER_ROWS // GROUP_ROWS

    def add(k, _):
        spots = [pl.ds(ids_ref[step * SCATTER_ROWS + u * LANES + k], ROW_WORDS) for u in range(GROUP_ROWS)]
        from_row = lambda u: rows_ref[pl.ds((u // 2 * LANES + k) * PAIR_WORDS + (u % 2) * 4, ROW_WORDS), :]
        clash = clash_ref[step * groups + k]

        @pl.when(clash == 0)
        def _():
            sums = [acc[spots[u], :] + from_row(u) for u in range(GROUP_ROWS)]
            for u in range(GROUP_ROWS):
                acc[spots[u], :] = sums[u]

        @pl.when(clash != 0)
        def _():
            for u in range(GROUP_ROWS):
                acc[spots[u], :] += from_row(u)

        return 0

    lax.fori_loop(0, groups, add, 0)

    @pl.when(step == blocks - 1)
    def _():
        if last:
            wide = FLUSH_ROWS

            def flush(b, _):
                slot = lax.rem(b, 2)
                at = pl.multiple_of(b * wide, wide)
                store = pltpu.make_async_copy(tbuf.at[slot], out_ref.at[:, pl.ds(at, wide)], sem.at[slot])

                @pl.when(b >= 2)
                def _():
                    store.wait()

                word = lambda w, r: acc[pl.ds((at + r) * ACC_WORDS + w, LANES, stride=ACC_WORDS), :]
                for r in range(0, wide, LANES):
                    for j in range(4):
                        tbuf[slot, j * LANES:j * LANES + LANES, r:r + LANES] = word(1 + j, r).T
                    tail = word(5, r) + pltpu.roll(word(0, r), HEAD, 1)
                    tbuf[slot, 512:D, r:r + LANES] = tail.T[:HEAD]
                store.start()
                return 0

            lax.fori_loop(0, rows // wide, flush, 0)
            for slot in range(2):
                pltpu.make_async_copy(tbuf.at[slot], out_ref.at[:, pl.ds(0, wide)], sem.at[slot]).wait()
        else:
            store = pltpu.make_async_copy(acc, out_ref, sem.at[0])
            store.start()
            store.wait()


SCATTER_ROWS = LANES * GROUP_ROWS
FLUSH_ROWS = 512


def scatter_rows(ids, clash, rows_in, table_rows, carry, last):
    first = carry is None
    blocks = rows_in.shape[0] // (SCATTER_ROWS // 2 * PAIR_WORDS)
    acc_shape = ((table_rows + PAD_ROWS) * ACC_WORDS, LANES)
    anyspec = pl.BlockSpec(memory_space=pl.ANY)
    scratch = [pltpu.VMEM(acc_shape, F32), pltpu.SemaphoreType.DMA((2,))]
    if last:
        scratch.append(pltpu.VMEM((2, D, FLUSH_ROWS), F32))
    return pl.pallas_call(
        functools.partial(scatter_kernel, first, last, blocks),
        grid_spec=pltpu.PrefetchScalarGridSpec(
            num_scalar_prefetch=2,
            grid=(blocks,),
            in_specs=[pl.BlockSpec((SCATTER_ROWS // 2 * PAIR_WORDS, LANES), lambda i, *_: (i, 0))] + ([] if first else [anyspec]),
            out_specs=anyspec,
            scratch_shapes=scratch,
        ),
        out_shape=jax.ShapeDtypeStruct((D, table_rows) if last else acc_shape, F32),
        input_output_aliases={} if first or last else {3: 0},
        compiler_params=pltpu.CompilerParams(dimension_semantics=('arbitrary',), vmem_limit_bytes=48 << 20),
        cost_estimate=pl.CostEstimate(flops=20_000_000_000, bytes_accessed=60_000_000, transcendentals=0),
        name='scatter_rows',
    )(*([ids, clash, rows_in] + ([] if first else [carry])))


def layer_chunk(x, dy, cs, w_pack, w_down, gains, head_gains, core, start, carry, last, total):
    steps = x.shape[0] // (SEQS * HALF_SEQ)
    start = start // SEQS
    first = carry is None
    whole = lambda shape: pl.BlockSpec(shape, lambda i: (0,) * len(shape), pipeline_mode=pl.Buffered(1))
    here = lambda cols: pl.BlockSpec((SEQS * SEQ, cols), lambda i: (i + start, 0))
    anyspec = pl.BlockSpec(memory_space=pl.ANY)
    in_specs = [pl.BlockSpec((SEQS * HALF_SEQ, 2 * D), lambda i: (i, 0)), pl.BlockSpec((D, SEQ), lambda i: (i + start, 0)), pl.BlockSpec((HEAD, SEQ), lambda i: (0, i + start)), whole(w_pack.shape), whole(w_down.shape), whole(gains.shape), whole(head_gains.shape), pl.BlockSpec(memory_space=pltpu.SMEM)]
    args = [x, dy, cs, w_pack, w_down, gains, head_gains, core]
    aliases = {}
    if not first:
        in_specs += [anyspec] * 3
        args += list(carry)
        aliases = {10: 0} if last else {8: 2, 9: 3, 10: 0}
    out_shape = [
        jax.ShapeDtypeStruct((total, D), BF),
        jax.ShapeDtypeStruct((steps * SEQS * HALF_SEQ * PAIR_WORDS, LANES), F32),
    ]
    grad_shapes = [(4, 72, G_COLS)] * 2 + [(4, 192, D)] * 2 if last else [(D, G_COLS), (D, FF)]
    out_shape += [jax.ShapeDtypeStruct(shape, F32) for shape in grad_shapes]
    y, dx, *grads = pl.pallas_call(
        functools.partial(layer_kernel, first, last, steps),
        grid=(steps,),
        in_specs=in_specs,
        out_specs=[here(D), pl.BlockSpec((SEQS * HALF_SEQ * PAIR_WORDS, LANES), lambda i: (i, 0))] + [anyspec] * len(grad_shapes),
        out_shape=out_shape,
        scratch_shapes=[
            pltpu.VMEM((D, G_COLS), F32),
            pltpu.VMEM((D, FF), F32),
            pltpu.VMEM((2, 8, D), F32),
            pltpu.VMEM((2, 8, LANES), F32),
            pltpu.VMEM((D, X_COLS), BF),
            pltpu.VMEM((HEADS * LANES, D), BF),
            pltpu.VMEM((SEQS * SEQ, X_COLS), BF),
            pltpu.VMEM((SEQS * KV, GRP * HALF_SEQ, HALF_SEQ), F32),
            pltpu.VMEM((SEQS * KV, GRP * HALF_SEQ, SEQ), F32),
            pltpu.VMEM((SEQ, LANES), F32),
            pltpu.VMEM((FF // 2, D) if last else (8, LANES), F32),
            pltpu.SemaphoreType.DMA((2,)),
        ],
        input_output_aliases=aliases,
        compiler_params=pltpu.CompilerParams(dimension_semantics=('arbitrary',), vmem_limit_bytes=62 << 20),
        cost_estimate=pl.CostEstimate(flops=steps * SEQS * 6_000_000_000, bytes_accessed=steps * SEQS * 2_500_000 + 45_000_000, transcendentals=steps * SEQS * 1_000_000),
        name='layer_chunk',
    )(*args)
    return dx, (*grads, y)


def swap_with(bit, values):
    return lax.ppermute(values, AXIS_NAME, [(i, i ^ bit) for i in range(8)])


def gather_by_swaps(shard):
    index = lax.axis_index(AXIS_NAME)
    for bit in (1, 2, 4):
        got = swap_with(bit, shard)
        second = (index // bit) % 2 == 1
        shard = jnp.where(second, jnp.concatenate([got, shard], axis=0), jnp.concatenate([shard, got], axis=0))
    return shard


def reduce_by_swaps(kept, sent, axis, cut):
    index = lax.axis_index(AXIS_NAME)
    x, y = (index // 2) % 2, index // 4
    at = lambda values, axis, idx: lax.dynamic_index_in_dim(values, idx, axis, keepdims=False)
    got = swap_with(1, sent)
    summed = (kept + got).reshape(2, 2, *kept.shape[1:])
    one, two = lax.slice_in_dim(summed, 0, cut, axis=axis), lax.slice_in_dim(summed, cut, summed.shape[axis], axis=axis)
    one_got, two_got = swap_with(2, at(one, 1, 1 - x)), swap_with(4, at(two, 0, 1 - y))
    one, two = at(one, 1, x) + one_got, at(two, 0, y) + two_got
    one_got, two_got = swap_with(4, at(one, 0, 1 - y)), swap_with(2, at(two, 0, 1 - x))
    return jnp.concatenate([at(one, 0, y) + one_got, at(two, 0, x) + two_got], axis=axis)


def solution(mesh):
    row_spec = P(AXIS_NAME, None)
    vec_spec = P(AXIS_NAME)
    full_spec = P(None)
    batch_spec = P(AXIS_NAME, None, None)
    weight_specs = (vec_spec, row_spec, row_spec, row_spec, full_spec, full_spec, row_spec, vec_spec, row_spec, row_spec, row_spec)

    def device_step(tokens, positions, table_shard, attn_norm, w_query, w_key, w_value, q_norm, k_norm, w_out, mlp_norm, w_gate, w_up, w_down, dy_out):
        batch_len, seq_len = tokens.shape
        devices = lax.axis_size(AXIS_NAME)
        rows_local = table_shard.shape[0]
        shard = w_query.shape[0]
        all_ids = lax.all_gather(tokens, AXIS_NAME)
        norms = jnp.concatenate([attn_norm[:, None], mlp_norm[:, None], jnp.zeros((shard, W_COLS - C_NORM - 2), BF)], axis=1)
        pad = jnp.zeros((shard, HEAD), BF)
        packed = jnp.concatenate([w_query, w_key, w_value, pad, w_out, pad, w_gate, w_up, norms], axis=1)
        w_pack = lax.all_gather(packed, AXIS_NAME, tiled=True)
        w_down_full = gather_by_swaps(w_down)
        gains = w_pack[:, C_NORM:C_NORM + 2].T.astype(F32)
        head_gains = jnp.stack([q_norm, k_norm]).astype(F32)
        swapped = jnp.concatenate([head_gains[:, 32:], head_gains[:, :32]], axis=1)
        head_gains = jnp.concatenate([head_gains, swapped], axis=1)

        inv_freq = jnp.exp(jnp.arange(HEAD // 2, dtype=F32) * (-2.0 * math.log(ROPE_THETA) / HEAD))
        angles = inv_freq[:, None] * positions.reshape(1, -1).astype(F32)
        cs = jnp.concatenate([jnp.cos(angles), jnp.sin(angles)], axis=0)
        dy_t = dy_out.swapaxes(1, 2).reshape(-1, seq_len)

        starts = [sum(CHUNKS[:c]) for c in range(len(CHUNKS))]
        take_from, add_to, clashes = [], [], []
        for first, size in zip(starts, CHUNKS):
            local_ids = all_ids[:, first:first + size].reshape(-1, LANES) - lax.axis_index(AXIS_NAME) * rows_local
            is_owner = (local_ids >= 0) & (local_ids < rows_local)
            line = lax.broadcasted_iota(jnp.int32, local_ids.shape, 0)
            take_from.append((jnp.where(is_owner, local_ids, rows_local) * ROW_WORDS).reshape(-1))
            spot = jnp.where(is_owner, local_ids, rows_local + line % GROUP_ROWS)
            add_to.append((spot * ACC_WORDS + 1 - line % 2).reshape(-1))
            groups = spot.reshape(-1, GROUP_ROWS, LANES)
            twice = jnp.concatenate([groups, groups], axis=1)
            same = [jnp.any(groups == twice[:, shift:shift + GROUP_ROWS], axis=1) for shift in range(1, GROUP_ROWS // 2 + 1)]
            clashes.append(functools.reduce(jnp.logical_or, same).astype(jnp.int32).reshape(-1))

        table_t = table_shard.T
        parity = lax.axis_index(AXIS_NAME) % 2
        *mids, last_ids = take_from[1:]
        by_core = last_ids.reshape(devices // 2, 2, -1)
        kept = jnp.where(parity == 0, by_core[:, 0], by_core[:, 1]).reshape(-1)
        sent = jnp.where(parity == 0, by_core[:, 1], by_core[:, 0]).reshape(-1)
        picked = gather_rows(take_from[0], table_t, (devices * CHUNKS[0],))
        half_rows = devices // 2 * CHUNKS[-1]
        picked += gather_rows(jnp.concatenate(mids + [kept, sent]), table_t, tuple(devices * n for n in CHUNKS[1:-1]) + (half_rows, half_rows))
        *picked, kept, sent = picked
        xs = [lax.psum_scatter(rows, AXIS_NAME, scatter_dimension=0, tiled=True) for rows in picked]
        pair_rows = CHUNKS[-1] * HALF_SEQ
        split = lambda rows: rows.reshape(devices // 2, pair_rows, 2 * D)
        xs.append(reduce_by_swaps(split(kept), split(sent), -2, pair_rows // 2))
        core = lax.rem(lax.axis_index(AXIS_NAME), 2).reshape(1)
        carry = None
        rows_of = []
        for idx in range(len(CHUNKS)):
            x_chunk = xs[idx]
            dx, carry = layer_chunk(x_chunk, dy_t, cs, w_pack, w_down_full, gains, head_gains, core, starts[idx], carry, idx == len(CHUNKS) - 1, batch_len * seq_len)
            rows_of.append(lax.all_gather(dx, AXIS_NAME, tiled=True))
        *grads, y = carry
        d_table = None
        for idx in range(len(CHUNKS)):
            d_table = scatter_rows(add_to[idx], clashes[idx], rows_of[idx], rows_local, d_table, idx == len(CHUNKS) - 1)
        d_table = d_table.T
        g_pack = reduce_by_swaps(grads[0], grads[1], -1, 2560)
        d_w_down = reduce_by_swaps(grads[2], grads[3], -2, 96)
        kv_cols = w_key.shape[1]
        return (y.reshape(batch_len, seq_len, D), d_table, g_pack[:, C_NORM], g_pack[:, :D], g_pack[:, D:D + kv_cols], g_pack[:, D + kv_cols:D + 2 * kv_cols],
                g_pack[0, C_HEAD:C_HEAD + HEAD], g_pack[0, C_HEAD + HEAD:C_HEAD + 2 * HEAD], g_pack[:, C_OUT:C_OUT + D], g_pack[:, C_NORM + 1],
                g_pack[:, C_GATE:C_GATE + FF], g_pack[:, C_UP:C_UP + FF], d_w_down)

    return jax.shard_map(device_step, mesh=mesh, in_specs=(row_spec, row_spec, row_spec) + weight_specs + (batch_spec,), out_specs=(batch_spec, row_spec) + weight_specs, check_vma=False)
```

```python
import functools
import math
import jax
import jax.numpy as jnp
from jax import lax
from jax.experimental import pallas as pl
from jax.experimental.pallas import tpu as pltpu
from jax.sharding import PartitionSpec as P

NORM_EPS = 1e-6
ROPE_THETA = 1.0e6
AXIS_NAME = 'fsdp'
SEQ = 256
HALF_SEQ = SEQ // 2
SEQS = 1
LANES = 128
D = 576
FF = 1536
HEAD = 64
HEADS = 9
KV = 3
GRP = 3
C_OUT, C_GATE, C_UP, C_NORM, C_HEAD = 1024, 1664, 3200, 4736, 4864
W_COLS, G_COLS = 4864, 4992
X_K, X_V, X_COLS = HEADS * LANES, (HEADS + KV) * LANES, (HEADS + 2 * KV) * LANES
FF_STEP = 512
DOWN = FF // 8
CHUNKS = (4, 4, 4)
PAIR_WORDS = 9
BF, F32 = jnp.bfloat16, jnp.float32


def mm(lhs, rhs, lhs_dim=1, rhs_dim=0):
    return lax.dot_general(lhs, rhs, (((lhs_dim,), (rhs_dim,)), ((), ())), preferred_element_type=F32)


def fold8(values):
    return jnp.sum(values.reshape(values.shape[0] // 8, 8, values.shape[1]), axis=0)


def norm_bwd(grad_out, normed, inv_rms, norm_gain):
    grad_normed = grad_out * norm_gain
    return inv_rms * (grad_normed - normed * jnp.mean(grad_normed * normed, axis=-1, keepdims=True))


def head_norm_rope(head_ext, gain_ext, cs):
    head_f = head_ext.astype(F32)
    inv = lax.rsqrt(jnp.sum(head_f * head_f, axis=-1, keepdims=True) * (1.0 / LANES) + NORM_EPS)
    turned = head_f * inv * gain_ext * cs
    return turned + pltpu.roll(turned, HEAD, 1), inv


def head_norm_rope_bwd(grad_ext, head_ext, inv, gain_low, cs_bwd, low):
    turned = grad_ext * cs_bwd
    grad_t = turned + pltpu.roll(turned, HEAD, 1)
    normed = jnp.where(low, head_ext.astype(F32), 0.0) * inv
    grad_normed = grad_t * gain_low
    mean_term = jnp.sum(grad_normed * normed, axis=-1, keepdims=True) * (1.0 / HEAD)
    return inv * (grad_normed - normed * mean_term), fold8(grad_t * normed)


def pack_pairs(heads):
    tiles = []
    for idx in range(0, len(heads), 2):
        tile = heads[idx]
        if idx + 1 < len(heads):
            tile = tile + pltpu.roll(heads[idx + 1], HEAD, 1)
        tiles.append(tile.astype(BF))
    return tiles


def layer_kernel(first, last, steps, *refs):
    (x_ref, dy_ref, cs_ref, w_ref, wd_ref, gains_ref, head_gains_ref, core_ref) = refs[:8]
    refs = refs[8:]
    if not first:
        acc_in, accd_in, _ = refs[:3]
        refs = refs[3:]
    y_ref, dx_ref = refs[:2]
    outs = refs[2:6] if last else refs[2:4]
    (acc, accd, norm_acc, head_acc, wx, wox, qkv_s, upper_s, lower_s, cs_s, tbuf, sems) = refs[2 + len(outs):]
    step = pl.program_id(0)
    low = lax.broadcasted_iota(jnp.int32, (1, LANES), 1) < HEAD

    @pl.when(step == 0)
    def _():
        if first:
            acc[...] = jnp.zeros_like(acc)
            accd[...] = jnp.zeros_like(accd)
        else:
            load_acc = pltpu.make_async_copy(acc_in, acc, sems.at[0])
            load_accd = pltpu.make_async_copy(accd_in, accd, sems.at[1])
            load_acc.start()
            load_accd.start()
        norm_acc[...] = jnp.zeros_like(norm_acc)
        head_acc[...] = jnp.zeros_like(head_acc)
        for h in range(HEADS + 2 * KV):
            tile = w_ref[:, (h // 2) * LANES:(h // 2) * LANES + LANES].astype(F32)
            moved = pltpu.roll(tile, HEAD, 1)
            if h >= HEADS + KV:
                both = jnp.where(low, moved if h % 2 else tile, 0.0)
            else:
                twice = jnp.where(low, moved, tile) if h % 2 else jnp.where(low, tile, moved)
                both = jnp.where(low, twice, pltpu.roll(twice, 32, 1))
            wx[:, h * LANES:h * LANES + LANES] = both.astype(BF)
        for h in range(HEADS):
            wox[h * LANES:h * LANES + HEAD, :] = w_ref[h * HEAD:h * HEAD + HEAD, C_OUT:C_OUT + D]
            wox[h * LANES + HEAD:h * LANES + LANES, :] = jnp.zeros((HEAD, D), BF)
        if not first:
            load_acc.wait()
            load_accd.wait()

    gain1 = gains_ref[0:1, :]
    gain2 = gains_ref[1:2, :]
    gain_q, gain_k = head_gains_ref[0:1, :], head_gains_ref[1:2, :]
    low_q, low_k = jnp.where(low, gain_q, 0.0), jnp.where(low, gain_k, 0.0)
    scale = HEAD ** -0.5
    stacked = GRP * HALF_SEQ
    row = lax.broadcasted_iota(jnp.int32, (stacked, SEQ), 0) & (HALF_SEQ - 1)
    lower_mask = lax.broadcasted_iota(jnp.int32, (stacked, SEQ), 1) - HALF_SEQ <= row
    upper_mask = lower_mask[:, HALF_SEQ:]

    def halves(tiles):
        return jnp.concatenate([t[:HALF_SEQ] for t in tiles], axis=0), jnp.concatenate([t[HALF_SEQ:] for t in tiles], axis=0)

    def joined(upper, lower, r):
        return jnp.concatenate([part[r * HALF_SEQ:(r + 1) * HALF_SEQ] for part in (upper, lower)], axis=0)

    def softmax(scores, mask):
        scores = jnp.where(mask, scores, -1e30)
        expd = jnp.exp(scores - jnp.max(scores, axis=-1, keepdims=True))
        return expd * (1.0 / jnp.sum(expd, axis=-1, keepdims=True))

    cos_t, sin_t = cs_ref[:HEAD // 2, :], cs_ref[HEAD // 2:, :]
    cs_s[...] = jnp.concatenate([cos_t, cos_t, -sin_t, sin_t], axis=0).T

    parts = []
    for s in range(SEQS):
        pairs = x_ref[s * HALF_SEQ:(s + 1) * HALF_SEQ, :].astype(F32)
        tails = pairs[:, 512:640]
        parts.append(jnp.concatenate([pairs[:, :512], tails[:, :HEAD]], axis=1))
        parts.append(jnp.concatenate([pairs[:, 640:], pltpu.roll(tails, HEAD, 1)[:, :HEAD]], axis=1))
    x = jnp.concatenate(parts, axis=0)
    inv1 = lax.rsqrt(jnp.mean(x * x, axis=-1, keepdims=True) + NORM_EPS)
    m1 = (x * inv1 * gain1).astype(BF)
    qkv_s[...] = mm(m1, wx[...]).astype(BF)
    saved, packed = [], []
    for s in range(SEQS):
        rows = slice(s * SEQ, (s + 1) * SEQ)
        cs = cs_s[...]
        heads = []
        for g in range(KV):
            ke = qkv_s[rows, X_K + g * LANES:X_K + (g + 1) * LANES]
            v0 = qkv_s[rows, X_V + g * LANES:X_V + (g + 1) * LANES]
            k_rot, k_inv = head_norm_rope(ke, gain_k, cs)
            k0 = jnp.where(low, k_rot, 0.0).astype(BF)
            k_swap = (jnp.where(low, k_rot, pltpu.roll(k_rot, 32, 1)) * scale).astype(BF)
            qs, q_swaps, q_invs = [], [], []
            for r in range(GRP):
                h = g * GRP + r
                q_rot, q_inv = head_norm_rope(qkv_s[rows, h * LANES:(h + 1) * LANES], gain_q, cs * scale)
                qs.append(q_rot.astype(BF))
                q_swaps.append(jnp.where(low, q_rot, pltpu.roll(q_rot, 32, 1)).astype(BF))
                q_invs.append(q_inv)
            q_upper, q_lower = halves(qs)
            upper = softmax(mm(q_upper, k0[:HALF_SEQ], 1, 1), upper_mask)
            lower = softmax(mm(q_lower, k0, 1, 1), lower_mask)
            upper_s[s * KV + g] = upper
            lower_s[s * KV + g] = lower
            o_upper, o_lower = mm(upper.astype(BF), v0[:HALF_SEQ]), mm(lower.astype(BF), v0)
            heads += [joined(o_upper, o_lower, r) for r in range(GRP)]
            saved.append((k_swap, halves(q_swaps), q_invs, k_inv))
        packed.append(jnp.concatenate(pack_pairs(heads), axis=1))
    attn = jnp.concatenate(packed, axis=0)
    hidden_b = (x + mm(attn[:, :D], w_ref[:, C_OUT:C_OUT + D])).astype(BF)
    hidden = hidden_b.astype(F32)
    inv2 = lax.rsqrt(jnp.mean(hidden * hidden, axis=-1, keepdims=True) + NORM_EPS)
    m2 = (hidden * inv2 * gain2).astype(BF)

    dy_t = dy_ref[...]
    dy = dy_t.T
    m2_t = m2.T
    y = hidden
    dm2 = jnp.zeros((SEQS * SEQ, D), F32)
    for f in range(0, FF, FF_STEP):
        wg = w_ref[:, C_GATE + f:C_GATE + f + FF_STEP]
        wu = w_ref[:, C_UP + f:C_UP + f + FF_STEP]
        wd = wd_ref[f:f + FF_STEP, :]
        gate = mm(m2, wg)
        up = mm(m2, wu)
        dact = mm(dy, wd, 1, 1)
        sig = 1.0 / (1.0 + jnp.exp(-gate))
        silu = gate * sig
        act = (silu * up).astype(BF)
        y = y + mm(act, wd)
        dgate = (dact * up * sig * (1.0 + gate * (1.0 - sig))).astype(BF)
        dup = (dact * silu).astype(BF)
        dm2 = dm2 + mm(dgate, wg, 1, 1) + mm(dup, wu, 1, 1)
        acc[:, C_GATE + f:C_GATE + f + FF_STEP] += mm(m2_t, dgate)
        acc[:, C_UP + f:C_UP + f + FF_STEP] += mm(m2_t, dup)
        accd[:, f:f + FF_STEP] += mm(dy_t, act)
    y_ref[...] = y.astype(BF)
    n2 = hidden * inv2
    norm_acc[1] += fold8(dm2 * n2)
    dh = dy.astype(F32) + norm_bwd(dm2, n2, inv2, gain2)
    dh_b = dh.astype(BF)
    acc[:, C_OUT:C_OUT + D] += mm(attn.T, dh_b)[:D]

    do = mm(dh_b, wox[...], 1, 1).astype(BF)
    packed = []
    for s in range(SEQS):
        rows = slice(s * SEQ, (s + 1) * SEQ)
        cs = cs_s[...]
        cs_bwd = jnp.where(low, cs, -cs)
        dqs, dks, dvs = [], [], []
        for g in range(KV):
            k_swap, (swap_upper, swap_lower), q_invs, k_inv = saved[s * KV + g]
            v0 = qkv_s[rows, X_V + g * LANES:X_V + (g + 1) * LANES]
            do_upper, do_lower = halves([do[rows, h * LANES:(h + 1) * LANES] for h in range(g * GRP, (g + 1) * GRP)])
            upper, lower = upper_s[s * KV + g], lower_s[s * KV + g]
            d_upper, d_lower = mm(do_upper, v0[:HALF_SEQ], 1, 1), mm(do_lower, v0, 1, 1)
            ds_upper = (upper * (d_upper - jnp.sum(d_upper * upper, axis=-1, keepdims=True))).astype(BF)
            ds_lower = (lower * (d_lower - jnp.sum(d_lower * lower, axis=-1, keepdims=True))).astype(BF)

            def over_queries(left_upper, left_lower, right_upper, right_lower):
                short, full = mm(left_upper.T, right_upper), mm(left_lower.T, right_lower)
                return jnp.concatenate([(full[:, :HALF_SEQ] + short).T, full[:, HALF_SEQ:].T], axis=0)

            dvs.append(over_queries(do_upper, do_lower, upper.astype(BF), lower.astype(BF)))
            dk = over_queries(swap_upper, swap_lower, ds_upper, ds_lower)
            dk, dk_gain = head_norm_rope_bwd(dk, qkv_s[rows, X_K + g * LANES:X_K + (g + 1) * LANES], k_inv, low_k, cs_bwd, low)
            dks.append(dk)
            head_acc[1] += dk_gain
            dq_upper, dq_lower = mm(ds_upper, k_swap[:HALF_SEQ]), mm(ds_lower, k_swap)
            for r in range(GRP):
                h = g * GRP + r
                dq_h, dq_gain = head_norm_rope_bwd(joined(dq_upper, dq_lower, r), qkv_s[rows, h * LANES:(h + 1) * LANES], q_invs[r], low_q, cs_bwd, low)
                dqs.append(dq_h)
                head_acc[0] += dq_gain
        packed.append(jnp.concatenate(pack_pairs(dqs + dks + dvs), axis=1))
    dqkv = jnp.concatenate(packed, axis=0)
    acc[:, 0:1024] += mm(m1.T, dqkv)
    dm1 = mm(dqkv, w_ref[:, 0:1024], 1, 1)
    n1 = x * inv1
    norm_acc[0] += fold8(dm1 * n1)
    dx = dh + norm_bwd(dm1, n1, inv1, gain1)
    for s in range(SEQS):
        upper, lower = dx[s * SEQ:s * SEQ + HALF_SEQ], dx[s * SEQ + HALF_SEQ:(s + 1) * SEQ]
        base = s * HALF_SEQ * PAIR_WORDS
        for j in range(4):
            dx_ref[pl.ds(base + j, HALF_SEQ, stride=PAIR_WORDS), :] = upper[:, j * LANES:(j + 1) * LANES]
            dx_ref[pl.ds(base + 5 + j, HALF_SEQ, stride=PAIR_WORDS), :] = lower[:, j * LANES:(j + 1) * LANES]
        dx_ref[pl.ds(base + 4, HALF_SEQ, stride=PAIR_WORDS), :] = jnp.concatenate([upper[:, 512:], lower[:, 512:]], axis=1)

    @pl.when(step == steps - 1)
    def _():
        top = lax.broadcasted_iota(jnp.int32, (LANES, 1), 0)
        rows1 = jnp.sum(norm_acc[0], axis=0, keepdims=True)
        rows2 = jnp.sum(norm_acc[1], axis=0, keepdims=True)
        both = jnp.where(top == 0, rows1, 0.0) + jnp.where(top == 1, rows2, 0.0)
        for c in range(0, D, LANES):
            width = min(LANES, D - c)
            acc[c:c + width, C_NORM:C_NORM + LANES] += both[:, c:c + width].T
        head_q = jnp.sum(head_acc[0], axis=0, keepdims=True)
        head_k = jnp.sum(head_acc[1], axis=0, keepdims=True)
        head_row = jnp.where(low, head_q, pltpu.roll(head_k, HEAD, 1))
        acc[:, C_HEAD:C_HEAD + LANES] += jnp.broadcast_to(head_row, (D, LANES))
        if last:
            mine = core_ref[0]

            def send_block(d, src, keep, send, sem):
                @pl.when(mine == d % 2)
                def _():
                    pltpu.make_async_copy(src, keep.at[d // 2], sem).start()

                @pl.when(mine != d % 2)
                def _():
                    pltpu.make_async_copy(src, send.at[d // 2], sem).start()

                return pltpu.make_async_copy(src, keep.at[d // 2], sem)

            stores = [send_block(d, acc.at[pl.ds(d * 72, 72), :], outs[0], outs[1], sems.at[0]) for d in range(8)]
            for part in range(0, 8, 4):
                for c in range(0, 4 * DOWN, LANES):
                    for t in range(0, D, LANES):
                        width = min(LANES, D - t)
                        tbuf[c:c + LANES, t:t + width] = accd[t:t + width, part * DOWN + c:part * DOWN + c + LANES].T
                moved = [send_block(part + d, tbuf.at[pl.ds(d * DOWN, DOWN), :], outs[2], outs[3], sems.at[1]) for d in range(4)]
                for store in moved:
                    store.wait()
        else:
            stores = [pltpu.make_async_copy(acc, outs[0], sems.at[0]), pltpu.make_async_copy(accd, outs[1], sems.at[0])]
            for store in stores:
                store.start()
        for store in stores:
            store.wait()


ROW_WORDS = 5
ACC_WORDS = 6
GROUP_ROWS = 16
PAD_ROWS = 16


def gather_kernel(blocks, ids_ref, tab_ref, *refs):
    outs, (lin, buf) = refs[:-2], refs[-2:]
    step = pl.program_id(0)
    rows = tab_ref.shape[1]

    @pl.when(step == 0)
    def _():
        def build(b, _):
            at = pl.multiple_of(b * LANES, LANES)
            for j in range(ROW_WORDS):
                part = tab_ref[j * LANES:min(j * LANES + LANES, D), pl.ds(at, LANES)].astype(F32)
                if part.shape[0] < LANES:
                    part = jnp.concatenate([part, jnp.zeros((LANES - part.shape[0], LANES), F32)], axis=0)
                lin[pl.ds(at * ROW_WORDS + j, LANES, stride=ROW_WORDS), :] = part.T
            return 0

        lax.fori_loop(0, rows // LANES, build, 0)
        lin[rows * ROW_WORDS:(rows + PAD_ROWS) * ROW_WORDS, :] = jnp.zeros((PAD_ROWS * ROW_WORDS, LANES), F32)

    def pick(k, _):
        base = k * GROUP_ROWS
        got = [lin[pl.ds(ids_ref[step * SEQ + base + u], ROW_WORDS), :] for u in range(GROUP_ROWS)]
        for u in range(GROUP_ROWS):
            buf[pl.ds((base + u) * ROW_WORDS, ROW_WORDS), :] = got[u]
        return 0

    lax.fori_loop(0, SEQ // GROUP_ROWS, pick, 0)
    first = 0
    half = HALF_SEQ * ROW_WORDS
    for out, count in zip(outs, blocks):
        @pl.when((step >= first) & (step < first + count))
        def _():
            for j in range(4):
                out[:, j * LANES:j * LANES + LANES] = buf[pl.ds(j, HALF_SEQ, stride=ROW_WORDS), :].astype(BF)
                out[:, 640 + j * LANES:768 + j * LANES] = buf[pl.ds(half + j, HALF_SEQ, stride=ROW_WORDS), :].astype(BF)
            tails = buf[pl.ds(4, HALF_SEQ, stride=ROW_WORDS), :] + pltpu.roll(buf[pl.ds(half + 4, HALF_SEQ, stride=ROW_WORDS), :], HEAD, 1)
            out[:, 512:640] = tails.astype(BF)

        first += count


def gather_rows(ids, table_t, blocks):
    starts = [sum(blocks[:c]) for c in range(len(blocks))]
    rows = table_t.shape[1]
    out_spec = lambda c: pl.BlockSpec((HALF_SEQ, 2 * D), lambda i, ids: (jnp.clip(i - starts[c], 0, blocks[c] - 1), 0))
    return pl.pallas_call(
        functools.partial(gather_kernel, blocks),
        grid_spec=pltpu.PrefetchScalarGridSpec(
            num_scalar_prefetch=1,
            grid=(sum(blocks),),
            in_specs=[pl.BlockSpec(table_t.shape, lambda i, ids: (0, 0), pipeline_mode=pl.Buffered(1))],
            out_specs=[out_spec(c) for c in range(len(blocks))],
            scratch_shapes=[pltpu.VMEM(((rows + PAD_ROWS) * ROW_WORDS, LANES), F32), pltpu.VMEM((SEQ * ROW_WORDS, LANES), F32)],
        ),
        out_shape=[jax.ShapeDtypeStruct((count * HALF_SEQ, 2 * D), BF) for count in blocks],
        compiler_params=pltpu.CompilerParams(dimension_semantics=('arbitrary',), vmem_limit_bytes=48 << 20),
        cost_estimate=pl.CostEstimate(flops=40_000_000_000, bytes_accessed=40_000_000, transcendentals=0),
        name='gather_rows',
    )(ids, table_t)


def scatter_kernel(first, last, blocks, ids_ref, clash_ref, rows_ref, *refs):
    if not first:
        acc_in, refs = refs[0], refs[1:]
    out_ref, acc, sem = refs[:3]
    tbuf = refs[3] if last else None
    step = pl.program_id(0)
    rows = acc.shape[0] // ACC_WORDS - PAD_ROWS

    @pl.when(step == 0)
    def _():
        if first:
            acc[...] = jnp.zeros_like(acc)
        else:
            load = pltpu.make_async_copy(acc_in, acc, sem.at[0])
            load.start()
            load.wait()

    groups = SCATTER_ROWS // GROUP_ROWS

    def add(k, _):
        spots = [pl.ds(ids_ref[step * SCATTER_ROWS + u * LANES + k], ROW_WORDS) for u in range(GROUP_ROWS)]
        from_row = lambda u: rows_ref[pl.ds((u // 2 * LANES + k) * PAIR_WORDS + (u % 2) * 4, ROW_WORDS), :]
        clash = clash_ref[step * groups + k]

        @pl.when(clash == 0)
        def _():
            sums = [acc[spots[u], :] + from_row(u) for u in range(GROUP_ROWS)]
            for u in range(GROUP_ROWS):
                acc[spots[u], :] = sums[u]

        @pl.when(clash != 0)
        def _():
            for u in range(GROUP_ROWS):
                acc[spots[u], :] += from_row(u)

        return 0

    lax.fori_loop(0, groups, add, 0)

    @pl.when(step == blocks - 1)
    def _():
        if last:
            wide = FLUSH_ROWS

            def flush(b, _):
                slot = lax.rem(b, 2)
                at = pl.multiple_of(b * wide, wide)
                store = pltpu.make_async_copy(tbuf.at[slot], out_ref.at[:, pl.ds(at, wide)], sem.at[slot])

                @pl.when(b >= 2)
                def _():
                    store.wait()

                word = lambda w, r: acc[pl.ds((at + r) * ACC_WORDS + w, LANES, stride=ACC_WORDS), :]
                for r in range(0, wide, LANES):
                    for j in range(4):
                        tbuf[slot, j * LANES:j * LANES + LANES, r:r + LANES] = word(1 + j, r).T
                    tail = word(5, r) + pltpu.roll(word(0, r), HEAD, 1)
                    tbuf[slot, 512:D, r:r + LANES] = tail.T[:HEAD]
                store.start()
                return 0

            lax.fori_loop(0, rows // wide, flush, 0)
            for slot in range(2):
                pltpu.make_async_copy(tbuf.at[slot], out_ref.at[:, pl.ds(0, wide)], sem.at[slot]).wait()
        else:
            store = pltpu.make_async_copy(acc, out_ref, sem.at[0])
            store.start()
            store.wait()


SCATTER_ROWS = LANES * GROUP_ROWS
FLUSH_ROWS = 512


def scatter_rows(ids, clash, rows_in, table_rows, carry, last):
    first = carry is None
    blocks = rows_in.shape[0] // (SCATTER_ROWS // 2 * PAIR_WORDS)
    acc_shape = ((table_rows + PAD_ROWS) * ACC_WORDS, LANES)
    anyspec = pl.BlockSpec(memory_space=pl.ANY)
    scratch = [pltpu.VMEM(acc_shape, F32), pltpu.SemaphoreType.DMA((2,))]
    if last:
        scratch.append(pltpu.VMEM((2, D, FLUSH_ROWS), F32))
    return pl.pallas_call(
        functools.partial(scatter_kernel, first, last, blocks),
        grid_spec=pltpu.PrefetchScalarGridSpec(
            num_scalar_prefetch=2,
            grid=(blocks,),
            in_specs=[pl.BlockSpec((SCATTER_ROWS // 2 * PAIR_WORDS, LANES), lambda i, *_: (i, 0))] + ([] if first else [anyspec]),
            out_specs=anyspec,
            scratch_shapes=scratch,
        ),
        out_shape=jax.ShapeDtypeStruct((D, table_rows) if last else acc_shape, F32),
        input_output_aliases={} if first or last else {3: 0},
        compiler_params=pltpu.CompilerParams(dimension_semantics=('arbitrary',), vmem_limit_bytes=48 << 20),
        cost_estimate=pl.CostEstimate(flops=20_000_000_000, bytes_accessed=60_000_000, transcendentals=0),
        name='scatter_rows',
    )(*([ids, clash, rows_in] + ([] if first else [carry])))


def layer_chunk(x, dy, cs, w_pack, w_down, gains, head_gains, core, start, carry, last, total):
    steps = x.shape[0] // (SEQS * HALF_SEQ)
    start = start // SEQS
    first = carry is None
    whole = lambda shape: pl.BlockSpec(shape, lambda i: (0,) * len(shape), pipeline_mode=pl.Buffered(1))
    here = lambda cols: pl.BlockSpec((SEQS * SEQ, cols), lambda i: (i + start, 0))
    anyspec = pl.BlockSpec(memory_space=pl.ANY)
    in_specs = [pl.BlockSpec((SEQS * HALF_SEQ, 2 * D), lambda i: (i, 0)), pl.BlockSpec((D, SEQ), lambda i: (i + start, 0)), pl.BlockSpec((HEAD, SEQ), lambda i: (0, i + start)), whole(w_pack.shape), whole(w_down.shape), whole(gains.shape), whole(head_gains.shape), pl.BlockSpec(memory_space=pltpu.SMEM)]
    args = [x, dy, cs, w_pack, w_down, gains, head_gains, core]
    aliases = {}
    if not first:
        in_specs += [anyspec] * 3
        args += list(carry)
        aliases = {10: 0} if last else {8: 2, 9: 3, 10: 0}
    out_shape = [
        jax.ShapeDtypeStruct((total, D), BF),
        jax.ShapeDtypeStruct((steps * SEQS * HALF_SEQ * PAIR_WORDS, LANES), F32),
    ]
    grad_shapes = [(4, 72, G_COLS)] * 2 + [(4, DOWN, D)] * 2 if last else [(D, G_COLS), (D, FF)]
    out_shape += [jax.ShapeDtypeStruct(shape, F32) for shape in grad_shapes]
    y, dx, *grads = pl.pallas_call(
        functools.partial(layer_kernel, first, last, steps),
        grid=(steps,),
        in_specs=in_specs,
        out_specs=[here(D), pl.BlockSpec((SEQS * HALF_SEQ * PAIR_WORDS, LANES), lambda i: (i, 0))] + [anyspec] * len(grad_shapes),
        out_shape=out_shape,
        scratch_shapes=[
            pltpu.VMEM((D, G_COLS), F32),
            pltpu.VMEM((D, FF), F32),
            pltpu.VMEM((2, 8, D), F32),
            pltpu.VMEM((2, 8, LANES), F32),
            pltpu.VMEM((D, X_COLS), BF),
            pltpu.VMEM((HEADS * LANES, D), BF),
            pltpu.VMEM((SEQS * SEQ, X_COLS), BF),
            pltpu.VMEM((SEQS * KV, GRP * HALF_SEQ, HALF_SEQ), F32),
            pltpu.VMEM((SEQS * KV, GRP * HALF_SEQ, SEQ), F32),
            pltpu.VMEM((SEQ, LANES), F32),
            pltpu.VMEM((FF // 2, D) if last else (8, LANES), F32),
            pltpu.SemaphoreType.DMA((2,)),
        ],
        input_output_aliases=aliases,
        compiler_params=pltpu.CompilerParams(dimension_semantics=('arbitrary',), vmem_limit_bytes=62 << 20),
        cost_estimate=pl.CostEstimate(flops=steps * SEQS * 6_000_000_000, bytes_accessed=steps * SEQS * 2_500_000 + 45_000_000, transcendentals=steps * SEQS * 1_000_000),
        name='layer_chunk',
    )(*args)
    return dx, (*grads, y)


def swap_with(bit, values):
    return lax.ppermute(values, AXIS_NAME, [(i, i ^ bit) for i in range(8)])


def gather_by_swaps(shard):
    index = lax.axis_index(AXIS_NAME)
    for bit in (1, 2, 4):
        got = swap_with(bit, shard)
        second = (index // bit) % 2 == 1
        shard = jnp.where(second, jnp.concatenate([got, shard], axis=0), jnp.concatenate([shard, got], axis=0))
    return shard


def reduce_by_swaps(kept, sent, axis, cut):
    index = lax.axis_index(AXIS_NAME)
    x, y = (index // 2) % 2, index // 4
    at = lambda values, axis, idx: lax.dynamic_index_in_dim(values, idx, axis, keepdims=False)
    got = swap_with(1, sent)
    summed = (kept + got).reshape(2, 2, *kept.shape[1:])
    one, two = lax.slice_in_dim(summed, 0, cut, axis=axis), lax.slice_in_dim(summed, cut, summed.shape[axis], axis=axis)
    one_got, two_got = swap_with(2, at(one, 1, 1 - x)), swap_with(4, at(two, 0, 1 - y))
    one, two = at(one, 1, x) + one_got, at(two, 0, y) + two_got
    one_got, two_got = swap_with(4, at(one, 0, 1 - y)), swap_with(2, at(two, 0, 1 - x))
    return jnp.concatenate([at(one, 0, y) + one_got, at(two, 0, x) + two_got], axis=axis)


def solution(mesh):
    row_spec = P(AXIS_NAME, None)
    vec_spec = P(AXIS_NAME)
    full_spec = P(None)
    batch_spec = P(AXIS_NAME, None, None)
    weight_specs = (vec_spec, row_spec, row_spec, row_spec, full_spec, full_spec, row_spec, vec_spec, row_spec, row_spec, row_spec)

    def device_step(tokens, positions, table_shard, attn_norm, w_query, w_key, w_value, q_norm, k_norm, w_out, mlp_norm, w_gate, w_up, w_down, dy_out):
        batch_len, seq_len = tokens.shape
        devices = lax.axis_size(AXIS_NAME)
        rows_local = table_shard.shape[0]
        shard = w_query.shape[0]
        all_ids = lax.all_gather(tokens, AXIS_NAME)
        norms = jnp.concatenate([attn_norm[:, None], mlp_norm[:, None], jnp.zeros((shard, W_COLS - C_NORM - 2), BF)], axis=1)
        pad = jnp.zeros((shard, HEAD), BF)
        packed = jnp.concatenate([w_query, w_key, w_value, pad, w_out, pad, w_gate, w_up, norms], axis=1)
        w_pack = lax.all_gather(packed, AXIS_NAME, tiled=True)
        w_down_full = gather_by_swaps(w_down)
        gains = w_pack[:, C_NORM:C_NORM + 2].T.astype(F32)
        head_gains = jnp.stack([q_norm, k_norm]).astype(F32)
        swapped = jnp.concatenate([head_gains[:, 32:], head_gains[:, :32]], axis=1)
        head_gains = jnp.concatenate([head_gains, swapped], axis=1)

        inv_freq = jnp.exp(jnp.arange(HEAD // 2, dtype=F32) * (-2.0 * math.log(ROPE_THETA) / HEAD))
        angles = inv_freq[:, None] * positions.reshape(1, -1).astype(F32)
        cs = jnp.concatenate([jnp.cos(angles), jnp.sin(angles)], axis=0)
        dy_t = dy_out.swapaxes(1, 2).reshape(-1, seq_len)

        starts = [sum(CHUNKS[:c]) for c in range(len(CHUNKS))]
        take_from, add_to, clashes = [], [], []
        for first, size in zip(starts, CHUNKS):
            local_ids = all_ids[:, first:first + size].reshape(-1, LANES) - lax.axis_index(AXIS_NAME) * rows_local
            is_owner = (local_ids >= 0) & (local_ids < rows_local)
            line = lax.broadcasted_iota(jnp.int32, local_ids.shape, 0)
            take_from.append((jnp.where(is_owner, local_ids, rows_local) * ROW_WORDS).reshape(-1))
            spot = jnp.where(is_owner, local_ids, rows_local + line % GROUP_ROWS)
            add_to.append((spot * ACC_WORDS + 1 - line % 2).reshape(-1))
            groups = spot.reshape(-1, GROUP_ROWS, LANES)
            twice = jnp.concatenate([groups, groups], axis=1)
            same = [jnp.any(groups == twice[:, shift:shift + GROUP_ROWS], axis=1) for shift in range(1, GROUP_ROWS // 2 + 1)]
            clashes.append(functools.reduce(jnp.logical_or, same).astype(jnp.int32).reshape(-1))

        table_t = table_shard.T
        parity = lax.axis_index(AXIS_NAME) % 2
        *mids, last_ids = take_from[1:]
        by_core = last_ids.reshape(devices // 2, 2, -1)
        kept = jnp.where(parity == 0, by_core[:, 0], by_core[:, 1]).reshape(-1)
        sent = jnp.where(parity == 0, by_core[:, 1], by_core[:, 0]).reshape(-1)
        picked = gather_rows(take_from[0], table_t, (devices * CHUNKS[0],))
        half_rows = devices // 2 * CHUNKS[-1]
        picked += gather_rows(jnp.concatenate(mids + [kept, sent]), table_t, tuple(devices * n for n in CHUNKS[1:-1]) + (half_rows, half_rows))
        *picked, kept, sent = picked
        xs = [lax.psum_scatter(rows, AXIS_NAME, scatter_dimension=0, tiled=True) for rows in picked]
        pair_rows = CHUNKS[-1] * HALF_SEQ
        split = lambda rows: rows.reshape(devices // 2, pair_rows, 2 * D)
        xs.append(reduce_by_swaps(split(kept), split(sent), -2, pair_rows // 2))
        core = lax.rem(lax.axis_index(AXIS_NAME), 2).reshape(1)
        carry = None
        rows_of = []
        for idx in range(len(CHUNKS)):
            x_chunk = xs[idx]
            dx, carry = layer_chunk(x_chunk, dy_t, cs, w_pack, w_down_full, gains, head_gains, core, starts[idx], carry, idx == len(CHUNKS) - 1, batch_len * seq_len)
            rows_of.append(lax.all_gather(dx, AXIS_NAME, tiled=True))
        *grads, y = carry
        d_table = None
        for idx in range(len(CHUNKS)):
            d_table = scatter_rows(add_to[idx], clashes[idx], rows_of[idx], rows_local, d_table, idx == len(CHUNKS) - 1)
        d_table = d_table.T
        g_pack = reduce_by_swaps(grads[0], grads[1], -1, 2560)
        d_w_down = reduce_by_swaps(grads[2], grads[3], -2, 96)
        kv_cols = w_key.shape[1]
        return (y.reshape(batch_len, seq_len, D), d_table, g_pack[:, C_NORM], g_pack[:, :D], g_pack[:, D:D + kv_cols], g_pack[:, D + kv_cols:D + 2 * kv_cols],
                g_pack[0, C_HEAD:C_HEAD + HEAD], g_pack[0, C_HEAD + HEAD:C_HEAD + 2 * HEAD], g_pack[:, C_OUT:C_OUT + D], g_pack[:, C_NORM + 1],
                g_pack[:, C_GATE:C_GATE + FF], g_pack[:, C_UP:C_UP + FF], d_w_down)

    return jax.shard_map(device_step, mesh=mesh, in_specs=(row_spec, row_spec, row_spec) + weight_specs + (batch_spec,), out_specs=(batch_spec, row_spec) + weight_specs, check_vma=False)
```
